32 devices in a mesh: slab: 8 (over y, x, core), cross: 4 (over z).
Axes of the slice: x: 2, y: 2, z: 4, core: 2. Of those that a mesh axis runs over, the one named last changes fastest.
Arguments:
- velocity: float32 [3, 32, 64, 128], P(None, 'slab', 'cross'), may hold values from -6 to 6
- density: float32 [32, 64, 128], P('slab', 'cross'), may hold values from 0.5 to 2
- source: float32 [32, 64, 128], P('slab', 'cross'), may hold values from -6 to 6
- species: float32 [9, 32, 64, 128], P(None, 'slab', 'cross'), may hold values from 0 to 1
Outputs:
- velocity_out: float32 [3, 32, 64, 128], P(None, 'slab', 'cross')
- pressure: float32 [32, 64, 128], P('slab', 'cross')
- species_out: float32 [9, 32, 64, 128], P(None, 'slab', 'cross')
The draws below stay inside these ranges and needn't reach their ends.
All inputs are finite; a program needn't handle non-finite values.
Results may differ from the reference program's by a relative error of at most 0.0001.
Values sent between devices are 32-bit elements; how exact they have to be, the bound alone decides.
A program may use at most 64 MiB of HBM per device.

```python
import math
import jax
import jax.numpy as jnp

NZ = 128
SPECIES = 9
CYCLES = 2
SMOOTH = 2
COARSE = 4
NX = 32
NY = 64


def shard_levels(key, shape, pieces, low, largest):
    gain = 1.0
    for axis_at, blocks in pieces:
        heights = jax.random.uniform(jax.random.fold_in(jax.random.fold_in(key, 6), axis_at), (blocks,), jnp.float32, low / len(pieces), largest / len(pieces))
        gain = gain * jnp.repeat(jnp.exp(heights), shape[axis_at] // blocks).reshape((-1,) + (1,) * (len(shape) - 1 - axis_at))
    return gain


def centred(rng, shape, scale, reach, pieces=(), dtype=jnp.bfloat16):
    drawn = jax.random.normal(rng, shape, jnp.float32) * scale
    if len(pieces) > 0:
        drawn = shard_levels(rng, shape, pieces, -0.22, 0.18) * drawn
    return jnp.clip(drawn, min=-reach, max=reach).astype(dtype)


def setup_inputs(seed: int = 0) -> dict:
    key_of = jax.random.split(jax.random.key(seed), 5)
    velocity = centred(key_of[0], (3, NX, NY, NZ), 1.0, 6.0, ((1, 8), (2, 4)), jnp.float32)
    density = jnp.clip(jnp.exp(math.log(2.0) - 1.3862944 * jax.random.uniform(key_of[1], (NX, NY, NZ), jnp.float32) ** shard_levels(key_of[1], (NX, NY, NZ), ((0, 8), (1, 4)), -0.2, 0.2)), 0.5, 2.0)
    source = centred(key_of[2], (NX, NY, NZ), 1.0, 6.0, ((0, 8), (1, 4)), jnp.float32)
    species = jnp.clip(1.0 * jax.random.uniform(key_of[3], (SPECIES, NX, NY, NZ), jnp.float32) ** shard_levels(key_of[3], (SPECIES, NX, NY, NZ), ((1, 8), (2, 4)), -0.2, 0.2), 0.0, 1.0)
    return dict(velocity=velocity, density=density, source=source, species=species)


damping = 0.8
time_step = 0.25


def pad_plane(field, width):
    return jnp.pad(field, ((width, width), (width, width), (0, 0)))


def pad_stack(field, width):
    return jnp.pad(field, ((0, 0), (width, width), (width, width), (0, 0)))


def pad_depth(field):
    return jnp.pad(field, ((0, 0), (0, 0), (1, 1)))


def face_weights(mobile):
    face_x = 0.5 * (mobile[:-1, 1:-1] + mobile[1:, 1:-1])
    face_y = 0.5 * (mobile[1:-1, :-1] + mobile[1:-1, 1:])
    inner = pad_depth(mobile[1:-1, 1:-1])
    face_z = 0.5 * (inner[..., :-1] + inner[..., 1:])
    diagonal = face_x[:-1] + face_x[1:] + face_y[:, :-1] + face_y[:, 1:] + face_z[..., :-1] + face_z[..., 1:]
    return face_x, face_y, face_z, diagonal


def operate(field, weights):
    face_x, face_y, face_z = weights[0], weights[1], weights[2]
    center = field[1:-1, 1:-1]
    column = pad_depth(center)
    total = face_x[1:] * (field[2:, 1:-1] - center) + face_x[:-1] * (field[:-2, 1:-1] - center)
    total = total + face_y[:, 1:] * (field[1:-1, 2:] - center) + face_y[:, :-1] * (field[1:-1, :-2] - center)
    total = total + face_z[..., 1:] * (column[..., 2:] - center) + face_z[..., :-1] * (column[..., :-2] - center)
    return total


def jacobi_step(field, target, weights):
    center = field[1:-1, 1:-1]
    return center + damping * (operate(field, weights) - target) / weights[3]


def divergence(moving):
    column = pad_depth(moving[2][1:-1, 1:-1])
    total = (moving[0][2:, 1:-1] - moving[0][:-2, 1:-1]) + (moving[1][1:-1, 2:] - moving[1][1:-1, :-2])
    return 0.5 * (total + (column[..., 2:] - column[..., :-2]))


def gradient(field):
    column = pad_depth(field[1:-1, 1:-1])
    along_x = 0.5 * (field[2:, 1:-1] - field[:-2, 1:-1])
    along_y = 0.5 * (field[1:-1, 2:] - field[1:-1, :-2])
    along_z = 0.5 * (column[..., 2:] - column[..., :-2])
    return jnp.stack([along_x, along_y, along_z], 0)


def restrict(field):
    cells_x, cells_y, cells_z = field.shape
    return field.reshape(cells_x // 2, 2, cells_y // 2, 2, cells_z // 2, 2).mean(axis=(1, 3, 5))


def prolong(field):
    cells_x, cells_y, cells_z = field.shape
    spread = jnp.broadcast_to(field[:, None, :, None, :, None], (cells_x, 2, cells_y, 2, cells_z, 2))
    return spread.reshape(2 * cells_x, 2 * cells_y, 2 * cells_z)


def advect(amounts, moving):
    flow_x = 0.5 * (moving[0][:-1, 1:-1] + moving[0][1:, 1:-1])
    flux_x = jnp.maximum(flow_x, 0.0) * amounts[:, :-1, 1:-1] + jnp.minimum(flow_x, 0.0) * amounts[:, 1:, 1:-1]
    flow_y = 0.5 * (moving[1][1:-1, :-1] + moving[1][1:-1, 1:])
    flux_y = jnp.maximum(flow_y, 0.0) * amounts[:, 1:-1, :-1] + jnp.minimum(flow_y, 0.0) * amounts[:, 1:-1, 1:]
    column = pad_depth(moving[2][1:-1, 1:-1])
    flow_z = 0.5 * (column[..., :-1] + column[..., 1:])
    center = amounts[:, 1:-1, 1:-1]
    stacked = jnp.pad(center, ((0, 0), (0, 0), (0, 0), (1, 1)))
    flux_z = jnp.maximum(flow_z, 0.0) * stacked[..., :-1] + jnp.minimum(flow_z, 0.0) * stacked[..., 1:]
    change = (flux_x[:, 1:] - flux_x[:, :-1]) + (flux_y[:, :, 1:] - flux_y[:, :, :-1]) + (flux_z[..., 1:] - flux_z[..., :-1])
    return center - time_step * change


def reference(velocity, density, source, species):
    mobility = 1.0 / density
    weights = face_weights(pad_plane(mobility, 1))
    target = divergence(pad_stack(velocity, 1)) - source
    coarse_weights = tuple(0.25 * part for part in face_weights(pad_plane(restrict(mobility), 1)))
    pressure = jnp.zeros_like(density)
    for cycle_index in range(CYCLES):
        for sweep_index in range(SMOOTH):
            pressure = jacobi_step(pad_plane(pressure, 1), target, weights)
        residual = target - operate(pad_plane(pressure, 1), weights)
        coarse_target = restrict(residual)
        correction = jnp.zeros_like(coarse_target)
        for sweep_index in range(COARSE):
            correction = jacobi_step(pad_plane(correction, 1), coarse_target, coarse_weights)
        pressure = pressure + prolong(correction)
        for sweep_index in range(SMOOTH):
            pressure = jacobi_step(pad_plane(pressure, 1), target, weights)
    velocity_out = velocity - mobility[None] * gradient(pad_plane(pressure, 1))
    species_out = advect(pad_stack(species, 1), pad_stack(velocity_out, 1))
    return velocity_out, pressure, species_out
```

```python
import functools

import jax
import jax.numpy as jnp
from jax import lax
from jax.experimental import pallas as pl
from jax.experimental.pallas import tpu as pltpu
from jax.sharding import PartitionSpec as P

CYCLES = 2
COARSE = 4
damping = 0.8
time_step = 0.25
MESH = pl.DeviceIdType.MESH
RX = 5
RY = 8
CX = 6
CY = 12

NEAR = [(dx, dy) for dx in (-1, 0, 1) for dy in (-1, 0, 1) if (dx, dy) != (0, 0)] + [(-2, 0), (2, 0)]
WIDE = [(dx, dy) for dx in range(-3, 4) for dy in (-1, 0, 1) if (dx, dy) != (0, 0)]
SIDE = [(-1, 0), (1, 0), (0, -1), (0, 1)]
HX, HY = RX, RY


def kernel(
    slabs, crosses, velocity_in, density_in, source_in, species,
    out_x, out_y, out_z, out_p, rim_x, rim_y, kinds,
    velocity, density, source, fields, packed_m, packed_r, press, coarse_m, right,
    xa, xb, ya, yb, za, zb, goal, scale_back, pa, pb,
    cxa, cxb, cya, cyb, cza, czb, cinv, ca, cb, in_sem,
    f_send, f_recv, m_send, m_recv, r_send, r_recv, p_send, p_recv, s_send, s_recv,
):
    cells_x, cells_y, cells_z = density.shape
    wx, wy = cells_x + 2 * HX, cells_y + 2 * HY
    half = cells_x // 2
    cw, cy = half + 2 * CX, cells_y + 2 * CY
    own_y = pl.ds(HY, cells_y)
    own_x = pl.ds(HX, cells_x)
    own_cy = pl.ds(CY, cells_y)
    slab, cross = lax.axis_index("slab"), lax.axis_index("cross")
    f32 = jnp.float32

    def there(dx, dy):
        return (slab + dx >= 0) & (slab + dx < slabs) & (cross + dy >= 0) & (cross + dy < crosses)

    def ys(dy, k, rim):
        if dy == 0:
            return pl.ds(rim, cells_y), pl.ds(rim, cells_y)
        if dy > 0:
            return pl.ds(rim + cells_y - k, k), pl.ds(rim - k, k)
        return pl.ds(rim, k), pl.ds(rim + cells_y, k)

    def fine_cut(dx, dy):
        step = max(0, (abs(dx) - 1) * cells_x + 1) if dx != 0 else 0
        k = RX - step
        sy, dyy = ys(dy, k, HY)
        depth = min(cells_x, RX + 1 - step) if dx != 0 else cells_x
        if dx == 0:
            sx, dst_x = own_x, own_x
        elif dx > 0:
            sx, dst_x = pl.ds(HX + cells_x - depth, depth), pl.ds(HX + (1 - dx) * cells_x - depth, depth)
        else:
            sx, dst_x = pl.ds(HX, depth), pl.ds(HX - dx * cells_x, depth)
        return (sx, sy), (dst_x, dyy)

    def coarse_cut(dx, dy):
        step = (abs(dx) - 1) * half + 1 if dx != 0 else 0
        sy, dyy = ys(dy, 2 * (CX - step), CY)
        return (CX // half, sy), (CX // half - dx, dyy)

    def within(cut, ref, *lead):
        def both(dx, dy):
            src, dst = cut(dx, dy)
            return ref.at[lead + src], ref.at[lead + dst]

        return both

    def exchange(directions, cut, send, recv):
        def copy(index, dx, dy):
            src, dst = cut(dx, dy)
            return pltpu.make_async_remote_copy(
                src_ref=src, dst_ref=dst, send_sem=send.at[index], recv_sem=recv.at[index],
                device_id=(slab + dx, cross + dy), device_id_type=MESH,
            )

        def start():
            for index, (dx, dy) in enumerate(directions):
                @pl.when(there(dx, dy))
                def _():
                    copy(index, dx, dy).start()

        def arrive():
            for index, (dx, dy) in enumerate(directions):
                @pl.when(there(-dx, -dy))
                def _():
                    copy(index, dx, dy).wait_recv()

        def leave():
            for index, (dx, dy) in enumerate(directions):
                @pl.when(there(dx, dy))
                def _():
                    copy(index, dx, dy).wait_send()

        return start, arrive, leave

    def fields_cut(dx, dy):
        return within(fine_cut, fields, slice(0, 2) if abs(dx) > 1 else slice(None))(dx, dy)

    f_x = exchange(NEAR, fields_cut, f_send, f_recv)
    m_x = exchange(WIDE, within(coarse_cut, packed_m), m_send, m_recv)
    r_x = [exchange(WIDE, within(coarse_cut, packed_r, at), r_send.at[at], r_recv.at[at]) for at in range(CYCLES)]
    p_x = [exchange(NEAR, within(fine_cut, press, at), p_send.at[at], p_recv.at[at]) for at in range(CYCLES)]

    def species_cut(dx, dy):
        if dx != 0:
            return kinds.at[:, cells_x - 1 if dx > 0 else 0], rim_x.at[0 if dx > 0 else 1]
        return kinds.at[:, :, cells_y - 1 if dy > 0 else 0], rim_y.at[0 if dy > 0 else 1]

    s_x = exchange(SIDE, species_cut, s_send, s_recv)

    def grids(rows):
        lane = lax.broadcasted_iota(jnp.int32, (rows, cells_z), 1)
        row = lax.broadcasted_iota(jnp.int32, (rows, cells_z), 0)
        return row, lane

    def next_z(v, k=1):
        return pltpu.roll(v, cells_z - k, 1)

    def prev_z(v, k=1):
        return pltpu.roll(v, k, 1)

    def next_y(v, k=1):
        return pltpu.roll(v, v.shape[0] - k, 0)

    def prev_y(v, k=1):
        return pltpu.roll(v, k, 0)

    row_w, lane_w = grids(wy)
    row_c, lane_c = grids(cy)
    row_o, lane_o = grids(cells_y)

    def pair_sum(v, row, lane):
        v = v + jnp.where(row % 2 == 0, next_y(v), prev_y(v))
        return v + jnp.where(lane % 2 == 0, next_z(v), prev_z(v))

    def pack(two):
        return jnp.where(lane_o % 2 == 0, two[0], two[1])

    def unpack(ref, dst):
        for block in range(2 * CX // half + 1):
            e = ref[block]
            dst[2 * block] = jnp.where(lane_c % 2 == 0, e, prev_z(e))
            dst[2 * block + 1] = jnp.where(lane_c % 2 == 0, next_z(e), e)

    inputs = [
        pltpu.make_async_copy(src, dst, in_sem.at[at])
        for at, (src, dst) in enumerate(
            ((velocity_in, velocity), (density_in, density), (source_in, source), (species, kinds))
        )
    ]
    for copy in inputs:
        copy.start()
    for ref in (fields, packed_m, packed_r, press, rim_x, rim_y):
        ref[...] = jnp.zeros(ref.shape, f32)
    barrier = pltpu.get_barrier_semaphore()
    count = jnp.int32(0)
    for dx, dy in WIDE:
        here = there(dx, dy)
        count = count + here.astype(jnp.int32)

        @pl.when(here)
        def _():
            pl.semaphore_signal(barrier, inc=1, device_id=(slab + dx, cross + dy), device_id_type=MESH)

    for copy in inputs[:3]:
        copy.wait()
    for x in range(cells_x):
        v2 = velocity[2, x]
        dz = jnp.where(lane_o == cells_z - 1, 0.0, next_z(v2)) - jnp.where(lane_o == 0, 0.0, prev_z(v2))
        fields[0, HX + x, own_y] = 1.0 / density[x]
        fields[1, HX + x, own_y] = velocity[0, x]
        fields[2, HX + x, own_y] = velocity[1, x]
        fields[3, HX + x, own_y] = 0.5 * dz - source[x]
    means = []
    for c in range(half):
        m = 1.0 / density[2 * c] + 1.0 / density[2 * c + 1]
        means.append(0.125 * pair_sum(m, row_o, lane_o))
    packed_m[CX // half, own_cy] = pack(means)
    pl.semaphore_wait(barrier, count)
    f_x[0]()
    m_x[0]()
    inputs[3].wait()
    s_x[0]()
    f_x[1]()

    def fine_setup(rows):
        for x in rows:
            m = fields[0, x]
            lo_x, hi_x = 0.5 * (m + fields[0, x - 1]), 0.5 * (m + fields[0, x + 1])
            lo_y, hi_y = 0.5 * (m + prev_y(m)), 0.5 * (m + next_y(m))
            lo_z = 0.5 * (m + jnp.where(lane_w == 0, 0.0, prev_z(m)))
            hi_z = 0.5 * (m + jnp.where(lane_w == cells_z - 1, 0.0, next_z(m)))
            diag = lo_x + hi_x + lo_y + hi_y + lo_z + hi_z
            inside = m > 0.0
            inv = jnp.where(inside, damping / jnp.where(inside, diag, 1.0), 0.0)
            xa[x], xb[x] = lo_x * inv, hi_x * inv
            ya[x], yb[x] = lo_y * inv, hi_y * inv
            za[x] = jnp.where(lane_w == 0, 0.0, lo_z * inv)
            zb[x] = jnp.where(lane_w == cells_z - 1, 0.0, hi_z * inv)
            if HX <= x < HX + cells_x:
                scale_back[x - HX] = (diag * (1.0 / damping))[HY : HY + cells_y]
            v1 = fields[2, x]
            t = 0.5 * ((fields[1, x + 1] - fields[1, x - 1]) + (next_y(v1) - prev_y(v1))) + fields[3, x]
            b = t * inv
            goal[x] = b
            pa[x] = -b

    early = range(HX - 2, HX + cells_x + 2)
    fine_setup(early)

    def sweep(src, dst, coefs, right, low, high, k):
        xl, xu, yl, yu, zl, zu = coefs
        for x in range(low, high):
            v = src[x]
            t = xl[x] * src[x - 1] + xu[x] * src[x + 1]
            t = t + (yl[x] * prev_y(v, k) + yu[x] * next_y(v, k))
            t = t + (zl[x] * prev_z(v, k) + zu[x] * next_z(v, k))
            dst[x] = (1.0 - damping) * v + (t - right[x])

    fine = (xa, xb, ya, yb, za, zb)
    coarse = (cxa, cxb, cya, cyb, cza, czb)

    def coarse_setup(rows):
        for x in rows:
            m = coarse_m[x]
            lo_x, hi_x = 0.5 * (m + coarse_m[x - 1]), 0.5 * (m + coarse_m[x + 1])
            lo_y, hi_y = 0.5 * (m + prev_y(m, 2)), 0.5 * (m + next_y(m, 2))
            lo_z = 0.5 * (m + jnp.where(lane_c < 2, 0.0, prev_z(m, 2)))
            hi_z = 0.5 * (m + jnp.where(lane_c >= cells_z - 2, 0.0, next_z(m, 2)))
            diag = lo_x + hi_x + lo_y + hi_y + lo_z + hi_z
            inside = m > 0.0
            inv = jnp.where(inside, damping / jnp.where(inside, diag, 1.0), 0.0)
            cxa[x], cxb[x] = lo_x * inv, hi_x * inv
            cya[x], cyb[x] = lo_y * inv, hi_y * inv
            cza[x] = jnp.where(lane_c < 2, 0.0, lo_z * inv)
            czb[x] = jnp.where(lane_c >= cells_z - 2, 0.0, hi_z * inv)
            if CX <= x < CX + half:
                cinv[x - CX] = inv[CY : CY + cells_y]

    def correct(at, pre, free, reach):
        for x in range(HX, HX + cells_x):
            press[at, x, own_y] = pre[x, own_y]
        own_rows = range(CX, CX + half)
        if at == 0:
            m_x[1]()
            unpack(packed_m, coarse_m)
            coarse_setup(own_rows)
        sums = []
        for c in range(half):
            r = None
            for x in (HX + 2 * c, HX + 2 * c + 1):
                v = pre[x]
                t = xa[x] * pre[x - 1] + xb[x] * pre[x + 1]
                t = t + (ya[x] * prev_y(v) + yb[x] * next_y(v))
                t = t + (za[x] * prev_z(v) + zb[x] * next_z(v))
                d = (damping * v - (t - goal[x]))[HY : HY + cells_y] * scale_back[x - HX]
                r = d if r is None else r + d
            sums.append(0.5 * pair_sum(r, row_o, lane_o) * cinv[c])
        packed_r[at, CX // half, own_cy] = pack(sums)
        r_x[at][0]()
        p_x[at][0]()
        if at == 0:
            coarse_setup([x for x in range(1, cw - 1) if x not in own_rows])
            fine_setup([x for x in range(1, wx - 1) if x not in early])
        r_x[at][1]()
        unpack(packed_r.at[at], right)
        for x in range(cw):
            ca[x] = -right[x]
        src, dst = ca, cb
        for step in range(1, COARSE):
            sweep(src, dst, coarse, right, step, cw - step, 2)
            src, dst = dst, src
        p_x[at][1]()
        low, high = HX - reach - 2, HX + cells_x + reach + 2
        for x in range(low, high):
            pre[x] = press[at, x] + src[CX + (x - HX) // 2, pl.ds(CY - HY, wy)]
        sweep(pre, free, fine, goal, low + 1, high - 1, 1)
        sweep(free, pre, fine, goal, low + 2, high - 2, 1)

    sweep(pa, pb, fine, goal, HX - 1, HX + cells_x + 1, 1)
    correct(0, pb, pa, 3)
    sweep(pb, pa, fine, goal, HX - 2, HX + cells_x + 2, 1)
    sweep(pa, pb, fine, goal, HX - 1, HX + cells_x + 1, 1)
    correct(1, pb, pa, 2)
    last = pb

    for x in range(HX - 1, HX + cells_x + 1):
        grad = 0.5 * (last[x + 1, own_y] - last[x - 1, own_y])
        out_x[x - HX + 1] = fields[1, x, own_y] - fields[0, x, own_y] * grad
    for x in range(cells_x):
        w = x + HX
        v = last[w]
        out_y[x] = fields[2, w] - fields[0, w] * (0.5 * (next_y(v) - prev_y(v)))
        own = v[HY : HY + cells_y]
        dz = jnp.where(lane_o == cells_z - 1, 0.0, next_z(own)) - jnp.where(lane_o == 0, 0.0, prev_z(own))
        out_z[x] = velocity[2, x] - fields[0, w, own_y] * (0.5 * dz)
        out_p[x] = own
    s_x[1]()
    for x in (f_x, m_x, s_x, *r_x, *p_x):
        x[2]()


def transport(in_x, in_y, in_z, in_p, rim_x, rim_y, species, vel_out, pres_out, spec_out):
    cells_x, cells_y, cells_z = in_p.shape
    lane_o = lax.broadcasted_iota(jnp.int32, (cells_y, cells_z), 1)
    row_o = lax.broadcasted_iota(jnp.int32, (cells_y, cells_z), 0)

    def next_z(v):
        return pltpu.roll(v, cells_z - 1, 1)

    def prev_z(v):
        return pltpu.roll(v, 1, 1)

    def next_y(v):
        return pltpu.roll(v, v.shape[0] - 1, 0)

    def prev_y(v):
        return pltpu.roll(v, 1, 0)

    mid = slice(HY, HY + cells_y)
    pres_out[...] = in_p[...]
    move_x = [in_x[x] for x in range(cells_x + 2)]
    for x in range(cells_x):
        move_y, move_z = in_y[x], in_z[x]
        vel_out[0, x] = move_x[x + 1]
        vel_out[1, x] = move_y[mid]
        vel_out[2, x] = move_z
        lo_x, hi_x = 0.5 * (move_x[x] + move_x[x + 1]), 0.5 * (move_x[x + 1] + move_x[x + 2])
        lo_y, hi_y = (0.5 * (move_y + prev_y(move_y)))[mid], (0.5 * (move_y + next_y(move_y)))[mid]
        lo_z = 0.5 * (move_z + jnp.where(lane_o == 0, 0.0, prev_z(move_z)))
        hi_z = 0.5 * (move_z + jnp.where(lane_o == cells_z - 1, 0.0, next_z(move_z)))

        def into(flow):
            return time_step * jnp.maximum(flow, 0.0)

        def back(flow):
            return -time_step * jnp.minimum(flow, 0.0)

        keep = 1.0 - (into(hi_x) + into(hi_y) + into(hi_z)) - (back(lo_x) + back(lo_y) + back(lo_z))
        from_xl, from_xu = into(lo_x), back(hi_x)
        from_yl, from_yu = into(lo_y), back(hi_y)
        from_zl = jnp.where(lane_o == 0, 0.0, into(lo_z))
        from_zu = jnp.where(lane_o == cells_z - 1, 0.0, back(hi_z))
        for s in range(species.shape[0]):
            q = species[s, x]
            xl = rim_x[0, s] if x == 0 else species[s, x - 1]
            xu = rim_x[1, s] if x == cells_x - 1 else species[s, x + 1]
            yl = jnp.where(row_o == 0, rim_y[0, s, pl.ds(x, 1)], prev_y(q))
            yu = jnp.where(row_o == cells_y - 1, rim_y[1, s, pl.ds(x, 1)], next_y(q))
            total = keep * q + (from_xl * xl + from_xu * xu) + (from_yl * yl + from_yu * yu)
            spec_out[s, x] = total + (from_zl * prev_z(q) + from_zu * next_z(q))


def local(slabs, crosses, velocity, density, source, species):
    cells_x, cells_y, cells_z = density.shape
    assert cells_x == 4 and CX % (cells_x // 2) == 0 and cells_y % 8 == 0 and cells_y >= CY
    wx, wy = cells_x + 2 * HX, cells_y + 2 * HY
    half = cells_x // 2
    kinds = species.shape[0]
    f32 = jnp.float32

    def vmem(*shape):
        return pltpu.VMEM(shape, f32)

    fine, coarse = (wx, wy, cells_z), (half + 2 * CX, cells_y + 2 * CY, cells_z)
    packed = (2 * CX // half + 1,) + coarse[1:]
    near, wide, side = len(NEAR), len(WIDE), len(SIDE)
    dma = pltpu.SemaphoreType.DMA
    spec = pl.BlockSpec(memory_space=pltpu.VMEM)
    far = pl.BlockSpec(memory_space=pltpu.HBM)
    moved = [
        (cells_x + 2, cells_y, cells_z), (cells_x, wy, cells_z), density.shape, density.shape,
        (2, kinds, cells_y, cells_z), (2, kinds, cells_x, cells_z), species.shape,
    ]
    between = pl.pallas_call(
        functools.partial(kernel, slabs, crosses),
        out_shape=tuple(pltpu.VMEM(shape, f32) for shape in moved),
        in_specs=[far] * 4,
        out_specs=(spec,) * 7,
        scratch_shapes=[vmem(*velocity.shape), vmem(*density.shape), vmem(*density.shape)]
        + [vmem(4, *fine), vmem(*packed), vmem(CYCLES, *packed), vmem(CYCLES, *fine)]
        + [vmem(*coarse)] * 2
        + [vmem(*fine)] * 7 + [vmem(*density.shape)] + [vmem(*fine)] * 2
        + [vmem(*coarse)] * 6 + [vmem(half, cells_y, cells_z)] + [vmem(*coarse)] * 2
        + [dma((4,))] + [dma((near,))] * 2 + [dma((wide,))] * 2
        + [dma((CYCLES, wide))] * 2 + [dma((CYCLES, near))] * 2 + [dma((side,))] * 2,
        compiler_params=pltpu.CompilerParams(
            collective_id=0, has_side_effects=True, vmem_limit_bytes=16 << 20
        ),
        name="projection",
    )(*(pltpu.with_memory_space_constraint(a, pltpu.HBM) for a in (velocity, density, source, species)))
    return pl.pallas_call(
        transport,
        out_shape=tuple(jax.ShapeDtypeStruct(a.shape, f32) for a in (velocity, density, species)),
        in_specs=[spec] * 7,
        out_specs=(spec,) * 3,
        compiler_params=pltpu.CompilerParams(vmem_limit_bytes=8 << 20),
        name="transport",
    )(*between)


def solution(mesh):
    plane, stack = P("slab", "cross", None), P(None, "slab", "cross", None)
    return jax.shard_map(
        functools.partial(local, mesh.shape["slab"], mesh.shape["cross"]),
        mesh=mesh,
        in_specs=(stack, plane, plane, stack),
        out_specs=(stack, plane, stack),
        check_vma=False,
    )
```

```python
import functools

import jax
import jax.numpy as jnp
from jax import lax
from jax.experimental import pallas as pl
from jax.experimental.pallas import tpu as pltpu
from jax.sharding import PartitionSpec as P

CYCLES = 2
COARSE = 4
damping = 0.8
time_step = 0.25
MESH = pl.DeviceIdType.MESH
HX = 5
HY = 8
EVEN, ODD = 0, 1
OWN = 3

EDGES = (-5, -1, 0, 3, 4, 7, 8, 12)
BELOW = {-1: 2, 3: 4, 7: 6, 11: 7}
ABOVE = {-4: 0, 0: 1, 4: 3, 8: 5}


def kernel(
    slabs, crosses, velocity_in, density_in, source_in, species,
    out_x, out_y, out_z, out_p, rim_x, rim_y, kinds,
    velocity, density, source, stage, stage_x, stage_y, stage_c,
    near, later, edge_x, edge_y, press, coarse_m, packed_r, given,
    xa, xb, ya, yb, za, zb, goal, scale_back, pa, pb,
    cxa, cxb, cya, cyb, cza, czb, ca, cb, fold, spread, rim_v, rim_w, in_sem, *sems,
):
    cells_x, cells_y, cells_z = density.shape
    rows = 2 * cells_x
    wx, wy = rows + 2 * HX, cells_y + 2 * HY
    half_y = cells_y // 2
    blocks = packed_r.shape[1]
    own_y = pl.ds(HY, cells_y)
    own_c = pl.ds(half_y, half_y)
    slab, cross = lax.axis_index("slab"), lax.axis_index("cross")
    odd = slab % 2 == 1
    f32 = jnp.float32

    def there(dx, dy):
        return (slab + dx >= 0) & (slab + dx < slabs) & (cross + dy >= 0) & (cross + dy < crosses)

    groups = []

    def exchange(moves):
        at = len(groups)
        send, recv = sems[2 * at], sems[2 * at + 1]
        groups.append(len(moves))

        def copy(index):
            _, dx, dy, src, dst = moves[index]
            return pltpu.make_async_remote_copy(
                src_ref=src, dst_ref=dst, send_sem=send.at[index], recv_sem=recv.at[index],
                device_id=(slab + dx, cross + dy), device_id_type=MESH,
            )

        def each(role, sender, act):
            for index, (by, dx, dy, _, _) in enumerate(moves):
                if sender and by == role:
                    @pl.when(there(dx, dy))
                    def _():
                        act(copy(index))
                if not sender and (by + dx) % 2 == role:
                    @pl.when(there(-dx, -dy))
                    def _():
                        act(copy(index))

        def start(role):
            each(role, True, lambda c: c.start())

        def arrive(role):
            each(role, False, lambda c: c.wait_recv())

        def leave(role):
            each(role, True, lambda c: c.wait_send())

        return start, arrive, leave

    def cut_y(dy, low, high, home=0, rim=HY, span=cells_y):
        depth = high - low + 1
        if dy > 0:
            return pl.ds(home + span - high, depth), pl.ds(rim - high, depth)
        return pl.ds(home + low - 1, depth), pl.ds(rim + span + low - 1, depth)

    whole = slice(None)
    first, rest = [], []
    for by, base, out in ((EVEN, 0, -1), (ODD, cells_x, 2)):
        to = 1 - by
        lo_edge, hi_edge = EDGES.index(base), EDGES.index(base + cells_x - 1)
        at = rows if by == EVEN else -cells_x
        touch = 0 if by == EVEN else cells_x - 1
        edge = EDGES.index(at + touch)

        def seen(deep, count, at=at, by=by):
            start = deep - 1 if by == EVEN else cells_x - deep - count + 1
            return pl.ds(start, count), pl.ds(HX + at + start, count)

        for dy in (-1, 1):
            j, k = (2, 0) if dy > 0 else (1, 3)
            src, dst = seen(1, 2)
            ys, yd = cut_y(dy, 1, 2)
            first.append((by, out, dy, stage.at[whole, src, ys], near.at[whole, dst, yd]))
            ys, yd = cut_y(dy, 1, 4)
            first.append((by, out, dy, stage_x.at[min(touch, 1), ys], edge_x.at[edge, yd]))
            first.append((by, out, dy, stage_y.at[whole, j], edge_y.at[pl.ds(HX + at, cells_x), k]))
        src, dst = seen(1, 3)
        first.append((by, out, 0, stage.at[whole, src], near.at[whole, dst, own_y]))
        first.append((by, out, 0, stage_x.at[min(touch, 1)], edge_x.at[edge, own_y]))
        first.append((by, out, 0, stage_y.at[whole, pl.ds(1, 2)], edge_y.at[pl.ds(HX + at, cells_x), pl.ds(1, 2)]))
        mine = pl.ds(HX + base, cells_x)
        for dy in (-1, 1):
            j, k = (2, 0) if dy > 0 else (1, 3)
            ys, yd = cut_y(dy, 1, 3)
            first.append((by, to, dy, stage.at[whole, whole, ys], near.at[whole, mine, yd]))
            ys, yd = cut_y(dy, 1, 4)
            first.append((by, to, dy, stage_x.at[whole, ys], edge_x.at[pl.ds(lo_edge, 2), yd]))
            first.append((by, to, dy, stage_y.at[whole, j], edge_y.at[mine, k]))
        if by == EVEN:
            first.append((by, 1, 0, stage, near.at[whole, mine, own_y]))
            first.append((by, 1, 0, stage_x, edge_x.at[pl.ds(lo_edge, 2), own_y]))
            first.append((by, 1, 0, stage_y.at[whole, pl.ds(1, 2)], edge_y.at[mine, pl.ds(1, 2)]))
            first.append((by, 1, 0, stage_c, coarse_m.at[OWN, own_c]))

        for dy in (-1, 1):
            for deep, low, high in ((1, 3, 4), (3, 1, 2)):
                src, dst = seen(deep, 2)
                ys, yd = cut_y(dy, low, high)
                rest.append((by, out, dy, stage.at[whole, src, ys], later.at[whole, dst, yd]))
        src, dst = seen(4, 1)
        rest.append((by, out, 0, stage.at[whole, src], later.at[whole, dst, own_y]))
        far, row, lands = (3, cells_x - 1, -HX) if by == EVEN else (-2, 0, rows + HX - 1)
        rest.append((by, far, 0, stage.at[0, row], later.at[0, HX + lands, own_y]))
        rest.append((by, far, 0, stage_x.at[min(row, 1)], edge_x.at[EDGES.index(lands), own_y]))
        for dy in (-1, 1):
            ys, yd = cut_y(dy, 4, 5)
            rest.append((by, to, dy, stage.at[whole, whole, ys], later.at[whole, mine, yd]))

    def coarse_moves(ref):
        moves = []
        for dy in (-1, 1, 0):
            for dx, src, dst, reach in (
                (2, OWN, OWN - 2, 5), (-2, OWN, OWN + 2, 5), (4, OWN + 1, OWN - 3, 1), (-4, OWN, OWN + 4, 1), (0, OWN, OWN, 6),
            ):
                if dx == 0 and dy == 0:
                    continue
                count = 1 if abs(dx) == 4 else 2
                ys, yd = (own_c, own_c) if dy == 0 else cut_y(dy, 1, reach, half_y, half_y, half_y)
                moves.append((ODD, dx, dy, ref.at[pl.ds(src, count), ys], ref.at[pl.ds(dst, count), yd]))
        return moves

    def press_moves(ref, reach):
        moves = []
        low, high = (pl.ds(HX, reach), pl.ds(HX + rows, reach)), (pl.ds(HX + rows - reach, reach), pl.ds(HX - reach, reach))
        corner = reach - 1
        low_c, high_c = (pl.ds(HX, corner), pl.ds(HX + rows, corner)), (pl.ds(HX + rows - corner, corner), pl.ds(HX - corner, corner))
        for dy in (-1, 1):
            ys, yd = cut_y(dy, 1, corner, HY)
            moves.append((ODD, 2, dy, ref.at[high_c[0], ys], ref.at[high_c[1], yd]))
            moves.append((ODD, -2, dy, ref.at[low_c[0], ys], ref.at[low_c[1], yd]))
        moves.append((ODD, 2, 0, ref.at[high[0], own_y], ref.at[high[1], own_y]))
        moves.append((ODD, -2, 0, ref.at[low[0], own_y], ref.at[low[1], own_y]))
        own_x = pl.ds(HX, rows)
        for dy in (-1, 1):
            ys, yd = cut_y(dy, 1, reach, HY)
            moves.append((ODD, 0, dy, ref.at[own_x, ys], ref.at[own_x, yd]))
        return moves

    def species_moves():
        moves = []
        for by in (EVEN, ODD):
            for dx, dy in ((-1, 0), (1, 0), (0, -1), (0, 1)):
                if dx != 0:
                    src, dst = kinds.at[:, cells_x - 1 if dx > 0 else 0], rim_x.at[0 if dx > 0 else 1]
                else:
                    src, dst = kinds.at[:, :, cells_y - 1 if dy > 0 else 0], rim_y.at[0 if dy > 0 else 1]
                moves.append((by, dx, dy, src, dst))
        return moves

    back = [(ODD, -1, 0, pb.at[pl.ds(HX - 1, cells_x + 2)], given)]
    sides = [
        (ODD, -1, 0, rim_v.at[0], out_x.at[0]),
        (ODD, -1, 0, rim_v.at[1], out_x.at[cells_x + 1]),
        (ODD, -1, 0, rim_w.at[whole, 0], out_y.at[whole, HY - 1]),
        (ODD, -1, 0, rim_w.at[whole, 1], out_y.at[whole, HY + cells_y]),
    ]

    f_x, g_x, m_x = exchange(first), exchange(rest), exchange(coarse_moves(coarse_m))
    r_x = [exchange(coarse_moves(packed_r.at[at])) for at in range(CYCLES)]
    p_x = [exchange(press_moves(press.at[at], HX - at)) for at in range(CYCLES)]
    s_x, b_x, v_x = exchange(species_moves()), exchange(back), exchange(sides)
    every = (f_x, g_x, m_x, *r_x, *p_x, s_x, b_x, v_x)

    def grids(count):
        lane = lax.broadcasted_iota(jnp.int32, (count, cells_z), 1)
        row = lax.broadcasted_iota(jnp.int32, (count, cells_z), 0)
        return row, lane

    def next_z(v, k=1):
        return pltpu.roll(v, cells_z - k, 1)

    def prev_z(v, k=1):
        return pltpu.roll(v, k, 1)

    def next_y(v):
        return pltpu.roll(v, v.shape[0] - 1, 0)

    def prev_y(v):
        return pltpu.roll(v, 1, 0)

    def pack(two):
        lane = grids(two[0].shape[0])[1]
        return jnp.where(lane % 2 == 0, two[0] + next_z(two[0]), two[1] + prev_z(two[1]))

    inputs = [
        pltpu.make_async_copy(src, dst, in_sem.at[at])
        for at, (src, dst) in enumerate(
            ((velocity_in, velocity), (density_in, density), (source_in, source), (species, kinds))
        )
    ]
    for copy in inputs:
        copy.start()
    for ref in (near, later, edge_x, edge_y, coarse_m, packed_r, press, rim_x, rim_y):
        ref[...] = jnp.zeros(ref.shape, f32)

    barrier = pltpu.get_barrier_semaphore()
    greet = {ODD: set(), EVEN: set()}
    for moves in (first, rest, coarse_moves(coarse_m), press_moves(press.at[0], HX), species_moves(), back):
        for by, dx, dy, _, _ in moves:
            greet[by].add((dx, dy))
            greet[(by + dx) % 2].add((-dx, -dy))
    count = jnp.int32(0)
    for role in (EVEN, ODD):
        for dx, dy in sorted(greet[role]):
            here = there(dx, dy) & (odd if role == ODD else jnp.logical_not(odd))
            count = count + here.astype(jnp.int32)

            @pl.when(here)
            def _():
                pl.semaphore_signal(barrier, inc=1, device_id=(slab + dx, cross + dy), device_id_type=MESH)

    for copy in inputs[:3]:
        copy.wait()
    row_o, lane_o = grids(cells_y)
    for x in range(cells_x):
        v0, v1, v2 = velocity[0, x], velocity[1, x], velocity[2, x]
        dz = jnp.where(lane_o == cells_z - 1, 0.0, next_z(v2)) - jnp.where(lane_o == 0, 0.0, prev_z(v2))
        dy = jnp.where(row_o == cells_y - 1, 0.0, next_y(v1)) - jnp.where(row_o == 0, 0.0, prev_y(v1))
        t = dy + dz
        if x + 1 < cells_x:
            t = t + velocity[0, x + 1]
        if x > 0:
            t = t - velocity[0, x - 1]
        m = 1.0 / density[x]
        stage[0, x] = m
        stage[1, x] = 0.5 * t - source[x]
        fold[x] = m
        stage_y[x, pl.ds(1, 1)] = 0.5 * v1[0:1]
        stage_y[x, pl.ds(2, 1)] = 0.5 * v1[cells_y - 1 : cells_y]
        if x == 0:
            stage_x[0] = 0.5 * v0
        if x == cells_x - 1:
            stage_x[1] = 0.5 * v0

    def folded(x):
        return fold[x, pl.ds(0, half_y, stride=2)] + fold[x, pl.ds(1, half_y, stride=2)]

    mean = 0.125 * pack([folded(0) + folded(1), folded(2) + folded(3)])
    stage_c[...] = mean
    pl.semaphore_wait(barrier, count)

    @pl.when(jnp.logical_not(odd))
    def _():
        f_x[0](EVEN)
        g_x[0](EVEN)
        inputs[3].wait()
        s_x[0](EVEN)
        b_x[1](EVEN)
        for x in range(cells_x):
            m = stage[0, x]
            p = given[1 + x, own_y]
            out_x[1 + x] = velocity[0, x] - m * (0.5 * (given[2 + x, own_y] - given[x, own_y]))
            grad = given[1 + x, pl.ds(HY + 1, cells_y)] - given[1 + x, pl.ds(HY - 1, cells_y)]
            out_y[x, own_y] = velocity[1, x] - m * (0.5 * grad)
            row_o, lane_o = grids(cells_y)
            dz = jnp.where(lane_o == cells_z - 1, 0.0, next_z(p)) - jnp.where(lane_o == 0, 0.0, prev_z(p))
            out_z[x] = velocity[2, x] - m * (0.5 * dz)
            out_p[x] = p
        v_x[1](EVEN)
        s_x[1](EVEN)
        for x in every:
            x[2](EVEN)

    @pl.when(odd)
    def _():
        f_x[0](ODD)
        g_x[0](ODD)
        row_w, lane_w = grids(wy)
        row_c, lane_c = grids(2 * half_y + half_y)
        even_c = lane_c % 2 == 0
        row_o, lane_o = grids(cells_y)
        mine = pl.ds(HX + cells_x, cells_x)
        near[0, mine, own_y] = stage[0]
        near[1, mine, own_y] = stage[1]
        edge_x[pl.ds(EDGES.index(cells_x), 2), own_y] = stage_x[...]
        edge_y[mine, pl.ds(1, 2)] = stage_y[:, pl.ds(1, 2)]
        coarse_m[OWN + 1, own_c] = stage_c[...]
        f_x[1](ODD)
        m_x[0](ODD)

        def fine_setup(span, full):
            def mob(x):
                return near[0, x] + later[0, x] if full else near[0, x]

            for x in span:
                m = mob(x)
                lo_x, hi_x = m + mob(x - 1), m + mob(x + 1)
                lo_y, hi_y = m + prev_y(m), m + next_y(m)
                lo_z = m + jnp.where(lane_w == 0, 0.0, prev_z(m))
                hi_z = m + jnp.where(lane_w == cells_z - 1, 0.0, next_z(m))
                diag = (lo_x + hi_x) + (lo_y + hi_y) + (lo_z + hi_z)
                inside = m > 0.0
                inv = jnp.where(inside, damping / jnp.where(inside, diag, 1.0), 0.0)
                xa[x], xb[x] = lo_x * inv, hi_x * inv
                ya[x], yb[x] = lo_y * inv, hi_y * inv
                za[x] = jnp.where(lane_w == 0, 0.0, lo_z * inv)
                zb[x] = jnp.where(lane_w == cells_z - 1, 0.0, hi_z * inv)
                t = near[1, x] + later[1, x] if full else near[1, x]
                at = x - HX
                if at in BELOW and (full or BELOW[at] not in (0, 7)):
                    t = t + edge_x[BELOW[at]]
                if at in ABOVE and (full or ABOVE[at] not in (0, 7)):
                    t = t - edge_x[ABOVE[at]]

                def side(j):
                    return jnp.broadcast_to(edge_y[x, pl.ds(j, 1)], t.shape)

                t = t + jnp.where(row_w == HY - 1, side(1), 0.0) - jnp.where(row_w == HY, side(0), 0.0)
                t = t + jnp.where(row_w == HY + cells_y - 1, side(3), 0.0)
                t = t - jnp.where(row_w == HY + cells_y, side(2), 0.0)
                b = t * (inv + inv)
                goal[x] = b
                if not full:
                    pa[x] = -b
                    if HX <= x < HX + rows:
                        scale_back[x - HX] = (diag * (0.5 / damping))[HY : HY + cells_y]

        fine_setup(range(HX - 2, HX + rows + 2), False)

        def sweep(src, dst, low, high):
            for x in range(low, high):
                v = src[x]
                t = xa[x] * src[x - 1] + xb[x] * src[x + 1]
                t = t + (ya[x] * prev_y(v) + yb[x] * next_y(v))
                t = t + (za[x] * prev_z(v) + zb[x] * next_z(v))
                dst[x] = (1.0 - damping) * v + (t - goal[x])

        def beside(ref, low, high):
            up = {b: next_z(ref[b]) for b in range(max(low - 1, 0), high)}
            down = {b: prev_z(ref[b]) for b in range(low, min(high + 1, blocks))}
            for b in range(low, high):
                yield b, jnp.where(even_c, up[max(b - 1, 0)], down[b]), jnp.where(even_c, up[b], down[min(b + 1, blocks - 1)])

        def coarse_setup():
            for b, lo, hi in beside(coarse_m, 0, blocks):
                m = coarse_m[b]
                if b == 0:
                    lo = jnp.where(even_c, 0.0, lo)
                if b == blocks - 1:
                    hi = jnp.where(even_c, hi, 0.0)
                lo_x, hi_x = m + lo, m + hi
                lo_y, hi_y = m + prev_y(m), m + next_y(m)
                lo_z = m + jnp.where(lane_c < 2, 0.0, prev_z(m, 2))
                hi_z = m + jnp.where(lane_c >= cells_z - 2, 0.0, next_z(m, 2))
                diag = (lo_x + hi_x) + (lo_y + hi_y) + (lo_z + hi_z)
                inside = m > 0.0
                inv = jnp.where(inside, damping / jnp.where(inside, diag, 1.0), 0.0)
                cxa[b], cxb[b] = lo_x * inv, hi_x * inv
                cya[b], cyb[b] = lo_y * inv, hi_y * inv
                cza[b] = jnp.where(lane_c < 2, 0.0, lo_z * inv)
                czb[b] = jnp.where(lane_c >= cells_z - 2, 0.0, hi_z * inv)

        def own_inverse(b):
            m = coarse_m[b]
            lo = jnp.where(even_c, next_z(coarse_m[b - 1]), prev_z(m))
            hi = jnp.where(even_c, next_z(m), prev_z(coarse_m[b + 1]))
            total = (lo + hi) + (prev_y(m) + next_y(m)) + 6.0 * m
            total = total + jnp.where(lane_c < 2, 0.0, prev_z(m, 2)) + jnp.where(lane_c >= cells_z - 2, 0.0, next_z(m, 2))
            return damping / total[half_y : 2 * half_y]

        def coarse_sweep(src, dst, right, low, high):
            for b, lo, hi in beside(src, low, high):
                v = src[b]
                t = cxa[b] * lo + cxb[b] * hi
                t = t + (cya[b] * prev_y(v) + cyb[b] * next_y(v))
                t = t + (cza[b] * prev_z(v, 2) + czb[b] * next_z(v, 2))
                dst[b] = (1.0 - damping) * v + (t - right[b])

        def correct(at, pre, free, reach):
            press[at, pl.ds(HX, rows), own_y] = pre[pl.ds(HX, rows), own_y]
            for x in range(HX, HX + rows, 2):
                total = None
                for w in (x, x + 1):
                    v = pre[w]
                    t = xa[w] * pre[w - 1] + xb[w] * pre[w + 1]
                    t = t + (ya[w] * prev_y(v) + yb[w] * next_y(v))
                    t = t + (za[w] * prev_z(v) + zb[w] * next_z(v))
                    d = (damping * v - (t - goal[w]))[HY : HY + cells_y] * scale_back[w - HX]
                    total = d if total is None else total + d
                fold[(x - HX) // 2] = total
            if at == 0:
                m_x[1](ODD)
            for b in range(2):
                packed_r[at, OWN + b, own_c] = pack([folded(2 * b), folded(2 * b + 1)]) * own_inverse(OWN + b)
            r_x[at][0](ODD)
            p_x[at][0](ODD)
            if at == 0:
                coarse_setup()
                inputs[3].wait()
                s_x[0](ODD)
                g_x[1](ODD)
                fine_setup(range(1, wx - 1), True)
            r_x[at][1](ODD)
            right = packed_r.at[at]
            for b in range(blocks):
                ca[b] = -right[b]
            coarse_sweep(ca, cb, right, 0, blocks)
            coarse_sweep(cb, ca, right, 1, blocks - 1)
            coarse_sweep(ca, cb, right, 1, blocks - 1)
            margin = half_y - HY // 2
            for q in range(-3, rows // 2 + 3):
                v = cb[OWN + q // 2]
                v = jnp.where(even_c, v, prev_z(v)) if q % 2 == 0 else jnp.where(even_c, next_z(v), v)
                v = v[margin : margin + wy // 2]
                spread[q + 3, pl.ds(0, wy // 2, stride=2)] = v
                spread[q + 3, pl.ds(1, wy // 2, stride=2)] = v
            p_x[at][1](ODD)
            low, high = HX - reach - 2, HX + rows + reach + 2
            for x in range(low, high):
                pre[x] = press[at, x] + spread[(x - HX) // 2 + 3]
            sweep(pre, free, low + 1, high - 1)
            sweep(free, pre, low + 2, high - 2)

        sweep(pa, pb, HX - 1, HX + rows + 1)
        correct(0, pb, pa, 3)
        sweep(pb, pa, HX - 2, HX + rows + 2)
        sweep(pa, pb, HX - 1, HX + rows + 1)
        correct(1, pb, pa, 2)
        last = pb
        b_x[0](ODD)

        def along_x(x):
            return near[0, x, own_y] * (0.5 * (last[x + 1, own_y] - last[x - 1, own_y]))

        def along_y(x, y):
            one = pl.ds(y, 1)
            return near[0, x, one] * (0.5 * (last[x, pl.ds(y + 1, 1)] - last[x, pl.ds(y - 1, 1)]))

        def edge(at):
            v = edge_x[EDGES.index(at), own_y]
            return (v + v) - along_x(HX + at)

        def ends(x):
            lo, hi = edge_y[x, pl.ds(0, 1)], edge_y[x, pl.ds(3, 1)]
            return (lo + lo) - along_y(x, HY - 1), (hi + hi) - along_y(x, HY + cells_y)

        rim_v[0] = edge(-1)
        rim_v[1] = edge(cells_x)
        for x in range(cells_x):
            lo, hi = ends(HX + x)
            rim_w[x, pl.ds(0, 1)] = lo
            rim_w[x, pl.ds(1, 1)] = hi
        v_x[0](ODD)
        out_x[0] = edge(cells_x - 1)
        out_x[cells_x + 1] = edge(rows)
        for x in range(cells_x):
            w = HX + cells_x + x
            m = near[0, w, own_y]
            p = last[w, own_y]
            out_x[1 + x] = velocity[0, x] - along_x(w)
            grad = last[w, pl.ds(HY + 1, cells_y)] - last[w, pl.ds(HY - 1, cells_y)]
            out_y[x, own_y] = velocity[1, x] - m * (0.5 * grad)
            lo, hi = ends(w)
            out_y[x, pl.ds(HY - 1, 1)] = lo
            out_y[x, pl.ds(HY + cells_y, 1)] = hi
            dz = jnp.where(lane_o == cells_z - 1, 0.0, next_z(p)) - jnp.where(lane_o == 0, 0.0, prev_z(p))
            out_z[x] = velocity[2, x] - m * (0.5 * dz)
            out_p[x] = p
        s_x[1](ODD)
        for x in every:
            x[2](ODD)

    assert groups == MOVES, groups


MOVES = [34, 18, 14, 14, 14, 8, 8, 8, 1, 4]


def transport(in_x, in_y, in_z, in_p, rim_x, rim_y, species, vel_out, pres_out, spec_out):
    cells_x, cells_y, cells_z = in_p.shape
    lane_o = lax.broadcasted_iota(jnp.int32, (cells_y, cells_z), 1)
    row_o = lax.broadcasted_iota(jnp.int32, (cells_y, cells_z), 0)

    def next_z(v):
        return pltpu.roll(v, cells_z - 1, 1)

    def prev_z(v):
        return pltpu.roll(v, 1, 1)

    def next_y(v):
        return pltpu.roll(v, v.shape[0] - 1, 0)

    def prev_y(v):
        return pltpu.roll(v, 1, 0)

    mid = slice(HY, HY + cells_y)
    pres_out[...] = in_p[...]
    move_x = [in_x[x] for x in range(cells_x + 2)]
    for x in range(cells_x):
        move_y, move_z = in_y[x], in_z[x]
        vel_out[0, x] = move_x[x + 1]
        vel_out[1, x] = move_y[mid]
        vel_out[2, x] = move_z
        lo_x, hi_x = 0.5 * (move_x[x] + move_x[x + 1]), 0.5 * (move_x[x + 1] + move_x[x + 2])
        lo_y, hi_y = (0.5 * (move_y + prev_y(move_y)))[mid], (0.5 * (move_y + next_y(move_y)))[mid]
        lo_z = 0.5 * (move_z + jnp.where(lane_o == 0, 0.0, prev_z(move_z)))
        hi_z = 0.5 * (move_z + jnp.where(lane_o == cells_z - 1, 0.0, next_z(move_z)))

        def into(flow):
            return time_step * jnp.maximum(flow, 0.0)

        def back(flow):
            return -time_step * jnp.minimum(flow, 0.0)

        keep = 1.0 - (into(hi_x) + into(hi_y) + into(hi_z)) - (back(lo_x) + back(lo_y) + back(lo_z))
        from_xl, from_xu = into(lo_x), back(hi_x)
        from_yl, from_yu = into(lo_y), back(hi_y)
        from_zl = jnp.where(lane_o == 0, 0.0, into(lo_z))
        from_zu = jnp.where(lane_o == cells_z - 1, 0.0, back(hi_z))
        for s in range(species.shape[0]):
            q = species[s, x]
            xl = rim_x[0, s] if x == 0 else species[s, x - 1]
            xu = rim_x[1, s] if x == cells_x - 1 else species[s, x + 1]
            yl = jnp.where(row_o == 0, rim_y[0, s, pl.ds(x, 1)], prev_y(q))
            yu = jnp.where(row_o == cells_y - 1, rim_y[1, s, pl.ds(x, 1)], next_y(q))
            total = keep * q + (from_xl * xl + from_xu * xu) + (from_yl * yl + from_yu * yu)
            spec_out[s, x] = total + (from_zl * prev_z(q) + from_zu * next_z(q))


def local(slabs, crosses, velocity, density, source, species):
    cells_x, cells_y, cells_z = density.shape
    assert cells_x == 4 and cells_y == 2 * HY and slabs % 2 == 0
    rows = 2 * cells_x
    wx, wy = rows + 2 * HX, cells_y + 2 * HY
    half_y = cells_y // 2
    kinds = species.shape[0]
    f32 = jnp.float32

    def vmem(*shape):
        return pltpu.VMEM(shape, f32)

    blocks = 2 * OWN + 2
    fine, coarse = (wx, wy, cells_z), (blocks, 3 * half_y, cells_z)
    dma = pltpu.SemaphoreType.DMA
    spec = pl.BlockSpec(memory_space=pltpu.VMEM)
    far = pl.BlockSpec(memory_space=pltpu.HBM)
    moved = [
        (cells_x + 2, cells_y, cells_z), (cells_x, wy, cells_z), density.shape, density.shape,
        (2, kinds, cells_y, cells_z), (2, kinds, cells_x, cells_z), species.shape,
    ]
    between = pl.pallas_call(
        functools.partial(kernel, slabs, crosses),
        out_shape=tuple(pltpu.VMEM(shape, f32) for shape in moved),
        in_specs=[far] * 4,
        out_specs=(spec,) * 7,
        scratch_shapes=[vmem(*velocity.shape), vmem(*density.shape), vmem(*density.shape)]
        + [vmem(2, *density.shape), vmem(2, cells_y, cells_z), vmem(cells_x, 8, cells_z), vmem(half_y, cells_z)]
        + [vmem(2, *fine)] * 2 + [vmem(len(EDGES), wy, cells_z), vmem(wx, 8, cells_z)]
        + [vmem(CYCLES, *fine), vmem(*coarse), vmem(CYCLES, *coarse), vmem(cells_x + 2, wy, cells_z)]
        + [vmem(*fine)] * 7 + [vmem(rows, cells_y, cells_z)] + [vmem(*fine)] * 2
        + [vmem(*coarse)] * 8 + [vmem(cells_x, cells_y, cells_z), vmem(rows // 2 + 6, wy, cells_z)]
        + [vmem(2, cells_y, cells_z), vmem(cells_x, 8, cells_z)]
        + [dma((4,))] + [dma((n,)) for n in MOVES for _ in range(2)],
        compiler_params=pltpu.CompilerParams(
            collective_id=0, has_side_effects=True, vmem_limit_bytes=16 << 20
        ),
        name="projection",
    )(*(pltpu.with_memory_space_constraint(a, pltpu.HBM) for a in (velocity, density, source, species)))
    return pl.pallas_call(
        transport,
        out_shape=tuple(jax.ShapeDtypeStruct(a.shape, f32) for a in (velocity, density, species)),
        in_specs=[spec] * 7,
        out_specs=(spec,) * 3,
        compiler_params=pltpu.CompilerParams(vmem_limit_bytes=8 << 20),
        name="transport",
    )(*between)


def solution(mesh):
    plane, stack = P("slab", "cross", None), P(None, "slab", "cross", None)
    return jax.shard_map(
        functools.partial(local, mesh.shape["slab"], mesh.shape["cross"]),
        mesh=mesh,
        in_specs=(stack, plane, plane, stack),
        out_specs=(stack, plane, stack),
        check_vma=False,
    )
```

```python
import functools

import jax
import jax.numpy as jnp
from jax import lax
from jax.experimental import pallas as pl
from jax.experimental.pallas import tpu as pltpu
from jax.sharding import PartitionSpec as P

CYCLES = 2
COARSE = 4
damping = 0.8
time_step = 0.25
MESH = pl.DeviceIdType.MESH
HX = 5
HY = 8
EVEN, ODD = 0, 1
OWN = 3

EDGES = (-5, -1, 0, 3, 4, 7, 8, 12)
BELOW = {-1: 2, 3: 4, 7: 6, 11: 7}
ABOVE = {-4: 0, 0: 1, 4: 3, 8: 5}


def kernel(
    slabs, crosses, velocity_in, density_in, source_in, species,
    out_x, out_y, out_z, out_p, rim_x, rim_y, kinds,
    velocity, density, source, stage, stage_x, stage_y, stage_c,
    near, later, edge_x, edge_y, press, coarse_m, packed_r, given,
    xa, xb, ya, yb, za, zb, goal, scale_back, pa, pb,
    cxa, cxb, cya, cyb, cza, czb, cinv, right, ca, cb, fold, spread, rim_v, rim_w, in_sem, *sems,
):
    cells_x, cells_y, cells_z = density.shape
    rows = 2 * cells_x
    wx, wy = rows + 2 * HX, cells_y + 2 * HY
    half_y = cells_y // 2
    blocks = packed_r.shape[1]
    own_y = pl.ds(HY, cells_y)
    own_c = pl.ds(half_y, half_y)
    slab, cross = lax.axis_index("slab"), lax.axis_index("cross")
    odd = slab % 2 == 1
    f32 = jnp.float32

    def there(dx, dy):
        return (slab + dx >= 0) & (slab + dx < slabs) & (cross + dy >= 0) & (cross + dy < crosses)

    groups = []

    def exchange(moves):
        at = len(groups)
        send, recv = sems[2 * at], sems[2 * at + 1]
        groups.append(len(moves))

        def copy(index):
            _, dx, dy, src, dst = moves[index]
            return pltpu.make_async_remote_copy(
                src_ref=src, dst_ref=dst, send_sem=send.at[index], recv_sem=recv.at[index],
                device_id=(slab + dx, cross + dy), device_id_type=MESH,
            )

        def each(role, sender, act):
            for index, (by, dx, dy, _, _) in enumerate(moves):
                if sender and by == role:
                    @pl.when(there(dx, dy))
                    def _():
                        act(copy(index))
                if not sender and (by + dx) % 2 == role:
                    @pl.when(there(-dx, -dy))
                    def _():
                        act(copy(index))

        def start(role):
            each(role, True, lambda c: c.start())

        def arrive(role):
            each(role, False, lambda c: c.wait_recv())

        def leave(role):
            each(role, True, lambda c: c.wait_send())

        return start, arrive, leave

    def cut_y(dy, low, high, home=0, rim=HY, span=cells_y):
        depth = high - low + 1
        if dy > 0:
            return pl.ds(home + span - high, depth), pl.ds(rim - high, depth)
        return pl.ds(home + low - 1, depth), pl.ds(rim + span + low - 1, depth)

    whole = slice(None)
    first, rest = [], []
    for by, base, out in ((EVEN, 0, -1), (ODD, cells_x, 2)):
        to = 1 - by
        lo_edge, hi_edge = EDGES.index(base), EDGES.index(base + cells_x - 1)
        at = rows if by == EVEN else -cells_x
        touch = 0 if by == EVEN else cells_x - 1
        edge = EDGES.index(at + touch)

        def seen(deep, count, at=at, by=by):
            start = deep - 1 if by == EVEN else cells_x - deep - count + 1
            return pl.ds(start, count), pl.ds(HX + at + start, count)

        for dy in (-1, 1):
            j, k = (2, 0) if dy > 0 else (1, 3)
            src, dst = seen(1, 2)
            ys, yd = cut_y(dy, 1, 2)
            first.append((by, out, dy, stage.at[whole, src, ys], near.at[whole, dst, yd]))
            ys, yd = cut_y(dy, 1, 4)
            first.append((by, out, dy, stage_x.at[min(touch, 1), ys], edge_x.at[edge, yd]))
            first.append((by, out, dy, stage_y.at[whole, j], edge_y.at[pl.ds(HX + at, cells_x), k]))
        src, dst = seen(1, 3)
        first.append((by, out, 0, stage.at[whole, src], near.at[whole, dst, own_y]))
        first.append((by, out, 0, stage_x.at[min(touch, 1)], edge_x.at[edge, own_y]))
        first.append((by, out, 0, stage_y.at[whole, pl.ds(1, 2)], edge_y.at[pl.ds(HX + at, cells_x), pl.ds(1, 2)]))
        mine = pl.ds(HX + base, cells_x)
        for dy in (-1, 1):
            j, k = (2, 0) if dy > 0 else (1, 3)
            ys, yd = cut_y(dy, 1, 3)
            first.append((by, to, dy, stage.at[whole, whole, ys], near.at[whole, mine, yd]))
            ys, yd = cut_y(dy, 1, 4)
            first.append((by, to, dy, stage_x.at[whole, ys], edge_x.at[pl.ds(lo_edge, 2), yd]))
            first.append((by, to, dy, stage_y.at[whole, j], edge_y.at[mine, k]))
        if by == EVEN:
            first.append((by, 1, 0, stage, near.at[whole, mine, own_y]))
            first.append((by, 1, 0, stage_x, edge_x.at[pl.ds(lo_edge, 2), own_y]))
            first.append((by, 1, 0, stage_y.at[whole, pl.ds(1, 2)], edge_y.at[mine, pl.ds(1, 2)]))
            first.append((by, 1, 0, stage_c, coarse_m.at[OWN, own_c]))

        for dy in (-1, 1):
            for deep, low, high in ((1, 3, 4), (3, 1, 2)):
                src, dst = seen(deep, 2)
                ys, yd = cut_y(dy, low, high)
                rest.append((by, out, dy, stage.at[whole, src, ys], later.at[whole, dst, yd]))
        src, dst = seen(4, 1)
        rest.append((by, out, 0, stage.at[whole, src], later.at[whole, dst, own_y]))
        far, row, lands = (3, cells_x - 1, -HX) if by == EVEN else (-2, 0, rows + HX - 1)
        rest.append((by, far, 0, stage.at[0, row], later.at[0, HX + lands, own_y]))
        rest.append((by, far, 0, stage_x.at[min(row, 1)], edge_x.at[EDGES.index(lands), own_y]))
        for dy in (-1, 1):
            ys, yd = cut_y(dy, 4, 5)
            rest.append((by, to, dy, stage.at[whole, whole, ys], later.at[whole, mine, yd]))

    def coarse_moves(ref):
        moves = []
        ahead, behind, ahead_far, behind_far, aside = (
            (2, OWN, OWN - 2, 2, 5), (-2, OWN, OWN + 2, 2, 5), (4, OWN + 1, OWN - 3, 1, 1), (-4, OWN, OWN + 4, 1, 1), (0, OWN, OWN, 2, 6),
        )
        for dy, kinds_of in (
            (-1, (ahead, behind)), (1, (ahead, behind)), (0, (ahead, behind)),
            (-1, (ahead_far, behind_far)), (1, (ahead_far, behind_far)), (0, (ahead_far, behind_far)), (-1, (aside,)), (1, (aside,)),
        ):
            for dx, src, dst, count, reach in kinds_of:
                ys, yd = (own_c, own_c) if dy == 0 else cut_y(dy, 1, reach, half_y, half_y, half_y)
                moves.append((ODD, dx, dy, ref.at[pl.ds(src, count), ys], ref.at[pl.ds(dst, count), yd]))
        return moves

    def press_moves(ref, reach):
        moves = []
        low, high = (pl.ds(HX, reach), pl.ds(HX + rows, reach)), (pl.ds(HX + rows - reach, reach), pl.ds(HX - reach, reach))
        corner = reach - 1
        low_c, high_c = (pl.ds(HX, corner), pl.ds(HX + rows, corner)), (pl.ds(HX + rows - corner, corner), pl.ds(HX - corner, corner))
        for dy in (-1, 1):
            ys, yd = cut_y(dy, 1, corner, HY)
            moves.append((ODD, 2, dy, ref.at[high_c[0], ys], ref.at[high_c[1], yd]))
            moves.append((ODD, -2, dy, ref.at[low_c[0], ys], ref.at[low_c[1], yd]))
        moves.append((ODD, 2, 0, ref.at[high[0], own_y], ref.at[high[1], own_y]))
        moves.append((ODD, -2, 0, ref.at[low[0], own_y], ref.at[low[1], own_y]))
        own_x = pl.ds(HX, rows)
        for dy in (-1, 1):
            ys, yd = cut_y(dy, 1, reach, HY)
            moves.append((ODD, 0, dy, ref.at[own_x, ys], ref.at[own_x, yd]))
        return moves

    def species_moves():
        moves = []
        for by in (EVEN, ODD):
            for dx, dy in ((-1, 0), (1, 0), (0, -1), (0, 1)):
                if dx != 0:
                    src, dst = kinds.at[:, cells_x - 1 if dx > 0 else 0], rim_x.at[0 if dx > 0 else 1]
                else:
                    src, dst = kinds.at[:, :, cells_y - 1 if dy > 0 else 0], rim_y.at[0 if dy > 0 else 1]
                moves.append((by, dx, dy, src, dst))
        return moves

    back = [(ODD, -1, 0, pb.at[pl.ds(HX - 1, cells_x + 2)], given)]
    sides = [
        (ODD, -1, 0, rim_v.at[0], out_x.at[0]),
        (ODD, -1, 0, rim_v.at[1], out_x.at[cells_x + 1]),
        (ODD, -1, 0, rim_w.at[whole, 0], out_y.at[whole, HY - 1]),
        (ODD, -1, 0, rim_w.at[whole, 1], out_y.at[whole, HY + cells_y]),
    ]

    f_x, g_x, m_x = exchange(first), exchange(rest), exchange(coarse_moves(coarse_m))
    r_x = [exchange(coarse_moves(packed_r.at[at])) for at in range(CYCLES)]
    p_x = [exchange(press_moves(press.at[at], HX - at)) for at in range(CYCLES)]
    s_x, b_x, v_x = exchange(species_moves()), exchange(back), exchange(sides)
    every = (f_x, g_x, m_x, *r_x, *p_x, s_x, b_x, v_x)

    def grids(count):
        lane = lax.broadcasted_iota(jnp.int32, (count, cells_z), 1)
        row = lax.broadcasted_iota(jnp.int32, (count, cells_z), 0)
        return row, lane

    def next_z(v, k=1):
        return pltpu.roll(v, cells_z - k, 1)

    def prev_z(v, k=1):
        return pltpu.roll(v, k, 1)

    def next_y(v):
        return pltpu.roll(v, v.shape[0] - 1, 0)

    def prev_y(v):
        return pltpu.roll(v, 1, 0)

    def pack(two):
        lane = grids(two[0].shape[0])[1]
        return jnp.where(lane % 2 == 0, two[0] + next_z(two[0]), two[1] + prev_z(two[1]))

    inputs = [
        pltpu.make_async_copy(src, dst, in_sem.at[at])
        for at, (src, dst) in enumerate(
            ((velocity_in, velocity), (density_in, density), (source_in, source), (species, kinds))
        )
    ]
    for copy in inputs:
        copy.start()
    barrier = pltpu.get_barrier_semaphore()
    greet = {ODD: set(), EVEN: set()}
    for moves in (first, rest, species_moves(), back):
        for by, dx, dy, _, _ in moves:
            greet[by].add((dx, dy))
            greet[(by + dx) % 2].add((-dx, -dy))

    def enter(role):
        for dx, dy in sorted(greet[role], key=lambda d: (-abs(d[0]) - 2 * abs(d[1]), d)):
            @pl.when(there(dx, dy))
            def _():
                pl.semaphore_signal(barrier, inc=1, device_id=(slab + dx, cross + dy), device_id_type=MESH)

    def entered(role):
        count = jnp.int32(0)
        for dx, dy in sorted(greet[role]):
            count = count + there(dx, dy).astype(jnp.int32)
        return count

    @pl.when(jnp.logical_not(odd))
    def _():
        for ref in (rim_x, rim_y):
            ref[...] = jnp.zeros(ref.shape, f32)
        enter(EVEN)

    @pl.when(odd)
    def _():
        for ref in (near, later, edge_x, edge_y, coarse_m, packed_r, press, rim_x, rim_y):
            ref[...] = jnp.zeros(ref.shape, f32)
        enter(ODD)

    for copy in inputs[:3]:
        copy.wait()
    row_o, lane_o = grids(cells_y)
    for x in range(cells_x):
        v0, v1, v2 = velocity[0, x], velocity[1, x], velocity[2, x]
        dz = jnp.where(lane_o == cells_z - 1, 0.0, next_z(v2)) - jnp.where(lane_o == 0, 0.0, prev_z(v2))
        dy = jnp.where(row_o == cells_y - 1, 0.0, next_y(v1)) - jnp.where(row_o == 0, 0.0, prev_y(v1))
        t = dy + dz
        if x + 1 < cells_x:
            t = t + velocity[0, x + 1]
        if x > 0:
            t = t - velocity[0, x - 1]
        m = 1.0 / density[x]
        stage[0, x] = m
        stage[1, x] = 0.5 * t - source[x]
        fold[x] = m
        stage_y[x, pl.ds(1, 1)] = 0.5 * v1[0:1]
        stage_y[x, pl.ds(2, 1)] = 0.5 * v1[cells_y - 1 : cells_y]
        if x == 0:
            stage_x[0] = 0.5 * v0
        if x == cells_x - 1:
            stage_x[1] = 0.5 * v0

    def folded(x):
        return fold[x, pl.ds(0, half_y, stride=2)] + fold[x, pl.ds(1, half_y, stride=2)]

    mean = 0.125 * pack([folded(0) + folded(1), folded(2) + folded(3)])
    stage_c[...] = mean
    pl.semaphore_wait(barrier, jnp.where(odd, entered(ODD), entered(EVEN)))

    @pl.when(jnp.logical_not(odd))
    def _():
        f_x[0](EVEN)
        g_x[0](EVEN)
        inputs[3].wait()
        s_x[0](EVEN)
        b_x[1](EVEN)
        for x in range(cells_x):
            m = stage[0, x]
            p = given[1 + x, own_y]
            out_x[1 + x] = velocity[0, x] - m * (0.5 * (given[2 + x, own_y] - given[x, own_y]))
            grad = given[1 + x, pl.ds(HY + 1, cells_y)] - given[1 + x, pl.ds(HY - 1, cells_y)]
            out_y[x, own_y] = velocity[1, x] - m * (0.5 * grad)
            row_o, lane_o = grids(cells_y)
            dz = jnp.where(lane_o == cells_z - 1, 0.0, next_z(p)) - jnp.where(lane_o == 0, 0.0, prev_z(p))
            out_z[x] = velocity[2, x] - m * (0.5 * dz)
            out_p[x] = p
        v_x[1](EVEN)
        s_x[1](EVEN)
        for x in every:
            x[2](EVEN)

    @pl.when(odd)
    def _():
        f_x[0](ODD)
        g_x[0](ODD)
        row_w, lane_w = grids(wy)
        row_c, lane_c = grids(2 * half_y + half_y)
        even_c = lane_c % 2 == 0
        row_o, lane_o = grids(cells_y)
        mine = pl.ds(HX + cells_x, cells_x)
        near[0, mine, own_y] = stage[0]
        near[1, mine, own_y] = stage[1]
        edge_x[pl.ds(EDGES.index(cells_x), 2), own_y] = stage_x[...]
        edge_y[mine, pl.ds(1, 2)] = stage_y[:, pl.ds(1, 2)]
        coarse_m[OWN + 1, own_c] = stage_c[...]
        f_x[1](ODD)
        m_x[0](ODD)

        def fine_setup(span, full):
            def mob(x):
                return near[0, x] + later[0, x] if full else near[0, x]

            for x in span:
                m = mob(x)
                lo_x, hi_x = m + mob(x - 1), m + mob(x + 1)
                lo_y, hi_y = m + prev_y(m), m + next_y(m)
                lo_z = m + jnp.where(lane_w == 0, 0.0, prev_z(m))
                hi_z = m + jnp.where(lane_w == cells_z - 1, 0.0, next_z(m))
                diag = (lo_x + hi_x) + (lo_y + hi_y) + (lo_z + hi_z)
                inside = m > 0.0
                inv = jnp.where(inside, damping / jnp.where(inside, diag, 1.0), 0.0)
                xa[x], xb[x] = lo_x * inv, hi_x * inv
                ya[x], yb[x] = lo_y * inv, hi_y * inv
                za[x] = jnp.where(lane_w == 0, 0.0, lo_z * inv)
                zb[x] = jnp.where(lane_w == cells_z - 1, 0.0, hi_z * inv)
                t = near[1, x] + later[1, x] if full else near[1, x]
                at = x - HX
                if at in BELOW and (full or BELOW[at] not in (0, 7)):
                    t = t + edge_x[BELOW[at]]
                if at in ABOVE and (full or ABOVE[at] not in (0, 7)):
                    t = t - edge_x[ABOVE[at]]

                def side(j):
                    return jnp.broadcast_to(edge_y[x, pl.ds(j, 1)], t.shape)

                t = t + jnp.where(row_w == HY - 1, side(1), 0.0) - jnp.where(row_w == HY, side(0), 0.0)
                t = t + jnp.where(row_w == HY + cells_y - 1, side(3), 0.0)
                t = t - jnp.where(row_w == HY + cells_y, side(2), 0.0)
                b = t * (inv + inv)
                goal[x] = b
                if not full:
                    pa[x] = -b
                    if HX <= x < HX + rows:
                        scale_back[x - HX] = (diag * (0.5 / damping))[HY : HY + cells_y]

        fine_setup(range(HX - 2, HX + rows + 2), False)

        def sweep(src, dst, low, high):
            for x in range(low, high):
                v = src[x]
                t = xa[x] * src[x - 1] + xb[x] * src[x + 1]
                t = t + (ya[x] * prev_y(v) + yb[x] * next_y(v))
                t = t + (za[x] * prev_z(v) + zb[x] * next_z(v))
                dst[x] = (1.0 - damping) * v + (t - goal[x])

        def beside(ref, low, high):
            up = {b: next_z(ref[b]) for b in range(max(low - 1, 0), high)}
            down = {b: prev_z(ref[b]) for b in range(low, min(high + 1, blocks))}
            for b in range(low, high):
                yield b, jnp.where(even_c, up[max(b - 1, 0)], down[b]), jnp.where(even_c, up[b], down[min(b + 1, blocks - 1)])

        def coarse_setup():
            for b, lo, hi in beside(coarse_m, 0, blocks):
                m = coarse_m[b]
                if b == 0:
                    lo = jnp.where(even_c, 0.0, lo)
                if b == blocks - 1:
                    hi = jnp.where(even_c, hi, 0.0)
                lo_x, hi_x = m + lo, m + hi
                lo_y, hi_y = m + prev_y(m), m + next_y(m)
                lo_z = m + jnp.where(lane_c < 2, 0.0, prev_z(m, 2))
                hi_z = m + jnp.where(lane_c >= cells_z - 2, 0.0, next_z(m, 2))
                diag = (lo_x + hi_x) + (lo_y + hi_y) + (lo_z + hi_z)
                inside = m > 0.0
                inv = jnp.where(inside, damping / jnp.where(inside, diag, 1.0), 0.0)
                cxa[b], cxb[b] = lo_x * inv, hi_x * inv
                cya[b], cyb[b] = lo_y * inv, hi_y * inv
                cza[b] = jnp.where(lane_c < 2, 0.0, lo_z * inv)
                czb[b] = jnp.where(lane_c >= cells_z - 2, 0.0, hi_z * inv)
                cinv[b] = inv

        def coarse_sweep(src, dst, low, high):
            for b, lo, hi in beside(src, low, high):
                v = src[b]
                t = cxa[b] * lo + cxb[b] * hi
                t = t + (cya[b] * prev_y(v) + cyb[b] * next_y(v))
                t = t + (cza[b] * prev_z(v, 2) + czb[b] * next_z(v, 2))
                dst[b] = (1.0 - damping) * v + (t - right[b])

        def correct(at, pre, free, reach):
            press[at, pl.ds(HX, rows), own_y] = pre[pl.ds(HX, rows), own_y]
            for x in range(HX, HX + rows, 2):
                total = None
                for w in (x, x + 1):
                    v = pre[w]
                    t = xa[w] * pre[w - 1] + xb[w] * pre[w + 1]
                    t = t + (ya[w] * prev_y(v) + yb[w] * next_y(v))
                    t = t + (za[w] * prev_z(v) + zb[w] * next_z(v))
                    d = (damping * v - (t - goal[w]))[HY : HY + cells_y] * scale_back[w - HX]
                    total = d if total is None else total + d
                fold[(x - HX) // 2] = total
            for b in range(2):
                packed_r[at, OWN + b, own_c] = pack([folded(2 * b), folded(2 * b + 1)])
            r_x[at][0](ODD)
            p_x[at][0](ODD)
            if at == 0:
                inputs[3].wait()
                s_x[0](ODD)
                g_x[1](ODD)
                fine_setup(range(1, wx - 1), True)
                m_x[1](ODD)
                coarse_setup()
            r_x[at][1](ODD)
            for b in range(blocks):
                r = packed_r[at, b] * cinv[b]
                right[b] = r
                ca[b] = -r
            coarse_sweep(ca, cb, 0, blocks)
            coarse_sweep(cb, ca, 1, blocks - 1)
            coarse_sweep(ca, cb, 1, blocks - 1)
            margin = half_y - HY // 2
            for q in range(-3, rows // 2 + 3):
                v = cb[OWN + q // 2]
                v = jnp.where(even_c, v, prev_z(v)) if q % 2 == 0 else jnp.where(even_c, next_z(v), v)
                v = v[margin : margin + wy // 2]
                spread[q + 3, pl.ds(0, wy // 2, stride=2)] = v
                spread[q + 3, pl.ds(1, wy // 2, stride=2)] = v
            p_x[at][1](ODD)
            low, high = HX - reach - 2, HX + rows + reach + 2
            for x in range(low, high):
                pre[x] = press[at, x] + spread[(x - HX) // 2 + 3]
            sweep(pre, free, low + 1, high - 1)
            sweep(free, pre, low + 2, high - 2)

        sweep(pa, pb, HX - 1, HX + rows + 1)
        correct(0, pb, pa, 3)
        sweep(pb, pa, HX - 2, HX + rows + 2)
        sweep(pa, pb, HX - 1, HX + rows + 1)
        correct(1, pb, pa, 2)
        last = pb
        b_x[0](ODD)

        def along_x(x):
            return near[0, x, own_y] * (0.5 * (last[x + 1, own_y] - last[x - 1, own_y]))

        def along_y(x, y):
            one = pl.ds(y, 1)
            return near[0, x, one] * (0.5 * (last[x, pl.ds(y + 1, 1)] - last[x, pl.ds(y - 1, 1)]))

        def edge(at):
            v = edge_x[EDGES.index(at), own_y]
            return (v + v) - along_x(HX + at)

        def ends(x):
            lo, hi = edge_y[x, pl.ds(0, 1)], edge_y[x, pl.ds(3, 1)]
            return (lo + lo) - along_y(x, HY - 1), (hi + hi) - along_y(x, HY + cells_y)

        rim_v[0] = edge(-1)
        rim_v[1] = edge(cells_x)
        for x in range(cells_x):
            lo, hi = ends(HX + x)
            rim_w[x, pl.ds(0, 1)] = lo
            rim_w[x, pl.ds(1, 1)] = hi
        v_x[0](ODD)
        out_x[0] = edge(cells_x - 1)
        out_x[cells_x + 1] = edge(rows)
        for x in range(cells_x):
            w = HX + cells_x + x
            m = near[0, w, own_y]
            p = last[w, own_y]
            out_x[1 + x] = velocity[0, x] - along_x(w)
            grad = last[w, pl.ds(HY + 1, cells_y)] - last[w, pl.ds(HY - 1, cells_y)]
            out_y[x, own_y] = velocity[1, x] - m * (0.5 * grad)
            lo, hi = ends(w)
            out_y[x, pl.ds(HY - 1, 1)] = lo
            out_y[x, pl.ds(HY + cells_y, 1)] = hi
            dz = jnp.where(lane_o == cells_z - 1, 0.0, next_z(p)) - jnp.where(lane_o == 0, 0.0, prev_z(p))
            out_z[x] = velocity[2, x] - m * (0.5 * dz)
            out_p[x] = p
        s_x[1](ODD)
        for x in every:
            x[2](ODD)

    assert groups == MOVES, groups


MOVES = [34, 18, 14, 14, 14, 8, 8, 8, 1, 4]


def transport(in_x, in_y, in_z, in_p, rim_x, rim_y, species, vel_out, pres_out, spec_out):
    cells_x, cells_y, cells_z = in_p.shape
    lane_o = lax.broadcasted_iota(jnp.int32, (cells_y, cells_z), 1)
    row_o = lax.broadcasted_iota(jnp.int32, (cells_y, cells_z), 0)

    def next_z(v):
        return pltpu.roll(v, cells_z - 1, 1)

    def prev_z(v):
        return pltpu.roll(v, 1, 1)

    def next_y(v):
        return pltpu.roll(v, v.shape[0] - 1, 0)

    def prev_y(v):
        return pltpu.roll(v, 1, 0)

    mid = slice(HY, HY + cells_y)
    pres_out[...] = in_p[...]
    move_x = [in_x[x] for x in range(cells_x + 2)]
    for x in range(cells_x):
        move_y, move_z = in_y[x], in_z[x]
        vel_out[0, x] = move_x[x + 1]
        vel_out[1, x] = move_y[mid]
        vel_out[2, x] = move_z
        lo_x, hi_x = 0.5 * (move_x[x] + move_x[x + 1]), 0.5 * (move_x[x + 1] + move_x[x + 2])
        lo_y, hi_y = (0.5 * (move_y + prev_y(move_y)))[mid], (0.5 * (move_y + next_y(move_y)))[mid]
        lo_z = 0.5 * (move_z + jnp.where(lane_o == 0, 0.0, prev_z(move_z)))
        hi_z = 0.5 * (move_z + jnp.where(lane_o == cells_z - 1, 0.0, next_z(move_z)))

        def into(flow):
            return time_step * jnp.maximum(flow, 0.0)

        def back(flow):
            return -time_step * jnp.minimum(flow, 0.0)

        keep = 1.0 - (into(hi_x) + into(hi_y) + into(hi_z)) - (back(lo_x) + back(lo_y) + back(lo_z))
        from_xl, from_xu = into(lo_x), back(hi_x)
        from_yl, from_yu = into(lo_y), back(hi_y)
        from_zl = jnp.where(lane_o == 0, 0.0, into(lo_z))
        from_zu = jnp.where(lane_o == cells_z - 1, 0.0, back(hi_z))
        for s in range(species.shape[0]):
            q = species[s, x]
            xl = rim_x[0, s] if x == 0 else species[s, x - 1]
            xu = rim_x[1, s] if x == cells_x - 1 else species[s, x + 1]
            yl = jnp.where(row_o == 0, rim_y[0, s, pl.ds(x, 1)], prev_y(q))
            yu = jnp.where(row_o == cells_y - 1, rim_y[1, s, pl.ds(x, 1)], next_y(q))
            total = keep * q + (from_xl * xl + from_xu * xu) + (from_yl * yl + from_yu * yu)
            spec_out[s, x] = total + (from_zl * prev_z(q) + from_zu * next_z(q))


def local(slabs, crosses, velocity, density, source, species):
    cells_x, cells_y, cells_z = density.shape
    assert cells_x == 4 and cells_y == 2 * HY and slabs % 2 == 0
    rows = 2 * cells_x
    wx, wy = rows + 2 * HX, cells_y + 2 * HY
    half_y = cells_y // 2
    kinds = species.shape[0]
    f32 = jnp.float32

    def vmem(*shape):
        return pltpu.VMEM(shape, f32)

    blocks = 2 * OWN + 2
    fine, coarse = (wx, wy, cells_z), (blocks, 3 * half_y, cells_z)
    dma = pltpu.SemaphoreType.DMA
    spec = pl.BlockSpec(memory_space=pltpu.VMEM)
    far = pl.BlockSpec(memory_space=pltpu.HBM)
    moved = [
        (cells_x + 2, cells_y, cells_z), (cells_x, wy, cells_z), density.shape, density.shape,
        (2, kinds, cells_y, cells_z), (2, kinds, cells_x, cells_z), species.shape,
    ]
    between = pl.pallas_call(
        functools.partial(kernel, slabs, crosses),
        out_shape=tuple(pltpu.VMEM(shape, f32) for shape in moved),
        in_specs=[far] * 4,
        out_specs=(spec,) * 7,
        scratch_shapes=[vmem(*velocity.shape), vmem(*density.shape), vmem(*density.shape)]
        + [vmem(2, *density.shape), vmem(2, cells_y, cells_z), vmem(cells_x, 8, cells_z), vmem(half_y, cells_z)]
        + [vmem(2, *fine)] * 2 + [vmem(len(EDGES), wy, cells_z), vmem(wx, 8, cells_z)]
        + [vmem(CYCLES, *fine), vmem(*coarse), vmem(CYCLES, *coarse), vmem(cells_x + 2, wy, cells_z)]
        + [vmem(*fine)] * 7 + [vmem(rows, cells_y, cells_z)] + [vmem(*fine)] * 2
        + [vmem(*coarse)] * 10 + [vmem(cells_x, cells_y, cells_z), vmem(rows // 2 + 6, wy, cells_z)]
        + [vmem(2, cells_y, cells_z), vmem(cells_x, 8, cells_z)]
        + [dma((4,))] + [dma((n,)) for n in MOVES for _ in range(2)],
        compiler_params=pltpu.CompilerParams(
            collective_id=0, has_side_effects=True, vmem_limit_bytes=16 << 20
        ),
        name="projection",
    )(*(pltpu.with_memory_space_constraint(a, pltpu.HBM) for a in (velocity, density, source, species)))
    return pl.pallas_call(
        transport,
        out_shape=tuple(jax.ShapeDtypeStruct(a.shape, f32) for a in (velocity, density, species)),
        in_specs=[spec] * 7,
        out_specs=(spec,) * 3,
        compiler_params=pltpu.CompilerParams(vmem_limit_bytes=8 << 20),
        name="transport",
    )(*between)


def solution(mesh):
    plane, stack = P("slab", "cross", None), P(None, "slab", "cross", None)
    return jax.shard_map(
        functools.partial(local, mesh.shape["slab"], mesh.shape["cross"]),
        mesh=mesh,
        in_specs=(stack, plane, plane, stack),
        out_specs=(stack, plane, stack),
        check_vma=False,
    )
```

```python
import functools

import jax
import jax.numpy as jnp
from jax import lax
from jax.experimental import pallas as pl
from jax.experimental.pallas import tpu as pltpu
from jax.sharding import PartitionSpec as P

CYCLES = 2
COARSE = 4
damping = 0.8
time_step = 0.25
MESH = pl.DeviceIdType.MESH
HX = 5
HY = 4
EVEN, ODD = 0, 1
OWN = 3

EDGES = (-5, -1, 0, 3, 4, 7, 8, 12)
BELOW = {-1: 2, 3: 4, 7: 6, 11: 7}
ABOVE = {-4: 0, 0: 1, 4: 3, 8: 5}


def kernel(
    slabs, crosses, velocity_in, density_in, source_in, species,
    out_x, out_y, out_z, out_p, rim_x, rim_y, kinds,
    velocity, density, source, stage, stage_x, stage_y, stage_c,
    near, later, fifth_m, edge_x, edge_y, press, fifth_p, coarse_m, packed_r, given,
    xa, xb, ya, yb, za, zb, goal, scale_back, pa, pb,
    cxa, cxb, cya, cyb, cza, czb, cinv, right, ca, cb, fold, spread, rim_v, rim_w, in_sem, *sems,
):
    cells_x, cells_y, cells_z = density.shape
    rows = 2 * cells_x
    wx, wy = rows + 2 * HX, cells_y + 2 * HY
    half_y = cells_y // 2
    blocks = packed_r.shape[1]
    own_y = pl.ds(0, cells_y)
    own_c = pl.ds(half_y, half_y)
    slab, cross = lax.axis_index("slab"), lax.axis_index("cross")
    odd = slab % 2 == 1
    f32 = jnp.float32

    def there(dx, dy):
        return (slab + dx >= 0) & (slab + dx < slabs) & (cross + dy >= 0) & (cross + dy < crosses)

    groups = []

    def exchange(moves):
        at = len(groups)
        send, recv = sems[2 * at], sems[2 * at + 1]
        groups.append(len(moves))

        def copy(index):
            _, dx, dy, src, dst = moves[index]
            return pltpu.make_async_remote_copy(
                src_ref=src, dst_ref=dst, send_sem=send.at[index], recv_sem=recv.at[index],
                device_id=(slab + dx, cross + dy), device_id_type=MESH,
            )

        def each(role, sender, act, only=None):
            for index, (by, dx, dy, _, _) in enumerate(moves):
                if only is not None and ((dx, dy) == (1, 0)) != only:
                    continue
                if sender and by == role:
                    @pl.when(there(dx, dy))
                    def _():
                        act(copy(index))
                if not sender and (by + dx) % 2 == role:
                    @pl.when(there(-dx, -dy))
                    def _():
                        act(copy(index))

        def start(role):
            each(role, True, lambda c: c.start())

        def arrive(role, only=None):
            each(role, False, lambda c: c.wait_recv(), only)

        def leave(role):
            each(role, True, lambda c: c.wait_send())

        return start, arrive, leave

    def cut_y(dy, low, high, home=0, span=cells_y, rim=wy, behind=cells_y):
        depth = high - low + 1
        if dy > 0:
            return pl.ds(home + span - high, depth), pl.ds(rim - high, depth)
        return pl.ds(home + low - 1, depth), pl.ds(behind + low - 1, depth)

    def fifth(dy):
        return (cells_y - 5, 3) if dy > 0 else (4, 4)

    whole = slice(None)
    first, rest = [], []
    for by, base, out in ((EVEN, 0, -1), (ODD, cells_x, 2)):
        to = 1 - by
        lo_edge, hi_edge = EDGES.index(base), EDGES.index(base + cells_x - 1)
        at = rows if by == EVEN else -cells_x
        touch = 0 if by == EVEN else cells_x - 1
        edge = EDGES.index(at + touch)

        def seen(deep, count, at=at, by=by):
            start = deep - 1 if by == EVEN else cells_x - deep - count + 1
            return pl.ds(start, count), pl.ds(HX + at + start, count)

        for dy in (-1, 1):
            j, k = (2, 0) if dy > 0 else (1, 3)
            src, dst = seen(1, 2)
            ys, yd = cut_y(dy, 1, 2)
            first.append((by, out, dy, stage.at[whole, src, ys], near.at[whole, dst, yd]))
            ys, yd = cut_y(dy, 1, 4)
            first.append((by, out, dy, stage_x.at[min(touch, 1), ys], edge_x.at[edge, yd]))
            first.append((by, out, dy, stage_y.at[whole, j], edge_y.at[pl.ds(HX + at, cells_x), k]))
        src, dst = seen(1, 3)
        first.append((by, out, 0, stage.at[whole, src], near.at[whole, dst, own_y]))
        first.append((by, out, 0, stage_x.at[min(touch, 1)], edge_x.at[edge, own_y]))
        first.append((by, out, 0, stage_y.at[whole, pl.ds(1, 2)], edge_y.at[pl.ds(HX + at, cells_x), pl.ds(1, 2)]))
        mine = pl.ds(HX + base, cells_x)
        for dy in (-1, 1):
            j, k = (2, 0) if dy > 0 else (1, 3)
            ys, yd = cut_y(dy, 1, 3)
            first.append((by, to, dy, stage.at[whole, whole, ys], near.at[whole, mine, yd]))
            ys, yd = cut_y(dy, 1, 4)
            first.append((by, to, dy, stage_x.at[whole, ys], edge_x.at[pl.ds(lo_edge, 2), yd]))
            first.append((by, to, dy, stage_y.at[whole, j], edge_y.at[mine, k]))
        if by == EVEN:
            first.append((by, 1, 0, stage, near.at[whole, mine, own_y]))
            first.append((by, 1, 0, stage_x, edge_x.at[pl.ds(lo_edge, 2), own_y]))
            first.append((by, 1, 0, stage_y.at[whole, pl.ds(1, 2)], edge_y.at[mine, pl.ds(1, 2)]))
            first.append((by, 1, 0, stage_c, coarse_m.at[OWN + 1, own_c]))

        for dy in (-1, 1):
            for deep, low, high in ((1, 3, 4), (3, 1, 2)):
                src, dst = seen(deep, 2)
                ys, yd = cut_y(dy, low, high)
                rest.append((by, out, dy, stage.at[whole, src, ys], later.at[whole, dst, yd]))
        src, dst = seen(4, 1)
        rest.append((by, out, 0, stage.at[whole, src], later.at[whole, dst, own_y]))
        far, row, lands = (3, cells_x - 1, -HX) if by == EVEN else (-2, 0, rows + HX - 1)
        rest.append((by, far, 0, stage.at[0, row], later.at[0, HX + lands, own_y]))
        rest.append((by, far, 0, stage_x.at[min(row, 1)], edge_x.at[EDGES.index(lands), own_y]))
        for dy in (-1, 1):
            ys, yd = cut_y(dy, 4, 4)
            rest.append((by, to, dy, stage.at[whole, whole, ys], later.at[whole, mine, yd]))
            y, j = fifth(dy)
            rest.append((by, to, dy, stage.at[0, whole, y], fifth_m.at[pl.ds(base, cells_x), j]))

    def coarse_moves(ref, own, reach):
        moves = []
        ahead, behind, aside = (2, own, own - 2, 2, reach - 1), (-2, own, own + 2, 2, reach - 1), (0, own, own, 2, reach)
        count = (reach - 3) // 2
        ahead_far, behind_far = (4, own + 2 - count, own - 2 - count, count, reach - 5), (-4, own, own + 4, count, reach - 5)
        for dy, kinds_of in (
            (-1, (ahead, behind)), (1, (ahead, behind)), (0, (ahead, behind)),
            (-1, (ahead_far, behind_far)), (1, (ahead_far, behind_far)), (0, (ahead_far, behind_far)), (-1, (aside,)), (1, (aside,)),
        ):
            for dx, src, dst, count, deep in kinds_of:
                ys, yd = (own_c, own_c) if dy == 0 else cut_y(dy, 1, deep, half_y, half_y, half_y, 2 * half_y)
                moves.append((ODD, dx, dy, ref.at[pl.ds(src, count), ys], ref.at[pl.ds(dst, count), yd]))
        return moves

    def press_moves(ref, reach):
        moves = []
        low, high = (pl.ds(HX, reach), pl.ds(HX + rows, reach)), (pl.ds(HX + rows - reach, reach), pl.ds(HX - reach, reach))
        corner = reach - 1
        low_c, high_c = (pl.ds(HX, corner), pl.ds(HX + rows, corner)), (pl.ds(HX + rows - corner, corner), pl.ds(HX - corner, corner))
        for dy in (-1, 1):
            ys, yd = cut_y(dy, 1, corner)
            moves.append((ODD, 2, dy, ref.at[high_c[0], ys], ref.at[high_c[1], yd]))
            moves.append((ODD, -2, dy, ref.at[low_c[0], ys], ref.at[low_c[1], yd]))
        moves.append((ODD, 2, 0, ref.at[high[0], own_y], ref.at[high[1], own_y]))
        moves.append((ODD, -2, 0, ref.at[low[0], own_y], ref.at[low[1], own_y]))
        own_x = pl.ds(HX, rows)
        for dy in (-1, 1):
            ys, yd = cut_y(dy, 1, HY)
            moves.append((ODD, 0, dy, ref.at[own_x, ys], ref.at[own_x, yd]))
            if reach > HY:
                y, j = fifth(dy)
                moves.append((ODD, 0, dy, ref.at[own_x, y], fifth_p.at[:, j]))
        return moves

    def species_moves():
        moves = []
        for by in (EVEN, ODD):
            for dx, dy in ((-1, 0), (1, 0), (0, -1), (0, 1)):
                if dx != 0:
                    src, dst = kinds.at[:, cells_x - 1 if dx > 0 else 0], rim_x.at[0 if dx > 0 else 1]
                else:
                    src, dst = kinds.at[:, :, cells_y - 1 if dy > 0 else 0], rim_y.at[0 if dy > 0 else 1]
                moves.append((by, dx, dy, src, dst))
        return moves

    back = [(ODD, -1, 0, pb.at[pl.ds(HX - 1, cells_x + 2)], given)]
    sides = [
        (ODD, -1, 0, rim_v.at[0], out_x.at[0]),
        (ODD, -1, 0, rim_v.at[1], out_x.at[cells_x + 1]),
        (ODD, -1, 0, rim_w.at[whole, 0], out_y.at[whole, wy - 1]),
        (ODD, -1, 0, rim_w.at[whole, 1], out_y.at[whole, cells_y]),
    ]

    f_x, g_x, m_x = exchange(first), exchange(rest), exchange(coarse_moves(coarse_m, OWN + 1, 7))
    r_x = [exchange(coarse_moves(packed_r.at[at], OWN, 6)) for at in range(CYCLES)]
    p_x = [exchange(press_moves(press.at[at], HX - at)) for at in range(CYCLES)]
    s_x, b_x, v_x = exchange(species_moves()), exchange(back), exchange(sides)
    every = (f_x, g_x, m_x, *r_x, *p_x, s_x, b_x, v_x)

    def grids(count):
        lane = lax.broadcasted_iota(jnp.int32, (count, cells_z), 1)
        row = lax.broadcasted_iota(jnp.int32, (count, cells_z), 0)
        return row, lane

    def next_z(v, k=1):
        return pltpu.roll(v, cells_z - k, 1)

    def prev_z(v, k=1):
        return pltpu.roll(v, k, 1)

    def next_y(v):
        return pltpu.roll(v, v.shape[0] - 1, 0)

    def prev_y(v):
        return pltpu.roll(v, 1, 0)

    def pack(two):
        lane = grids(two[0].shape[0])[1]
        return jnp.where(lane % 2 == 0, two[0] + next_z(two[0]), two[1] + prev_z(two[1]))

    inputs = [
        pltpu.make_async_copy(src, dst, in_sem.at[at])
        for at, (src, dst) in enumerate(
            ((velocity_in, velocity), (density_in, density), (source_in, source), (species, kinds))
        )
    ]
    for copy in inputs:
        copy.start()
    barrier = pltpu.get_barrier_semaphore()
    greet = {ODD: set(), EVEN: set()}
    for moves in (first, rest, coarse_moves(coarse_m, OWN + 1, 7), species_moves(), back):
        for by, dx, dy, _, _ in moves:
            greet[by].add((dx, dy))
            greet[(by + dx) % 2].add((-dx, -dy))

    def enter(role):
        for dx, dy in sorted(greet[role], key=lambda d: (-abs(d[0]) - 2 * abs(d[1]), d)):
            @pl.when(there(dx, dy))
            def _():
                pl.semaphore_signal(barrier, inc=1, device_id=(slab + dx, cross + dy), device_id_type=MESH)

    def entered(role):
        count = jnp.int32(0)
        for dx, dy in sorted(greet[role]):
            count = count + there(dx, dy).astype(jnp.int32)
        return count

    @pl.when(jnp.logical_not(odd))
    def _():
        for ref in (rim_x, rim_y):
            ref[...] = jnp.zeros(ref.shape, f32)
        enter(EVEN)

    @pl.when(odd)
    def _():
        for ref in (near, later, fifth_m, edge_x, edge_y, coarse_m, packed_r, press, fifth_p, rim_x, rim_y):
            ref[...] = jnp.zeros(ref.shape, f32)
        enter(ODD)

    for copy in inputs[:3]:
        copy.wait()
    row_o, lane_o = grids(cells_y)
    for x in range(cells_x):
        v0, v1, v2 = velocity[0, x], velocity[1, x], velocity[2, x]
        dz = jnp.where(lane_o == cells_z - 1, 0.0, next_z(v2)) - jnp.where(lane_o == 0, 0.0, prev_z(v2))
        dy = jnp.where(row_o == cells_y - 1, 0.0, next_y(v1)) - jnp.where(row_o == 0, 0.0, prev_y(v1))
        t = dy + dz
        if x + 1 < cells_x:
            t = t + velocity[0, x + 1]
        if x > 0:
            t = t - velocity[0, x - 1]
        m = 1.0 / density[x]
        stage[0, x] = m
        stage[1, x] = 0.5 * t - source[x]
        fold[x] = m
        stage_y[x, pl.ds(1, 1)] = 0.5 * v1[0:1]
        stage_y[x, pl.ds(2, 1)] = 0.5 * v1[cells_y - 1 : cells_y]
        if x == 0:
            stage_x[0] = 0.5 * v0
        if x == cells_x - 1:
            stage_x[1] = 0.5 * v0

    def folded(x):
        return fold[x, pl.ds(0, half_y, stride=2)] + fold[x, pl.ds(1, half_y, stride=2)]

    mean = 0.125 * pack([folded(0) + folded(1), folded(2) + folded(3)])
    stage_c[...] = mean
    pl.semaphore_wait(barrier, jnp.where(odd, entered(ODD), entered(EVEN)))

    @pl.when(jnp.logical_not(odd))
    def _():
        f_x[0](EVEN)
        f_x[2](EVEN)
        g_x[0](EVEN)
        inputs[3].wait()
        s_x[0](EVEN)
        b_x[1](EVEN)
        for x in range(cells_x):
            m = stage[0, x]
            p = given[1 + x, own_y]
            out_x[1 + x] = velocity[0, x] - m * (0.5 * (given[2 + x, own_y] - given[x, own_y]))
            v = given[1 + x]
            out_y[x, own_y] = velocity[1, x] - m * (0.5 * (next_y(v) - prev_y(v))[:cells_y])
            row_o, lane_o = grids(cells_y)
            dz = jnp.where(lane_o == cells_z - 1, 0.0, next_z(p)) - jnp.where(lane_o == 0, 0.0, prev_z(p))
            out_z[x] = velocity[2, x] - m * (0.5 * dz)
            out_p[x] = p
        v_x[1](EVEN)
        s_x[1](EVEN)
        for x in every[1:]:
            x[2](EVEN)

    @pl.when(odd)
    def _():
        f_x[0](ODD)
        f_x[2](ODD)
        row_w, lane_w = grids(wy)
        row_c, lane_c = grids(2 * half_y + half_y)
        even_c = lane_c % 2 == 0
        row_o, lane_o = grids(cells_y)
        mine = pl.ds(HX + cells_x, cells_x)
        near[0, mine, own_y] = stage[0]
        near[1, mine, own_y] = stage[1]
        edge_x[pl.ds(EDGES.index(cells_x), 2), own_y] = stage_x[...]
        edge_y[mine, pl.ds(1, 2)] = stage_y[:, pl.ds(1, 2)]
        coarse_m[OWN + 2, own_c] = stage_c[...]
        f_x[1](ODD, True)
        m_x[0](ODD)
        g_x[0](ODD)
        f_x[1](ODD, False)

        middle = grids(8)[0]

        def around_y(v, more=None):
            if more is None:
                return prev_y(v), next_y(v)
            own, rim = v[:cells_y], v[cells_y:]
            return (
                prev_y(jnp.concatenate([own, jnp.where(middle == 3, more, rim)], 0)),
                next_y(jnp.concatenate([own, jnp.where(middle == 4, more, rim)], 0)),
            )

        def fine_setup(span, full):
            def mob(x):
                return near[0, x] + later[0, x] if full else near[0, x]

            for x in span:
                m = mob(x)
                lo_x, hi_x = m + mob(x - 1), m + mob(x + 1)
                before, behind = around_y(m, fifth_m[x - HX] if full and HX <= x < HX + rows else None)
                lo_y, hi_y = m + before, m + behind
                lo_z = m + jnp.where(lane_w == 0, 0.0, prev_z(m))
                hi_z = m + jnp.where(lane_w == cells_z - 1, 0.0, next_z(m))
                diag = (lo_x + hi_x) + (lo_y + hi_y) + (lo_z + hi_z)
                inside = m > 0.0
                inv = jnp.where(inside, damping / jnp.where(inside, diag, 1.0), 0.0)
                xa[x], xb[x] = lo_x * inv, hi_x * inv
                ya[x], yb[x] = lo_y * inv, hi_y * inv
                za[x] = jnp.where(lane_w == 0, 0.0, lo_z * inv)
                zb[x] = jnp.where(lane_w == cells_z - 1, 0.0, hi_z * inv)
                t = near[1, x] + later[1, x] if full else near[1, x]
                at = x - HX
                if at in BELOW and (full or BELOW[at] not in (0, 7)):
                    t = t + edge_x[BELOW[at]]
                if at in ABOVE and (full or ABOVE[at] not in (0, 7)):
                    t = t - edge_x[ABOVE[at]]

                def side(j):
                    return jnp.broadcast_to(edge_y[x, pl.ds(j, 1)], t.shape)

                t = t + jnp.where(row_w == wy - 1, side(1), 0.0) - jnp.where(row_w == 0, side(0), 0.0)
                t = t + jnp.where(row_w == cells_y - 1, side(3), 0.0)
                t = t - jnp.where(row_w == cells_y, side(2), 0.0)
                b = t * (inv + inv)
                goal[x] = b
                if not full:
                    pa[x] = -b
                    if HX <= x < HX + rows:
                        scale_back[x - HX] = (diag * (0.5 / damping))[:cells_y]

        fine_setup(range(HX - 2, HX + rows + 2), False)

        def sweep(src, dst, low, high, deep=False):
            for x in range(low, high):
                v = src[x]
                before, behind = around_y(v, fifth_p[x - HX] if deep and HX <= x < HX + rows else None)
                t = xa[x] * src[x - 1] + xb[x] * src[x + 1]
                t = t + (ya[x] * before + yb[x] * behind)
                t = t + (za[x] * prev_z(v) + zb[x] * next_z(v))
                dst[x] = (1.0 - damping) * v + (t - goal[x])

        def beside(ref, low, high, last):
            up = {b: next_z(ref[b]) for b in range(max(low - 1, 0), high)}
            down = {b: prev_z(ref[b]) for b in range(low, min(high + 1, last))}
            for b in range(low, high):
                yield b, jnp.where(even_c, up[max(b - 1, 0)], down[b]), jnp.where(even_c, up[b], down[min(b + 1, last - 1)])

        def coarse_setup():
            for c, lo, hi in beside(coarse_m, 1, blocks + 1, blocks + 2):
                m, b = coarse_m[c], c - 1
                lo_x, hi_x = m + lo, m + hi
                lo_y, hi_y = m + prev_y(m), m + next_y(m)
                lo_z = m + jnp.where(lane_c < 2, 0.0, prev_z(m, 2))
                hi_z = m + jnp.where(lane_c >= cells_z - 2, 0.0, next_z(m, 2))
                diag = (lo_x + hi_x) + (lo_y + hi_y) + (lo_z + hi_z)
                inside = m > 0.0
                inv = jnp.where(inside, damping / jnp.where(inside, diag, 1.0), 0.0)
                cxa[b], cxb[b] = lo_x * inv, hi_x * inv
                cya[b], cyb[b] = lo_y * inv, hi_y * inv
                cza[b] = jnp.where(lane_c < 2, 0.0, lo_z * inv)
                czb[b] = jnp.where(lane_c >= cells_z - 2, 0.0, hi_z * inv)
                cinv[b] = inv

        def coarse_sweep(src, dst, low, high):
            for b, lo, hi in beside(src, low, high, blocks):
                v = src[b]
                t = cxa[b] * lo + cxb[b] * hi
                t = t + (cya[b] * prev_y(v) + cyb[b] * next_y(v))
                t = t + (cza[b] * prev_z(v, 2) + czb[b] * next_z(v, 2))
                dst[b] = (1.0 - damping) * v + (t - right[b])

        def correct(at, pre, free, reach, parts):
            press[at, pl.ds(HX, rows), own_y] = pre[pl.ds(HX, rows), own_y]
            for x in range(HX, HX + rows, 2):
                total = None
                for w in (x, x + 1):
                    v = pre[w]
                    t = xa[w] * pre[w - 1] + xb[w] * pre[w + 1]
                    t = t + (ya[w] * prev_y(v) + yb[w] * next_y(v))
                    t = t + (za[w] * prev_z(v) + zb[w] * next_z(v))
                    d = (damping * v - (t - goal[w]))[:cells_y] * scale_back[w - HX]
                    total = d if total is None else total + d
                fold[(x - HX) // 2] = total
            for b in range(2):
                packed_r[at, OWN + b, own_c] = pack([folded(2 * b), folded(2 * b + 1)])
            r_x[at][0](ODD)
            p_x[at][0](ODD)
            if at == 0:
                inputs[3].wait()
                s_x[0](ODD)
                g_x[1](ODD)
                fine_setup(range(1, wx - 1), True)
                m_x[1](ODD)
                coarse_setup()
            r_x[at][1](ODD)
            for b in range(blocks):
                r = packed_r[at, b] * cinv[b]
                right[b] = r
                ca[b] = -r
            coarse_sweep(ca, cb, 0, blocks)
            coarse_sweep(cb, ca, 1, blocks - 1)
            coarse_sweep(ca, cb, 1, blocks - 1)
            margin, tall = half_y - half_y // 2, 2 * cells_y
            for q in range(-3, rows // 2 + 3):
                v = cb[OWN + q // 2]
                v = jnp.where(even_c, v, prev_z(v)) if q % 2 == 0 else jnp.where(even_c, next_z(v), v)
                v = v[margin : margin + cells_y]
                spread[q + 3, pl.ds(0, tall // 2, stride=2)] = v
                spread[q + 3, pl.ds(1, tall // 2, stride=2)] = v
            p_x[at][1](ODD)
            low, high = HX - reach, HX + rows + reach
            done = [low - 2, low - 1, low]
            for end in parts:
                tops = [min(HX + end + 2, high + 2), min(HX + end + 1, high + 1), min(HX + end, high)]
                for x in range(done[0], tops[0]):
                    up = spread.at[(x - HX) // 2 + 3]
                    ahead, after = up[pl.ds(0, 8)], up[pl.ds(8 + cells_y, 8)]
                    pre[x, own_y] = press[at, x, own_y] + up[pl.ds(8, cells_y)]
                    pre[x, pl.ds(cells_y, 8)] = press[at, x, pl.ds(cells_y, 8)] + jnp.where(middle < HY, after, ahead)
                    if at == 0 and HX <= x < HX + rows:
                        fifth_p[x - HX] = fifth_p[x - HX] + jnp.where(middle < HY, ahead, after)
                sweep(pre, free, done[1], tops[1], at == 0)
                sweep(free, pre, done[2], tops[2])
                done = tops
                yield

        sweep(pa, pb, HX - 1, HX + rows + 1)
        list(correct(0, pb, pa, 3, (rows + 3,)))
        sweep(pb, pa, HX - 2, HX + rows + 2)
        sweep(pa, pb, HX - 1, HX + rows + 1)
        last = pb
        finish = correct(1, pb, pa, 2, (cells_x + 2, rows + 2))
        next(finish)
        b_x[0](ODD)

        def along_x(x):
            return near[0, x, own_y] * (0.5 * (last[x + 1, own_y] - last[x - 1, own_y]))

        def along_y(x, y):
            one = pl.ds(y, 1)
            return near[0, x, one] * (0.5 * (last[x, pl.ds((y + 1) % wy, 1)] - last[x, pl.ds(y - 1, 1)]))

        def edge(at):
            v = edge_x[EDGES.index(at), own_y]
            return (v + v) - along_x(HX + at)

        def ends(x):
            lo, hi = edge_y[x, pl.ds(0, 1)], edge_y[x, pl.ds(3, 1)]
            return (lo + lo) - along_y(x, wy - 1), (hi + hi) - along_y(x, cells_y)

        rim_v[0] = edge(-1)
        rim_v[1] = edge(cells_x)
        for x in range(cells_x):
            lo, hi = ends(HX + x)
            rim_w[x, pl.ds(0, 1)] = lo
            rim_w[x, pl.ds(1, 1)] = hi
        v_x[0](ODD)
        next(finish)
        out_x[0] = edge(cells_x - 1)
        out_x[cells_x + 1] = edge(rows)
        for x in range(cells_x):
            w = HX + cells_x + x
            m = near[0, w, own_y]
            p = last[w, own_y]
            out_x[1 + x] = velocity[0, x] - along_x(w)
            v = last[w]
            out_y[x, own_y] = velocity[1, x] - m * (0.5 * (next_y(v) - prev_y(v))[:cells_y])
            lo, hi = ends(w)
            out_y[x, pl.ds(wy - 1, 1)] = lo
            out_y[x, pl.ds(cells_y, 1)] = hi
            dz = jnp.where(lane_o == cells_z - 1, 0.0, next_z(p)) - jnp.where(lane_o == 0, 0.0, prev_z(p))
            out_z[x] = velocity[2, x] - m * (0.5 * dz)
            out_p[x] = p
        s_x[1](ODD)
        for x in every[1:]:
            x[2](ODD)

    assert groups == MOVES, groups


MOVES = [34, 22, 14, 14, 14, 10, 8, 8, 1, 4]


def transport(in_x, in_y, in_z, in_p, rim_x, rim_y, species, vel_out, pres_out, spec_out):
    cells_x, cells_y, cells_z = in_p.shape
    lane_o = lax.broadcasted_iota(jnp.int32, (cells_y, cells_z), 1)
    row_o = lax.broadcasted_iota(jnp.int32, (cells_y, cells_z), 0)

    def next_z(v):
        return pltpu.roll(v, cells_z - 1, 1)

    def prev_z(v):
        return pltpu.roll(v, 1, 1)

    def next_y(v):
        return pltpu.roll(v, v.shape[0] - 1, 0)

    def prev_y(v):
        return pltpu.roll(v, 1, 0)

    mid = slice(0, cells_y)
    pres_out[...] = in_p[...]
    move_x = [in_x[x] for x in range(cells_x + 2)]
    for x in range(cells_x):
        move_y, move_z = in_y[x], in_z[x]
        vel_out[0, x] = move_x[x + 1]
        vel_out[1, x] = move_y[mid]
        vel_out[2, x] = move_z
        lo_x, hi_x = 0.5 * (move_x[x] + move_x[x + 1]), 0.5 * (move_x[x + 1] + move_x[x + 2])
        lo_y, hi_y = (0.5 * (move_y + prev_y(move_y)))[mid], (0.5 * (move_y + next_y(move_y)))[mid]
        lo_z = 0.5 * (move_z + jnp.where(lane_o == 0, 0.0, prev_z(move_z)))
        hi_z = 0.5 * (move_z + jnp.where(lane_o == cells_z - 1, 0.0, next_z(move_z)))

        def into(flow):
            return time_step * jnp.maximum(flow, 0.0)

        def back(flow):
            return -time_step * jnp.minimum(flow, 0.0)

        keep = 1.0 - (into(hi_x) + into(hi_y) + into(hi_z)) - (back(lo_x) + back(lo_y) + back(lo_z))
        from_xl, from_xu = into(lo_x), back(hi_x)
        from_yl, from_yu = into(lo_y), back(hi_y)
        from_zl = jnp.where(lane_o == 0, 0.0, into(lo_z))
        from_zu = jnp.where(lane_o == cells_z - 1, 0.0, back(hi_z))
        for s in range(species.shape[0]):
            q = species[s, x]
            xl = rim_x[0, s] if x == 0 else species[s, x - 1]
            xu = rim_x[1, s] if x == cells_x - 1 else species[s, x + 1]
            yl = jnp.where(row_o == 0, rim_y[0, s, pl.ds(x, 1)], prev_y(q))
            yu = jnp.where(row_o == cells_y - 1, rim_y[1, s, pl.ds(x, 1)], next_y(q))
            total = keep * q + (from_xl * xl + from_xu * xu) + (from_yl * yl + from_yu * yu)
            spec_out[s, x] = total + (from_zl * prev_z(q) + from_zu * next_z(q))


def local(slabs, crosses, velocity, density, source, species):
    cells_x, cells_y, cells_z = density.shape
    assert cells_x == 4 and cells_y == 16 and slabs % 2 == 0
    rows = 2 * cells_x
    wx, wy = rows + 2 * HX, cells_y + 2 * HY
    half_y = cells_y // 2
    kinds = species.shape[0]
    f32 = jnp.float32

    def vmem(*shape):
        return pltpu.VMEM(shape, f32)

    blocks = 2 * OWN + 2
    fine, coarse = (wx, wy, cells_z), (blocks, 3 * half_y, cells_z)
    dma = pltpu.SemaphoreType.DMA
    spec = pl.BlockSpec(memory_space=pltpu.VMEM)
    far = pl.BlockSpec(memory_space=pltpu.HBM)
    moved = [
        (cells_x + 2, cells_y, cells_z), (cells_x, wy, cells_z), density.shape, density.shape,
        (2, kinds, cells_y, cells_z), (2, kinds, cells_x, cells_z), species.shape,
    ]
    between = pl.pallas_call(
        functools.partial(kernel, slabs, crosses),
        out_shape=tuple(pltpu.VMEM(shape, f32) for shape in moved),
        in_specs=[far] * 4,
        out_specs=(spec,) * 7,
        scratch_shapes=[vmem(*velocity.shape), vmem(*density.shape), vmem(*density.shape)]
        + [vmem(2, *density.shape), vmem(2, cells_y, cells_z), vmem(cells_x, 8, cells_z), vmem(half_y, cells_z)]
        + [vmem(2, *fine)] * 2 + [vmem(rows, 8, cells_z), vmem(len(EDGES), wy, cells_z), vmem(wx, 8, cells_z)]
        + [vmem(CYCLES, *fine), vmem(rows, 8, cells_z), vmem(blocks + 2, *coarse[1:]), vmem(CYCLES, *coarse), vmem(cells_x + 2, wy, cells_z)]
        + [vmem(*fine)] * 7 + [vmem(rows, cells_y, cells_z)] + [vmem(*fine)] * 2
        + [vmem(*coarse)] * 10 + [vmem(cells_x, cells_y, cells_z), vmem(rows // 2 + 6, 2 * cells_y, cells_z)]
        + [vmem(2, cells_y, cells_z), vmem(cells_x, 8, cells_z)]
        + [dma((4,))] + [dma((n,)) for n in MOVES for _ in range(2)],
        compiler_params=pltpu.CompilerParams(
            collective_id=0, has_side_effects=True, vmem_limit_bytes=16 << 20
        ),
        name="projection",
    )(*(pltpu.with_memory_space_constraint(a, pltpu.HBM) for a in (velocity, density, source, species)))
    return pl.pallas_call(
        transport,
        out_shape=tuple(jax.ShapeDtypeStruct(a.shape, f32) for a in (velocity, density, species)),
        in_specs=[spec] * 7,
        out_specs=(spec,) * 3,
        compiler_params=pltpu.CompilerParams(vmem_limit_bytes=8 << 20),
        name="transport",
    )(*between)


def solution(mesh):
    plane, stack = P("slab", "cross", None), P(None, "slab", "cross", None)
    return jax.shard_map(
        functools.partial(local, mesh.shape["slab"], mesh.shape["cross"]),
        mesh=mesh,
        in_specs=(stack, plane, plane, stack),
        out_specs=(stack, plane, stack),
        check_vma=False,
    )
```

```python
import functools

import jax
import jax.numpy as jnp
from jax import lax
from jax.experimental import pallas as pl
from jax.experimental.pallas import tpu as pltpu
from jax.sharding import PartitionSpec as P

CYCLES = 2
COARSE = 4
damping = 0.8
time_step = 0.25
MESH = pl.DeviceIdType.MESH
HX = 5
HY = 4
EVEN, ODD = 0, 1
OWN = 3

EDGES = (-5, -1, 0, 3, 4, 7, 8, 12)
BELOW = {-1: 2, 3: 4, 7: 6, 11: 7}
ABOVE = {-4: 0, 0: 1, 4: 3, 8: 5}


def kernel(
    slabs, crosses, velocity_in, density_in, source_in, species,
    out_x, out_y, out_z, out_p, rim_x, rim_y, kinds,
    velocity, density, source, stage, stage_x, stage_y, stage_c,
    near, later, fifth_m, edge_x, edge_y, press, fifth_p, coarse_m, packed_r, given,
    xa, xb, ya, yb, za, zb, goal, scale_back, pb,
    cxa, cxb, cya, cyb, cza, czb, cinv, right, fold, spread, rim_v, rim_w, in_sem, *sems,
):
    cells_x, cells_y, cells_z = density.shape
    rows = 2 * cells_x
    wx, wy = rows + 2 * HX, cells_y + 2 * HY
    half_y = cells_y // 2
    blocks = packed_r.shape[1]
    own_y = pl.ds(0, cells_y)
    own_c = pl.ds(half_y, half_y)
    slab, cross = lax.axis_index("slab"), lax.axis_index("cross")
    odd = slab % 2 == 1
    f32 = jnp.float32

    def there(dx, dy):
        return (slab + dx >= 0) & (slab + dx < slabs) & (cross + dy >= 0) & (cross + dy < crosses)

    groups = []

    def exchange(moves):
        at = len(groups)
        send, recv = sems[2 * at], sems[2 * at + 1]
        groups.append(len(moves))

        def copy(index):
            _, dx, dy, src, dst = moves[index]
            return pltpu.make_async_remote_copy(
                src_ref=src, dst_ref=dst, send_sem=send.at[index], recv_sem=recv.at[index],
                device_id=(slab + dx, cross + dy), device_id_type=MESH,
            )

        def each(role, sender, act, only=None):
            for index, (by, dx, dy, _, _) in enumerate(moves):
                if only is not None and ((dx, dy) == (1, 0)) != only:
                    continue
                if sender and by == role:
                    @pl.when(there(dx, dy))
                    def _():
                        act(copy(index))
                if not sender and (by + dx) % 2 == role:
                    @pl.when(there(-dx, -dy))
                    def _():
                        act(copy(index))

        def start(role):
            each(role, True, lambda c: c.start())

        def arrive(role, only=None):
            each(role, False, lambda c: c.wait_recv(), only)

        def leave(role):
            each(role, True, lambda c: c.wait_send())

        return start, arrive, leave

    def cut_y(dy, low, high, home=0, span=cells_y, rim=wy, behind=cells_y):
        depth = high - low + 1
        if dy > 0:
            return pl.ds(home + span - high, depth), pl.ds(rim - high, depth)
        return pl.ds(home + low - 1, depth), pl.ds(behind + low - 1, depth)

    def fifth(dy):
        return (cells_y - 5, 3) if dy > 0 else (4, 4)

    whole = slice(None)
    first, rest = [], []
    for by, base, out in ((EVEN, 0, -1), (ODD, cells_x, 2)):
        to = 1 - by
        lo_edge, hi_edge = EDGES.index(base), EDGES.index(base + cells_x - 1)
        at = rows if by == EVEN else -cells_x
        touch = 0 if by == EVEN else cells_x - 1
        edge = EDGES.index(at + touch)

        def seen(deep, count, at=at, by=by):
            start = deep - 1 if by == EVEN else cells_x - deep - count + 1
            return pl.ds(start, count), pl.ds(HX + at + start, count)

        for dy in (-1, 1):
            j, k = (2, 0) if dy > 0 else (1, 3)
            src, dst = seen(1, 2)
            ys, yd = cut_y(dy, 1, 2)
            first.append((by, out, dy, stage.at[whole, src, ys], near.at[whole, dst, yd]))
            ys, yd = cut_y(dy, 1, 4)
            first.append((by, out, dy, stage_x.at[min(touch, 1), ys], edge_x.at[edge, yd]))
            first.append((by, out, dy, stage_y.at[whole, j], edge_y.at[pl.ds(HX + at, cells_x), k]))
        src, dst = seen(1, 3)
        first.append((by, out, 0, stage.at[0, src], near.at[0, dst, own_y]))
        src, dst = seen(1, 2)
        first.append((by, out, 0, stage.at[1, src], near.at[1, dst, own_y]))
        first.append((by, out, 0, stage_x.at[min(touch, 1)], edge_x.at[edge, own_y]))
        first.append((by, out, 0, stage_y.at[whole, pl.ds(1, 2)], edge_y.at[pl.ds(HX + at, cells_x), pl.ds(1, 2)]))
        mine = pl.ds(HX + base, cells_x)
        for dy in (-1, 1):
            j, k = (2, 0) if dy > 0 else (1, 3)
            ys, yd = cut_y(dy, 1, 3)
            first.append((by, to, dy, stage.at[whole, whole, ys], near.at[whole, mine, yd]))
            ys, yd = cut_y(dy, 1, 4)
            first.append((by, to, dy, stage_x.at[whole, ys], edge_x.at[pl.ds(lo_edge, 2), yd]))
            first.append((by, to, dy, stage_y.at[whole, j], edge_y.at[mine, k]))
        if by == EVEN:
            first.append((by, 1, 0, stage, near.at[whole, mine, own_y]))
            first.append((by, 1, 0, stage_x, edge_x.at[pl.ds(lo_edge, 2), own_y]))
            first.append((by, 1, 0, stage_y.at[whole, pl.ds(1, 2)], edge_y.at[mine, pl.ds(1, 2)]))
            first.append((by, 1, 0, stage_c, coarse_m.at[OWN + 1, own_c]))

        for dy in (-1, 1):
            for deep, low, high in ((1, 3, 4), (3, 1, 2)):
                src, dst = seen(deep, 2)
                ys, yd = cut_y(dy, low, high)
                rest.append((by, out, dy, stage.at[whole, src, ys], later.at[whole, dst, yd]))
        src, dst = seen(4, 1)
        rest.append((by, out, 0, stage.at[0, src], later.at[0, dst, own_y]))
        src, dst = seen(3, 2)
        rest.append((by, out, 0, stage.at[1, src], later.at[1, dst, own_y]))
        far, row, lands = (3, cells_x - 1, -HX) if by == EVEN else (-2, 0, rows + HX - 1)
        rest.append((by, far, 0, stage.at[0, row], later.at[0, HX + lands, own_y]))
        rest.append((by, far, 0, stage_x.at[min(row, 1)], edge_x.at[EDGES.index(lands), own_y]))
        for dy in (-1, 1):
            ys, yd = cut_y(dy, 4, 4)
            rest.append((by, to, dy, stage.at[whole, whole, ys], later.at[whole, mine, yd]))
            y, j = fifth(dy)
            rest.append((by, to, dy, stage.at[0, whole, y], fifth_m.at[pl.ds(base, cells_x), j]))

    def coarse_moves(ref, own, reach):
        moves = []
        ahead, behind, aside = (2, own, own - 2, 2, reach - 1), (-2, own, own + 2, 2, reach - 1), (0, own, own, 2, reach)
        count = (reach - 3) // 2
        ahead_far, behind_far = (4, own + 2 - count, own - 2 - count, count, reach - 5), (-4, own, own + 4, count, reach - 5)
        for dy, kinds_of in (
            (-1, (ahead, behind)), (1, (ahead, behind)), (0, (ahead, behind)),
            (-1, (ahead_far, behind_far)), (1, (ahead_far, behind_far)), (0, (ahead_far, behind_far)), (-1, (aside,)), (1, (aside,)),
        ):
            for dx, src, dst, count, deep in kinds_of:
                ys, yd = (own_c, own_c) if dy == 0 else cut_y(dy, 1, deep, half_y, half_y, half_y, 2 * half_y)
                moves.append((ODD, dx, dy, ref.at[pl.ds(src, count), ys], ref.at[pl.ds(dst, count), yd]))
        return moves

    def press_moves(ref, reach):
        moves = []
        low, high = (pl.ds(HX, reach), pl.ds(HX + rows, reach)), (pl.ds(HX + rows - reach, reach), pl.ds(HX - reach, reach))
        corner = reach - 1
        low_c, high_c = (pl.ds(HX, corner), pl.ds(HX + rows, corner)), (pl.ds(HX + rows - corner, corner), pl.ds(HX - corner, corner))
        for dy in (-1, 1):
            ys, yd = cut_y(dy, 1, corner)
            moves.append((ODD, 2, dy, ref.at[high_c[0], ys], ref.at[high_c[1], yd]))
            moves.append((ODD, -2, dy, ref.at[low_c[0], ys], ref.at[low_c[1], yd]))
        moves.append((ODD, 2, 0, ref.at[high[0], own_y], ref.at[high[1], own_y]))
        moves.append((ODD, -2, 0, ref.at[low[0], own_y], ref.at[low[1], own_y]))
        own_x = pl.ds(HX, rows)
        for dy in (-1, 1):
            ys, yd = cut_y(dy, 1, HY)
            moves.append((ODD, 0, dy, ref.at[own_x, ys], ref.at[own_x, yd]))
            if reach > HY:
                y, j = fifth(dy)
                moves.append((ODD, 0, dy, ref.at[own_x, y], fifth_p.at[:, j]))
        return moves

    def species_moves():
        moves = []
        for by in (EVEN, ODD):
            for dx, dy in ((-1, 0), (1, 0), (0, -1), (0, 1)):
                if dx != 0:
                    src, dst = kinds.at[:, cells_x - 1 if dx > 0 else 0], rim_x.at[0 if dx > 0 else 1]
                else:
                    src, dst = kinds.at[:, :, cells_y - 1 if dy > 0 else 0], rim_y.at[0 if dy > 0 else 1]
                moves.append((by, dx, dy, src, dst))
        return moves

    back = [(ODD, -1, 0, pb.at[pl.ds(HX - 1, cells_x + 2)], given)]
    sides = [
        (ODD, -1, 0, rim_v.at[0], out_x.at[0]),
        (ODD, -1, 0, rim_v.at[1], out_x.at[cells_x + 1]),
        (ODD, -1, 0, rim_w.at[whole, 0], out_y.at[whole, wy - 1]),
        (ODD, -1, 0, rim_w.at[whole, 1], out_y.at[whole, cells_y]),
    ]

    f_x, g_x, m_x = exchange(first), exchange(rest), exchange(coarse_moves(coarse_m, OWN + 1, 7))
    r_x = [exchange(coarse_moves(packed_r.at[at], OWN, 6)) for at in range(CYCLES)]
    p_x = [exchange(press_moves(press.at[at], HX - at)) for at in range(CYCLES)]
    s_x, b_x, v_x = exchange(species_moves()), exchange(back), exchange(sides)
    every = (f_x, g_x, m_x, *r_x, *p_x, s_x, b_x, v_x)

    def grids(count):
        lane = lax.broadcasted_iota(jnp.int32, (count, cells_z), 1)
        row = lax.broadcasted_iota(jnp.int32, (count, cells_z), 0)
        return row, lane

    def next_z(v, k=1):
        return pltpu.roll(v, cells_z - k, 1)

    def prev_z(v, k=1):
        return pltpu.roll(v, k, 1)

    def next_y(v):
        return pltpu.roll(v, v.shape[0] - 1, 0)

    def prev_y(v):
        return pltpu.roll(v, 1, 0)

    def swap_z(v):
        lane = grids(v.shape[0])[1]
        return jnp.take_along_axis(v, lane + 1 - 2 * (lane % 2), axis=1)

    def pack(two):
        lane = grids(two[0].shape[0])[1]
        return jnp.where(lane % 2 == 0, two[0] + swap_z(two[0]), two[1] + swap_z(two[1]))

    inputs = [
        pltpu.make_async_copy(src, dst, in_sem.at[at])
        for at, (src, dst) in enumerate(
            ((velocity_in, velocity), (density_in, density), (source_in, source), (species, kinds))
        )
    ]
    for copy in inputs:
        copy.start()
    barrier = pltpu.get_barrier_semaphore()
    greet = {ODD: set(), EVEN: set()}
    for moves in (first, rest, coarse_moves(coarse_m, OWN + 1, 7), species_moves(), back):
        for by, dx, dy, _, _ in moves:
            greet[by].add((dx, dy))
            greet[(by + dx) % 2].add((-dx, -dy))

    def enter(role):
        for dx, dy in sorted(greet[role], key=lambda d: (abs(d[0]) == 4, -abs(d[0]) - 2 * abs(d[1]), d)):
            @pl.when(there(dx, dy))
            def _():
                pl.semaphore_signal(barrier, inc=1, device_id=(slab + dx, cross + dy), device_id_type=MESH)

    def entered(role):
        count = jnp.int32(0)
        for dx, dy in sorted(greet[role]):
            count = count + there(dx, dy).astype(jnp.int32)
        return count

    @pl.when(jnp.logical_not(odd))
    def _():
        for ref in (rim_x, rim_y):
            ref[...] = jnp.zeros(ref.shape, f32)
        enter(EVEN)

    @pl.when(odd)
    def _():
        for ref in (near, later, fifth_m, edge_x, edge_y, coarse_m, packed_r, press, fifth_p, rim_x, rim_y):
            ref[...] = jnp.zeros(ref.shape, f32)
        enter(ODD)

    for copy in inputs[:3]:
        copy.wait()
    row_o, lane_o = grids(cells_y)
    for x in range(cells_x):
        v0, v1, v2 = velocity[0, x], velocity[1, x], velocity[2, x]
        dz = jnp.where(lane_o == cells_z - 1, 0.0, next_z(v2)) - jnp.where(lane_o == 0, 0.0, prev_z(v2))
        dy = jnp.where(row_o == cells_y - 1, 0.0, next_y(v1)) - jnp.where(row_o == 0, 0.0, prev_y(v1))
        t = dy + dz
        if x + 1 < cells_x:
            t = t + velocity[0, x + 1]
        if x > 0:
            t = t - velocity[0, x - 1]
        m = 1.0 / density[x]
        stage[0, x] = m
        stage[1, x] = 0.5 * t - source[x]
        fold[x] = m
        stage_y[x, pl.ds(1, 1)] = 0.5 * v1[0:1]
        stage_y[x, pl.ds(2, 1)] = 0.5 * v1[cells_y - 1 : cells_y]
        if x == 0:
            stage_x[0] = 0.5 * v0
        if x == cells_x - 1:
            stage_x[1] = 0.5 * v0

    def folded(x):
        return fold[x, pl.ds(0, half_y, stride=2)] + fold[x, pl.ds(1, half_y, stride=2)]

    mean = 0.125 * pack([folded(0) + folded(1), folded(2) + folded(3)])
    stage_c[...] = mean
    pl.semaphore_wait(barrier, jnp.where(odd, entered(ODD), entered(EVEN)))

    @pl.when(jnp.logical_not(odd))
    def _():
        f_x[0](EVEN)
        f_x[2](EVEN)
        g_x[0](EVEN)
        inputs[3].wait()
        s_x[0](EVEN)
        b_x[1](EVEN)
        for x in range(cells_x):
            m = stage[0, x]
            p = given[1 + x, own_y]
            out_x[1 + x] = velocity[0, x] - m * (0.5 * (given[2 + x, own_y] - given[x, own_y]))
            v = given[1 + x]
            out_y[x, own_y] = velocity[1, x] - m * (0.5 * (next_y(v) - prev_y(v))[:cells_y])
            row_o, lane_o = grids(cells_y)
            dz = jnp.where(lane_o == cells_z - 1, 0.0, next_z(p)) - jnp.where(lane_o == 0, 0.0, prev_z(p))
            out_z[x] = velocity[2, x] - m * (0.5 * dz)
            out_p[x] = p
        v_x[1](EVEN)
        s_x[1](EVEN)
        for x in every[1:]:
            x[2](EVEN)

    @pl.when(odd)
    def _():
        f_x[0](ODD)
        f_x[2](ODD)
        row_w, lane_w = grids(wy)
        row_c, lane_c = grids(2 * half_y + half_y)
        even_c = lane_c % 2 == 0
        row_o, lane_o = grids(cells_y)
        mine = pl.ds(HX + cells_x, cells_x)
        near[0, mine, own_y] = stage[0]
        near[1, mine, own_y] = stage[1]
        edge_x[pl.ds(EDGES.index(cells_x), 2), own_y] = stage_x[...]
        edge_y[mine, pl.ds(1, 2)] = stage_y[:, pl.ds(1, 2)]
        coarse_m[OWN + 2, own_c] = stage_c[...]
        f_x[1](ODD, True)
        m_x[0](ODD)
        g_x[0](ODD)
        f_x[1](ODD, False)

        middle = grids(8)[0]

        def around_y(v, more=None):
            if more is None:
                return prev_y(v), next_y(v)
            own, rim = v[:cells_y], v[cells_y:]
            return (
                prev_y(jnp.concatenate([own, jnp.where(middle == 3, more, rim)], 0)),
                next_y(jnp.concatenate([own, jnp.where(middle == 4, more, rim)], 0)),
            )

        def fine_setup(span, full):
            def mob(x):
                return near[0, x] + later[0, x] if full else near[0, x]

            for x in span:
                m = mob(x)
                lo_x, hi_x = m + mob(x - 1), m + mob(x + 1)
                before, behind = around_y(m, fifth_m[x - HX] if full and HX <= x < HX + rows else None)
                lo_y, hi_y = m + before, m + behind
                lo_z = m + jnp.where(lane_w == 0, 0.0, prev_z(m))
                hi_z = m + jnp.where(lane_w == cells_z - 1, 0.0, next_z(m))
                diag = (lo_x + hi_x) + (lo_y + hi_y) + (lo_z + hi_z)
                inside = m > 0.0
                inv = jnp.where(inside, damping / jnp.where(inside, diag, 1.0), 0.0)
                xa[x], xb[x] = lo_x * inv, hi_x * inv
                ya[x], yb[x] = lo_y * inv, hi_y * inv
                za[x] = jnp.where(lane_w == 0, 0.0, lo_z * inv)
                zb[x] = jnp.where(lane_w == cells_z - 1, 0.0, hi_z * inv)
                t = near[1, x] + later[1, x] if full else near[1, x]
                at = x - HX
                if at in BELOW and (full or BELOW[at] not in (0, 7)):
                    t = t + edge_x[BELOW[at]]
                if at in ABOVE and (full or ABOVE[at] not in (0, 7)):
                    t = t - edge_x[ABOVE[at]]

                def side(j):
                    return jnp.broadcast_to(edge_y[x, pl.ds(j, 1)], t.shape)

                t = t + jnp.where(row_w == wy - 1, side(1), 0.0) - jnp.where(row_w == 0, side(0), 0.0)
                t = t + jnp.where(row_w == cells_y - 1, side(3), 0.0)
                t = t - jnp.where(row_w == cells_y, side(2), 0.0)
                b = t * (inv + inv)
                goal[x] = b
                if not full and HX <= x < HX + rows:
                    scale_back[x - HX] = (diag * (0.5 / damping))[:cells_y]
            return -b

        def faces(x, rows_of, more=None):
            v = rows_of[x]
            before, behind = around_y(v, more)
            t = xa[x] * rows_of[x - 1] + xb[x] * rows_of[x + 1]
            t = t + (ya[x] * before + yb[x] * behind)
            return v, t + (za[x] * prev_z(v) + zb[x] * next_z(v))

        def relax(x, rows_of, more=None):
            v, t = faces(x, rows_of, more)
            return (1.0 - damping) * v + (t - goal[x])

        def cascade(levels, lag, rows_of=None, part=None):
            if rows_of is None:
                rows_of = [{} for _ in levels]
            low = min(level[0] for level in levels)
            high = max(level[1] for level in levels)
            for step in range(low, high + lag * len(levels)):
                for k, (start, end, row) in enumerate(levels):
                    x = step - lag * k
                    if start <= x < end and x not in rows_of[k] and (part is None or x < part[k]):
                        rows_of[k][x] = row(x, rows_of[k - 1])
            return rows_of

        def coarse_setup():
            swapped = [swap_z(coarse_m[c]) for c in range(blocks + 2)]
            for c in range(1, blocks + 1):
                lo, hi = jnp.where(even_c, swapped[c - 1], swapped[c]), jnp.where(even_c, swapped[c], swapped[c + 1])
                m, b = coarse_m[c], c - 1
                lo_x, hi_x = m + lo, m + hi
                lo_y, hi_y = m + prev_y(m), m + next_y(m)
                lo_z = m + jnp.where(lane_c < 2, 0.0, prev_z(m, 2))
                hi_z = m + jnp.where(lane_c >= cells_z - 2, 0.0, next_z(m, 2))
                diag = (lo_x + hi_x) + (lo_y + hi_y) + (lo_z + hi_z)
                inside = m > 0.0
                inv = jnp.where(inside, damping / jnp.where(inside, diag, 1.0), 0.0)
                cxa[b], cxb[b] = lo_x * inv, hi_x * inv
                cya[b], cyb[b] = lo_y * inv, hi_y * inv
                cza[b] = jnp.where(lane_c < 2, 0.0, lo_z * inv)
                czb[b] = jnp.where(lane_c >= cells_z - 2, 0.0, hi_z * inv)
                cinv[b] = inv

        shifted = {}

        def swapped(rows_of, b):
            key = (id(rows_of), b)
            if key not in shifted:
                shifted[key] = swap_z(rows_of[b])
            return shifted[key]

        def coarse_relax(b, rows_of):
            v = rows_of[b]
            before = b - 1 if b - 1 in rows_of else b
            behind = b + 1 if b + 1 in rows_of else b
            lo = jnp.where(even_c, swapped(rows_of, before), swapped(rows_of, b))
            hi = jnp.where(even_c, swapped(rows_of, b), swapped(rows_of, behind))
            t = cxa[b] * lo + cxb[b] * hi
            t = t + (cya[b] * prev_y(v) + cyb[b] * next_y(v))
            t = t + (cza[b] * prev_z(v, 2) + czb[b] * next_z(v, 2))
            return (1.0 - damping) * v + (t - right[b])

        own = range(HX, HX + rows)
        margin, tall = half_y // 2, 2 * cells_y

        def send(at, deeper):
            totals = {}

            def smoothed(x, rows_of):
                v = deeper(x, rows_of)
                if x in own:
                    press[at, x, own_y] = v[:cells_y]
                return v

            def residual(x, rows_of):
                v, t = faces(x, rows_of)
                d = (damping * v - (t - goal[x]))[:cells_y] * scale_back[x - HX]
                totals[x] = d
                if (x - HX) % 2 == 1:
                    fold[(x - HX) // 2] = totals[x - 1] + d
                return d

            return smoothed, residual

        def leave_off(at):
            for b in range(2):
                packed_r[at, OWN + b, own_c] = pack([folded(2 * b), folded(2 * b + 1)])
            r_x[at][0](ODD)
            p_x[at][0](ODD)

        def correct(at):
            r_x[at][1](ODD)

            def begin(b, _):
                r = packed_r[at, b] * cinv[b]
                right[b] = r
                return -r

            def prolong(b, rows_of):
                c = coarse_relax(b, rows_of)
                d = swap_z(c)
                for odd_row in (0, 1):
                    q = 2 * (b - OWN) + odd_row
                    if -3 <= q < rows // 2 + 3:
                        v = jnp.where(even_c, d, c) if odd_row else jnp.where(even_c, c, d)
                        v = v[margin : margin + cells_y]
                        spread[q + 3, pl.ds(0, tall // 2, stride=2)] = v
                        spread[q + 3, pl.ds(1, tall // 2, stride=2)] = v
                return c

            held = [(0, blocks, begin), (0, blocks, coarse_relax), (1, blocks - 1, coarse_relax), (1, blocks - 1, prolong)]
            kept = cascade(held, 20)
            shifted.clear()
            p_x[at][1](ODD)
            fifths = {}

            def add(x, _):
                up = spread.at[(x - HX) // 2 + 3]
                ahead, after = up[pl.ds(0, 8)], up[pl.ds(8 + cells_y, 8)]
                if at == 0 and x in own:
                    fifths[x] = fifth_p[x - HX] + jnp.where(middle < HY, ahead, after)
                change = jnp.concatenate([up[pl.ds(8, cells_y)], jnp.where(middle < HY, after, ahead)], 0)
                return press[at, x] + change

            return add, lambda x, rows_of: relax(x, rows_of, fifths.get(x))

        low, high = HX, HX + rows
        smoothed, residual = send(0, relax)
        cascade(
            [
                (low - 2, high + 2, lambda x, _: fine_setup((x,), False)),
                (low - 1, high + 1, smoothed),
                (low, high, residual),
            ],
            20,
        )
        leave_off(0)
        inputs[3].wait()
        s_x[0](ODD)
        g_x[1](ODD)
        fine_setup(range(1, wx - 1), True)
        m_x[1](ODD)
        coarse_setup()
        add, first_relax = correct(0)
        smoothed, residual = send(1, relax)
        cascade(
            [
                (low - 5, high + 5, add),
                (low - 4, high + 4, first_relax),
                (low - 3, high + 3, relax),
                (low - 2, high + 2, relax),
                (low - 1, high + 1, smoothed),
                (low, high, residual),
            ],
            20,
        )
        leave_off(1)
        last = pb
        add, first_relax = correct(1)

        def final(x, rows_of):
            v = relax(x, rows_of)
            last[x] = v
            return v

        levels = [(low - 4, high + 4, add), (low - 3, high + 3, first_relax), (low - 2, high + 2, final)]
        top = HX + cells_x + 2
        kept = cascade(levels, 20, None, (top + 2, top + 1, top))
        b_x[0](ODD)

        def along_x(x):
            return near[0, x, own_y] * (0.5 * (last[x + 1, own_y] - last[x - 1, own_y]))

        def along_y(x, y):
            one = pl.ds(y, 1)
            return near[0, x, one] * (0.5 * (last[x, pl.ds((y + 1) % wy, 1)] - last[x, pl.ds(y - 1, 1)]))

        def edge(at):
            v = edge_x[EDGES.index(at), own_y]
            return (v + v) - along_x(HX + at)

        def ends(x):
            lo, hi = edge_y[x, pl.ds(0, 1)], edge_y[x, pl.ds(3, 1)]
            return (lo + lo) - along_y(x, wy - 1), (hi + hi) - along_y(x, cells_y)

        rim_v[0] = edge(-1)
        rim_v[1] = edge(cells_x)
        for x in range(cells_x):
            lo, hi = ends(HX + x)
            rim_w[x, pl.ds(0, 1)] = lo
            rim_w[x, pl.ds(1, 1)] = hi
        v_x[0](ODD)
        cascade(levels, 20, kept)
        out_x[0] = edge(cells_x - 1)
        out_x[cells_x + 1] = edge(rows)
        for x in range(cells_x):
            w = HX + cells_x + x
            m = near[0, w, own_y]
            p = last[w, own_y]
            out_x[1 + x] = velocity[0, x] - along_x(w)
            v = last[w]
            out_y[x, own_y] = velocity[1, x] - m * (0.5 * (next_y(v) - prev_y(v))[:cells_y])
            lo, hi = ends(w)
            out_y[x, pl.ds(wy - 1, 1)] = lo
            out_y[x, pl.ds(cells_y, 1)] = hi
            dz = jnp.where(lane_o == cells_z - 1, 0.0, next_z(p)) - jnp.where(lane_o == 0, 0.0, prev_z(p))
            out_z[x] = velocity[2, x] - m * (0.5 * dz)
            out_p[x] = p
        s_x[1](ODD)
        for x in every[1:]:
            x[2](ODD)

    assert groups == MOVES, groups


MOVES = [36, 24, 14, 14, 14, 10, 8, 8, 1, 4]


def transport(in_x, in_y, in_z, in_p, rim_x, rim_y, species, vel_out, pres_out, spec_out, stage, sems):
    cells_x, cells_y, cells_z = in_p.shape
    lane_o = lax.broadcasted_iota(jnp.int32, (cells_y, cells_z), 1)
    row_o = lax.broadcasted_iota(jnp.int32, (cells_y, cells_z), 0)

    def next_z(v):
        return pltpu.roll(v, cells_z - 1, 1)

    def prev_z(v):
        return pltpu.roll(v, 1, 1)

    def next_y(v):
        return pltpu.roll(v, v.shape[0] - 1, 0)

    def prev_y(v):
        return pltpu.roll(v, 1, 0)

    mid = slice(0, cells_y)
    copies = [
        pltpu.make_async_copy(src, dst, sems.at[at])
        for at, (src, dst) in enumerate(
            (
                (in_x.at[pl.ds(1, cells_x)], vel_out.at[0]),
                (in_y.at[:, pl.ds(0, cells_y)], vel_out.at[1]),
                (in_z, vel_out.at[2]),
                (in_p, pres_out),
                *((stage.at[x], spec_out.at[:, x]) for x in range(cells_x)),
            )
        )
    ]
    for copy in copies[:4]:
        copy.start()
    move_x = [in_x[x] for x in range(cells_x + 2)]
    for x in range(cells_x):
        move_y, move_z = in_y[x], in_z[x]
        lo_x, hi_x = 0.5 * (move_x[x] + move_x[x + 1]), 0.5 * (move_x[x + 1] + move_x[x + 2])
        lo_y, hi_y = (0.5 * (move_y + prev_y(move_y)))[mid], (0.5 * (move_y + next_y(move_y)))[mid]
        lo_z = 0.5 * (move_z + jnp.where(lane_o == 0, 0.0, prev_z(move_z)))
        hi_z = 0.5 * (move_z + jnp.where(lane_o == cells_z - 1, 0.0, next_z(move_z)))

        def into(flow):
            return time_step * jnp.maximum(flow, 0.0)

        def back(flow):
            return -time_step * jnp.minimum(flow, 0.0)

        keep = 1.0 - (into(hi_x) + into(hi_y) + into(hi_z)) - (back(lo_x) + back(lo_y) + back(lo_z))
        from_xl, from_xu = into(lo_x), back(hi_x)
        from_yl, from_yu = into(lo_y), back(hi_y)
        from_zl = jnp.where(lane_o == 0, 0.0, into(lo_z))
        from_zu = jnp.where(lane_o == cells_z - 1, 0.0, back(hi_z))
        for s in range(species.shape[0]):
            q = species[s, x]
            xl = rim_x[0, s] if x == 0 else species[s, x - 1]
            xu = rim_x[1, s] if x == cells_x - 1 else species[s, x + 1]
            yl = jnp.where(row_o == 0, rim_y[0, s, pl.ds(x, 1)], prev_y(q))
            yu = jnp.where(row_o == cells_y - 1, rim_y[1, s, pl.ds(x, 1)], next_y(q))
            total = keep * q + (from_xl * xl + from_xu * xu) + (from_yl * yl + from_yu * yu)
            stage[x, s] = total + (from_zl * prev_z(q) + from_zu * next_z(q))
        copies[4 + x].start()
    for copy in copies:
        copy.wait()


def local(slabs, crosses, velocity, density, source, species):
    cells_x, cells_y, cells_z = density.shape
    assert cells_x == 4 and cells_y == 16 and slabs % 2 == 0
    rows = 2 * cells_x
    wx, wy = rows + 2 * HX, cells_y + 2 * HY
    half_y = cells_y // 2
    kinds = species.shape[0]
    f32 = jnp.float32

    def vmem(*shape):
        return pltpu.VMEM(shape, f32)

    blocks = 2 * OWN + 2
    fine, coarse = (wx, wy, cells_z), (blocks, 3 * half_y, cells_z)
    dma = pltpu.SemaphoreType.DMA
    spec = pl.BlockSpec(memory_space=pltpu.VMEM)
    far = pl.BlockSpec(memory_space=pltpu.HBM)
    moved = [
        (cells_x + 2, cells_y, cells_z), (cells_x, wy, cells_z), density.shape, density.shape,
        (2, kinds, cells_y, cells_z), (2, kinds, cells_x, cells_z), species.shape,
    ]
    between = pl.pallas_call(
        functools.partial(kernel, slabs, crosses),
        out_shape=tuple(pltpu.VMEM(shape, f32) for shape in moved),
        in_specs=[far] * 4,
        out_specs=(spec,) * 7,
        scratch_shapes=[vmem(*velocity.shape), vmem(*density.shape), vmem(*density.shape)]
        + [vmem(2, *density.shape), vmem(2, cells_y, cells_z), vmem(cells_x, 8, cells_z), vmem(half_y, cells_z)]
        + [vmem(2, *fine)] * 2 + [vmem(rows, 8, cells_z), vmem(len(EDGES), wy, cells_z), vmem(wx, 8, cells_z)]
        + [vmem(CYCLES, *fine), vmem(rows, 8, cells_z), vmem(blocks + 2, *coarse[1:]), vmem(CYCLES, *coarse), vmem(cells_x + 2, wy, cells_z)]
        + [vmem(*fine)] * 7 + [vmem(rows, cells_y, cells_z), vmem(*fine)]
        + [vmem(*coarse)] * 8 + [vmem(cells_x, cells_y, cells_z), vmem(rows // 2 + 6, 2 * cells_y, cells_z)]
        + [vmem(2, cells_y, cells_z), vmem(cells_x, 8, cells_z)]
        + [dma((4,))] + [dma((n,)) for n in MOVES for _ in range(2)],
        compiler_params=pltpu.CompilerParams(
            collective_id=0, has_side_effects=True, vmem_limit_bytes=16 << 20
        ),
        name="projection",
    )(*(pltpu.with_memory_space_constraint(a, pltpu.HBM) for a in (velocity, density, source, species)))
    return pl.pallas_call(
        transport,
        out_shape=tuple(jax.ShapeDtypeStruct(a.shape, f32) for a in (velocity, density, species)),
        in_specs=[spec] * 7,
        out_specs=(far,) * 3,
        scratch_shapes=[vmem(cells_x, kinds, cells_y, cells_z), dma((4 + cells_x,))],
        compiler_params=pltpu.CompilerParams(vmem_limit_bytes=8 << 20),
        name="transport",
    )(*between)


def solution(mesh):
    plane, stack = P("slab", "cross", None), P(None, "slab", "cross", None)
    return jax.shard_map(
        functools.partial(local, mesh.shape["slab"], mesh.shape["cross"]),
        mesh=mesh,
        in_specs=(stack, plane, plane, stack),
        out_specs=(stack, plane, stack),
        check_vma=False,
    )
```

```python
import functools

import jax
import jax.numpy as jnp
from jax import lax
from jax.experimental import pallas as pl
from jax.experimental.pallas import tpu as pltpu
from jax.sharding import PartitionSpec as P

CYCLES = 2
COARSE = 4
damping = 0.8
time_step = 0.25
MESH = pl.DeviceIdType.MESH
HX = 5
HY = 4
EVEN, ODD = 0, 1
OWN = 3

EDGES = (-5, -1, 0, 3, 4, 7, 8, 12)
BELOW = {-1: 2, 3: 4, 7: 6, 11: 7}
ABOVE = {-4: 0, 0: 1, 4: 3, 8: 5}


def kernel(
    slabs, crosses, velocity_in, density_in, source_in, species,
    out_x, out_y, out_z, out_p, rim_x, rim_y, kinds,
    velocity, density, source, stage, stage_x, stage_y, stage_c,
    near, later, fifth_m, edge_x, edge_y, press, fifth_p, coarse_m, packed_r, given,
    xa, xb, ya, yb, za, zb, goal, scale_back, pb,
    cxa, cxb, cya, cyb, cza, czb, cinv, right, fold, spread, rim_v, rim_w, in_sem, *sems,
):
    cells_x, cells_y, cells_z = density.shape
    rows = 2 * cells_x
    wx, wy = rows + 2 * HX, cells_y + 2 * HY
    half_y = cells_y // 2
    blocks = packed_r.shape[1]
    own_y = pl.ds(0, cells_y)
    own_c = pl.ds(half_y, half_y)
    slab, cross = lax.axis_index("slab"), lax.axis_index("cross")
    odd = slab % 2 == 1
    f32 = jnp.float32

    def there(dx, dy):
        return (slab + dx >= 0) & (slab + dx < slabs) & (cross + dy >= 0) & (cross + dy < crosses)

    groups = []

    def exchange(moves):
        at = len(groups)
        send, recv = sems[2 * at], sems[2 * at + 1]
        groups.append(len(moves))

        def copy(index):
            _, dx, dy, src, dst = moves[index]
            return pltpu.make_async_remote_copy(
                src_ref=src, dst_ref=dst, send_sem=send.at[index], recv_sem=recv.at[index],
                device_id=(slab + dx, cross + dy), device_id_type=MESH,
            )

        def each(role, sender, act, only=None):
            for index, (by, dx, dy, _, _) in enumerate(moves):
                if only is not None and ((dx, dy) == (1, 0)) != only:
                    continue
                if sender and by == role:
                    @pl.when(there(dx, dy))
                    def _():
                        act(copy(index))
                if not sender and (by + dx) % 2 == role:
                    @pl.when(there(-dx, -dy))
                    def _():
                        act(copy(index))

        def start(role):
            each(role, True, lambda c: c.start())

        def arrive(role, only=None):
            each(role, False, lambda c: c.wait_recv(), only)

        def leave(role):
            each(role, True, lambda c: c.wait_send())

        return start, arrive, leave

    def cut_y(dy, low, high, home=0, span=cells_y, rim=wy, behind=cells_y):
        depth = high - low + 1
        if dy > 0:
            return pl.ds(home + span - high, depth), pl.ds(rim - high, depth)
        return pl.ds(home + low - 1, depth), pl.ds(behind + low - 1, depth)

    def fifth(dy):
        return (cells_y - 5, 3) if dy > 0 else (4, 4)

    whole = slice(None)
    first, rest = [], []
    for by, base, out in ((EVEN, 0, -1), (ODD, cells_x, 2)):
        to = 1 - by
        lo_edge, hi_edge = EDGES.index(base), EDGES.index(base + cells_x - 1)
        at = rows if by == EVEN else -cells_x
        touch = 0 if by == EVEN else cells_x - 1
        edge = EDGES.index(at + touch)

        def seen(deep, count, at=at, by=by):
            start = deep - 1 if by == EVEN else cells_x - deep - count + 1
            return pl.ds(start, count), pl.ds(HX + at + start, count)

        for dy in (-1, 1):
            j, k = (2, 0) if dy > 0 else (1, 3)
            src, dst = seen(1, 2)
            ys, yd = cut_y(dy, 1, 2)
            first.append((by, out, dy, stage.at[whole, src, ys], near.at[whole, dst, yd]))
            ys, yd = cut_y(dy, 1, 4)
            first.append((by, out, dy, stage_x.at[min(touch, 1), ys], edge_x.at[edge, yd]))
            first.append((by, out, dy, stage_y.at[whole, j], edge_y.at[pl.ds(HX + at, cells_x), k]))
        src, dst = seen(1, 3)
        first.append((by, out, 0, stage.at[0, src], near.at[0, dst, own_y]))
        src, dst = seen(1, 2)
        first.append((by, out, 0, stage.at[1, src], near.at[1, dst, own_y]))
        first.append((by, out, 0, stage_x.at[min(touch, 1)], edge_x.at[edge, own_y]))
        first.append((by, out, 0, stage_y.at[whole, pl.ds(1, 2)], edge_y.at[pl.ds(HX + at, cells_x), pl.ds(1, 2)]))
        mine = pl.ds(HX + base, cells_x)
        for dy in (-1, 1):
            j, k = (2, 0) if dy > 0 else (1, 3)
            ys, yd = cut_y(dy, 1, 3)
            first.append((by, to, dy, stage.at[whole, whole, ys], near.at[whole, mine, yd]))
            ys, yd = cut_y(dy, 1, 4)
            first.append((by, to, dy, stage_x.at[whole, ys], edge_x.at[pl.ds(lo_edge, 2), yd]))
            first.append((by, to, dy, stage_y.at[whole, j], edge_y.at[mine, k]))
        if by == EVEN:
            first.append((by, 1, 0, stage, near.at[whole, mine, own_y]))
            first.append((by, 1, 0, stage_x, edge_x.at[pl.ds(lo_edge, 2), own_y]))
            first.append((by, 1, 0, stage_y.at[whole, pl.ds(1, 2)], edge_y.at[mine, pl.ds(1, 2)]))
            first.append((by, 1, 0, stage_c, coarse_m.at[OWN + 1, own_c]))

        for dy in (-1, 1):
            for deep, low, high in ((1, 3, 4), (3, 1, 2)):
                src, dst = seen(deep, 2)
                ys, yd = cut_y(dy, low, high)
                rest.append((by, out, dy, stage.at[whole, src, ys], later.at[whole, dst, yd]))
        src, dst = seen(4, 1)
        rest.append((by, out, 0, stage.at[0, src], later.at[0, dst, own_y]))
        src, dst = seen(3, 2)
        rest.append((by, out, 0, stage.at[1, src], later.at[1, dst, own_y]))
        far, row, lands = (3, cells_x - 1, -HX) if by == EVEN else (-2, 0, rows + HX - 1)
        rest.append((by, far, 0, stage.at[0, row], later.at[0, HX + lands, own_y]))
        rest.append((by, far, 0, stage_x.at[min(row, 1)], edge_x.at[EDGES.index(lands), own_y]))
        for dy in (-1, 1):
            ys, yd = cut_y(dy, 4, 4)
            rest.append((by, to, dy, stage.at[whole, whole, ys], later.at[whole, mine, yd]))
            y, j = fifth(dy)
            rest.append((by, to, dy, stage.at[0, whole, y], fifth_m.at[pl.ds(base, cells_x), j]))

    def coarse_moves(ref, own, reach):
        moves = []
        ahead, behind, aside = (2, own, own - 2, 2, reach - 1), (-2, own, own + 2, 2, reach - 1), (0, own, own, 2, reach)
        count = (reach - 3) // 2
        ahead_far, behind_far = (4, own + 2 - count, own - 2 - count, count, reach - 5), (-4, own, own + 4, count, reach - 5)
        for dy, kinds_of in (
            (-1, (ahead, behind)), (1, (ahead, behind)), (0, (ahead, behind)),
            (-1, (ahead_far, behind_far)), (1, (ahead_far, behind_far)), (0, (ahead_far, behind_far)), (-1, (aside,)), (1, (aside,)),
        ):
            for dx, src, dst, count, deep in kinds_of:
                ys, yd = (own_c, own_c) if dy == 0 else cut_y(dy, 1, deep, half_y, half_y, half_y, 2 * half_y)
                moves.append((ODD, dx, dy, ref.at[pl.ds(src, count), ys], ref.at[pl.ds(dst, count), yd]))
        return moves

    def press_moves(ref, reach):
        moves = []
        low, high = (pl.ds(HX, reach), pl.ds(HX + rows, reach)), (pl.ds(HX + rows - reach, reach), pl.ds(HX - reach, reach))
        corner = reach - 1
        low_c, high_c = (pl.ds(HX, corner), pl.ds(HX + rows, corner)), (pl.ds(HX + rows - corner, corner), pl.ds(HX - corner, corner))
        for dy in (-1, 1):
            ys, yd = cut_y(dy, 1, corner)
            moves.append((ODD, 2, dy, ref.at[high_c[0], ys], ref.at[high_c[1], yd]))
            moves.append((ODD, -2, dy, ref.at[low_c[0], ys], ref.at[low_c[1], yd]))
        moves.append((ODD, 2, 0, ref.at[high[0], own_y], ref.at[high[1], own_y]))
        moves.append((ODD, -2, 0, ref.at[low[0], own_y], ref.at[low[1], own_y]))
        own_x = pl.ds(HX, rows)
        for dy in (-1, 1):
            ys, yd = cut_y(dy, 1, HY)
            moves.append((ODD, 0, dy, ref.at[own_x, ys], ref.at[own_x, yd]))
            if reach > HY:
                y, j = fifth(dy)
                moves.append((ODD, 0, dy, ref.at[own_x, y], fifth_p.at[:, j]))
        return moves

    def species_moves():
        moves = []
        for by in (EVEN, ODD):
            for dx, dy in ((-1, 0), (1, 0), (0, -1), (0, 1)):
                if dx != 0:
                    src, dst = kinds.at[:, cells_x - 1 if dx > 0 else 0], rim_x.at[0 if dx > 0 else 1]
                else:
                    src, dst = kinds.at[:, :, cells_y - 1 if dy > 0 else 0], rim_y.at[0 if dy > 0 else 1]
                moves.append((by, dx, dy, src, dst))
        return moves

    back = [(ODD, -1, 0, pb.at[pl.ds(HX - 1, cells_x + 2)], given)]
    sides = [
        (ODD, -1, 0, rim_v.at[0], out_x.at[0]),
        (ODD, -1, 0, rim_v.at[1], out_x.at[cells_x + 1]),
        (ODD, -1, 0, rim_w.at[whole, 0], out_y.at[whole, wy - 1]),
        (ODD, -1, 0, rim_w.at[whole, 1], out_y.at[whole, cells_y]),
    ]

    f_x, g_x, m_x = exchange(first), exchange(rest), exchange(coarse_moves(coarse_m, OWN + 1, 7))
    r_x = [exchange(coarse_moves(packed_r.at[at], OWN, 6)) for at in range(CYCLES)]
    p_x = [exchange(press_moves(press.at[at], HX - at)) for at in range(CYCLES)]
    s_x, b_x, v_x = exchange(species_moves()), exchange(back), exchange(sides)
    every = (f_x, g_x, m_x, *r_x, *p_x, s_x, b_x, v_x)

    def grids(count):
        lane = lax.broadcasted_iota(jnp.int32, (count, cells_z), 1)
        row = lax.broadcasted_iota(jnp.int32, (count, cells_z), 0)
        return row, lane

    def next_z(v, k=1):
        return pltpu.roll(v, cells_z - k, 1)

    def prev_z(v, k=1):
        return pltpu.roll(v, k, 1)

    def next_y(v):
        return pltpu.roll(v, v.shape[0] - 1, 0)

    def prev_y(v):
        return pltpu.roll(v, 1, 0)

    def swap_z(v):
        lane = grids(v.shape[0])[1]
        return jnp.take_along_axis(v, lane + 1 - 2 * (lane % 2), axis=1)

    def pack(two):
        lane = grids(two[0].shape[0])[1]
        return jnp.where(lane % 2 == 0, two[0] + swap_z(two[0]), two[1] + swap_z(two[1]))

    inputs = [
        pltpu.make_async_copy(src, dst, in_sem.at[at])
        for at, (src, dst) in enumerate(
            ((velocity_in, velocity), (density_in, density), (source_in, source), (species, kinds))
        )
    ]
    for copy in inputs:
        copy.start()
    barrier = pltpu.get_barrier_semaphore()
    greet = {ODD: set(), EVEN: set()}
    for moves in (first, rest, coarse_moves(coarse_m, OWN + 1, 7), species_moves(), back):
        for by, dx, dy, _, _ in moves:
            greet[by].add((dx, dy))
            greet[(by + dx) % 2].add((-dx, -dy))

    def enter(role):
        for dx, dy in sorted(greet[role], key=lambda d: (abs(d[0]) == 4, -abs(d[0]) - 2 * abs(d[1]), d)):
            @pl.when(there(dx, dy))
            def _():
                pl.semaphore_signal(barrier, inc=1, device_id=(slab + dx, cross + dy), device_id_type=MESH)

    def entered(role):
        count = jnp.int32(0)
        for dx, dy in sorted(greet[role]):
            count = count + there(dx, dy).astype(jnp.int32)
        return count

    @pl.when(jnp.logical_not(odd))
    def _():
        for ref in (rim_x, rim_y):
            ref[...] = jnp.zeros(ref.shape, f32)
        enter(EVEN)

    @pl.when(odd)
    def _():
        for ref in (near, later, fifth_m, edge_x, edge_y, coarse_m, packed_r, press, fifth_p, rim_x, rim_y):
            ref[...] = jnp.zeros(ref.shape, f32)
        enter(ODD)

    for copy in inputs[:3]:
        copy.wait()
    row_o, lane_o = grids(cells_y)
    for x in range(cells_x):
        v0, v1, v2 = velocity[0, x], velocity[1, x], velocity[2, x]
        dz = jnp.where(lane_o == cells_z - 1, 0.0, next_z(v2)) - jnp.where(lane_o == 0, 0.0, prev_z(v2))
        dy = jnp.where(row_o == cells_y - 1, 0.0, next_y(v1)) - jnp.where(row_o == 0, 0.0, prev_y(v1))
        t = dy + dz
        if x + 1 < cells_x:
            t = t + velocity[0, x + 1]
        if x > 0:
            t = t - velocity[0, x - 1]
        m = 1.0 / density[x]
        stage[0, x] = m
        stage[1, x] = 0.5 * t - source[x]
        fold[x] = m
        stage_y[x, pl.ds(1, 1)] = 0.5 * v1[0:1]
        stage_y[x, pl.ds(2, 1)] = 0.5 * v1[cells_y - 1 : cells_y]
        if x == 0:
            stage_x[0] = 0.5 * v0
        if x == cells_x - 1:
            stage_x[1] = 0.5 * v0

    def folded(x):
        return fold[x, pl.ds(0, half_y, stride=2)] + fold[x, pl.ds(1, half_y, stride=2)]

    mean = 0.125 * pack([folded(0) + folded(1), folded(2) + folded(3)])
    stage_c[...] = mean
    pl.semaphore_wait(barrier, jnp.where(odd, entered(ODD), entered(EVEN)))

    @pl.when(jnp.logical_not(odd))
    def _():
        f_x[0](EVEN)
        f_x[2](EVEN)
        g_x[0](EVEN)
        inputs[3].wait()
        s_x[0](EVEN)
        b_x[1](EVEN)
        for x in range(cells_x):
            m = stage[0, x]
            p = given[1 + x, own_y]
            out_x[1 + x] = velocity[0, x] - m * (0.5 * (given[2 + x, own_y] - given[x, own_y]))
            v = given[1 + x]
            out_y[x, own_y] = velocity[1, x] - m * (0.5 * (next_y(v) - prev_y(v))[:cells_y])
            row_o, lane_o = grids(cells_y)
            dz = jnp.where(lane_o == cells_z - 1, 0.0, next_z(p)) - jnp.where(lane_o == 0, 0.0, prev_z(p))
            out_z[x] = velocity[2, x] - m * (0.5 * dz)
            out_p[x] = p
        v_x[1](EVEN)
        s_x[1](EVEN)
        for x in every[1:]:
            x[2](EVEN)

    @pl.when(odd)
    def _():
        f_x[0](ODD)
        f_x[2](ODD)
        row_w, lane_w = grids(wy)
        row_c, lane_c = grids(2 * half_y + half_y)
        even_c = lane_c % 2 == 0
        row_o, lane_o = grids(cells_y)
        mine = pl.ds(HX + cells_x, cells_x)
        near[0, mine, own_y] = stage[0]
        near[1, mine, own_y] = stage[1]
        edge_x[pl.ds(EDGES.index(cells_x), 2), own_y] = stage_x[...]
        edge_y[mine, pl.ds(1, 2)] = stage_y[:, pl.ds(1, 2)]
        coarse_m[OWN + 2, own_c] = stage_c[...]
        f_x[1](ODD, True)
        m_x[0](ODD)
        g_x[0](ODD)
        f_x[1](ODD, False)

        middle = grids(8)[0]

        def around_y(v, more=None):
            if more is None:
                return prev_y(v), next_y(v)
            own, rim = v[:cells_y], v[cells_y:]
            return (
                prev_y(jnp.concatenate([own, jnp.where(middle == 3, more, rim)], 0)),
                next_y(jnp.concatenate([own, jnp.where(middle == 4, more, rim)], 0)),
            )

        def fine_setup(span, full, edge=False):
            def mob(x):
                return near[0, x] + later[0, x] if full else near[0, x]

            for x in span:
                m = mob(x)
                lo_x, hi_x = m + mob(x - 1), m + mob(x + 1)
                before, behind = around_y(m, fifth_m[x - HX] if full and HX <= x < HX + rows else None)
                lo_y, hi_y = m + before, m + behind
                lo_z = m + jnp.where(lane_w == 0, 0.0, prev_z(m))
                hi_z = m + jnp.where(lane_w == cells_z - 1, 0.0, next_z(m))
                diag = (lo_x + hi_x) + (lo_y + hi_y) + (lo_z + hi_z)
                inside = m > 0.0
                inv = jnp.where(inside, damping / jnp.where(inside, diag, 1.0), 0.0)
                if not edge:
                    xa[x], xb[x] = lo_x * inv, hi_x * inv
                    ya[x], yb[x] = lo_y * inv, hi_y * inv
                    za[x] = jnp.where(lane_w == 0, 0.0, lo_z * inv)
                    zb[x] = jnp.where(lane_w == cells_z - 1, 0.0, hi_z * inv)
                t = near[1, x] + later[1, x] if full else near[1, x]
                at = x - HX
                if at in BELOW and (full or BELOW[at] not in (0, 7)):
                    t = t + edge_x[BELOW[at]]
                if at in ABOVE and (full or ABOVE[at] not in (0, 7)):
                    t = t - edge_x[ABOVE[at]]

                def side(j):
                    return jnp.broadcast_to(edge_y[x, pl.ds(j, 1)], t.shape)

                t = t + jnp.where(row_w == wy - 1, side(1), 0.0) - jnp.where(row_w == 0, side(0), 0.0)
                t = t + jnp.where(row_w == cells_y - 1, side(3), 0.0)
                t = t - jnp.where(row_w == cells_y, side(2), 0.0)
                b = t * (inv + inv)
                if edge:
                    return -b[:cells_y]
                goal[x] = b
                if not full and HX <= x < HX + rows:
                    scale_back[x - HX] = (diag * (0.5 / damping))[:cells_y]
            return -b

        def faces(x, rows_of, more, tall):
            v = rows_of[x]
            before, behind = around_y(v, more)
            v = v[:tall]
            t = xa[x, :tall] * rows_of[x - 1][:tall] + xb[x, :tall] * rows_of[x + 1][:tall]
            t = t + (ya[x, :tall] * before[:tall] + yb[x, :tall] * behind[:tall])
            return v, t + (za[x, :tall] * prev_z(v) + zb[x, :tall] * next_z(v))

        def relax(x, rows_of, edge, more=None):
            tall = cells_y if edge else wy
            v, t = faces(x, rows_of, more, tall)
            return (1.0 - damping) * v + (t - goal[x, :tall])

        def cascade(levels, lag, rows_of=None, part=None):
            if rows_of is None:
                rows_of = [{} for _ in levels]
            low = min(level[0] for level in levels)
            high = max(level[1] for level in levels)
            for step in range(low, high + lag * len(levels)):
                for k, (start, end, row) in enumerate(levels):
                    x = step - lag * k
                    if start <= x < end and x not in rows_of[k] and (part is None or x < part[k]):
                        rows_of[k][x] = row(x, rows_of[k - 1], x in (start, end - 1))
            return rows_of

        def coarse_setup():
            swapped = [swap_z(coarse_m[c]) for c in range(blocks + 2)]
            for c in range(1, blocks + 1):
                lo, hi = jnp.where(even_c, swapped[c - 1], swapped[c]), jnp.where(even_c, swapped[c], swapped[c + 1])
                m, b = coarse_m[c], c - 1
                lo_x, hi_x = m + lo, m + hi
                lo_y, hi_y = m + prev_y(m), m + next_y(m)
                lo_z = m + jnp.where(lane_c < 2, 0.0, prev_z(m, 2))
                hi_z = m + jnp.where(lane_c >= cells_z - 2, 0.0, next_z(m, 2))
                diag = (lo_x + hi_x) + (lo_y + hi_y) + (lo_z + hi_z)
                inside = m > 0.0
                inv = jnp.where(inside, damping / jnp.where(inside, diag, 1.0), 0.0)
                cxa[b], cxb[b] = lo_x * inv, hi_x * inv
                cya[b], cyb[b] = lo_y * inv, hi_y * inv
                cza[b] = jnp.where(lane_c < 2, 0.0, lo_z * inv)
                czb[b] = jnp.where(lane_c >= cells_z - 2, 0.0, hi_z * inv)
                cinv[b] = inv

        shifted = {}

        def pad_c(v):
            if v.shape[0] == 3 * half_y:
                return v
            none = jnp.zeros((half_y, cells_z), f32)
            return jnp.concatenate([none, v, none], 0)

        def swapped(rows_of, b):
            key = (id(rows_of), b)
            if key not in shifted:
                shifted[key] = pad_c(swap_z(rows_of[b]))
            return shifted[key]

        def level_relax(b, rows_of, _):
            return coarse_relax(b, rows_of, False)

        def coarse_relax(b, rows_of, edge):
            v = rows_of[b]
            span = pl.ds(half_y, half_y) if edge else pl.ds(0, 3 * half_y)
            cut = slice(half_y, 2 * half_y) if edge else slice(None)
            before = b - 1 if b - 1 in rows_of else b
            behind = b + 1 if b + 1 in rows_of else b
            lo = jnp.where(even_c, swapped(rows_of, before), swapped(rows_of, b))
            hi = jnp.where(even_c, swapped(rows_of, b), swapped(rows_of, behind))
            before, behind = prev_y(v)[cut], next_y(v)[cut]
            v = v[cut]
            t = cxa[b, span] * lo[cut] + cxb[b, span] * hi[cut]
            t = t + (cya[b, span] * before + cyb[b, span] * behind)
            t = t + (cza[b, span] * prev_z(v, 2) + czb[b, span] * next_z(v, 2))
            return (1.0 - damping) * v + (t - right[b, span])

        own = range(HX, HX + rows)
        margin, tall = half_y // 2, 2 * cells_y

        def send(at, deeper):
            totals = {}

            def smoothed(x, rows_of, edge):
                v = deeper(x, rows_of, edge)
                if x in own:
                    press[at, x, own_y] = v[:cells_y]
                return v

            def residual(x, rows_of, _):
                v, t = faces(x, rows_of, None, cells_y)
                d = (damping * v - (t - goal[x, :cells_y])) * scale_back[x - HX]
                totals[x] = d
                if (x - HX) % 2 == 1:
                    fold[(x - HX) // 2] = totals[x - 1] + d
                return d

            return smoothed, residual

        def leave_off(at):
            for b in range(2):
                packed_r[at, OWN + b, own_c] = pack([folded(2 * b), folded(2 * b + 1)])
            r_x[at][0](ODD)
            p_x[at][0](ODD)

        def correct(at):
            r_x[at][1](ODD)

            def begin(b, _, edge):
                r = packed_r[at, b] * cinv[b]
                right[b] = r
                return -r

            def prolong(b, rows_of, edge):
                c = coarse_relax(b, rows_of, edge)
                d = swap_z(c)
                even = even_c[: c.shape[0]]
                for odd_row in (0, 1):
                    q = 2 * (b - OWN) + odd_row
                    if -3 <= q < rows // 2 + 3:
                        v = jnp.where(even, d, c) if odd_row else jnp.where(even, c, d)
                        v = pad_c(v)[margin : margin + cells_y]
                        spread[q + 3, pl.ds(0, tall // 2, stride=2)] = v
                        spread[q + 3, pl.ds(1, tall // 2, stride=2)] = v
                return c

            held = [(0, blocks, begin), (0, blocks, coarse_relax), (1, blocks - 1, level_relax), (1, blocks - 1, prolong)]
            kept = cascade(held, 20)
            shifted.clear()
            p_x[at][1](ODD)
            fifths = {}

            def add(x, _, edge):
                up = spread.at[(x - HX) // 2 + 3]
                if edge:
                    return press[at, x, own_y] + up[pl.ds(8, cells_y)]
                ahead, after = up[pl.ds(0, 8)], up[pl.ds(8 + cells_y, 8)]
                if at == 0 and x in own:
                    fifths[x] = fifth_p[x - HX] + jnp.where(middle < HY, ahead, after)
                change = jnp.concatenate([up[pl.ds(8, cells_y)], jnp.where(middle < HY, after, ahead)], 0)
                return press[at, x] + change

            return add, lambda x, rows_of, edge: relax(x, rows_of, edge, fifths.get(x))

        low, high = HX, HX + rows
        smoothed, residual = send(0, relax)
        cascade(
            [
                (low - 2, high + 2, lambda x, _, edge: fine_setup((x,), False, edge)),
                (low - 1, high + 1, smoothed),
                (low, high, residual),
            ],
            20,
        )
        leave_off(0)
        inputs[3].wait()
        s_x[0](ODD)
        g_x[1](ODD)
        fine_setup(range(1, wx - 1), True)
        m_x[1](ODD)
        coarse_setup()
        add, first_relax = correct(0)
        smoothed, residual = send(1, relax)
        cascade(
            [
                (low - 5, high + 5, add),
                (low - 4, high + 4, first_relax),
                (low - 3, high + 3, relax),
                (low - 2, high + 2, relax),
                (low - 1, high + 1, smoothed),
                (low, high, residual),
            ],
            20,
        )
        leave_off(1)
        last = pb
        add, first_relax = correct(1)

        def final(x, rows_of, edge):
            v = relax(x, rows_of, edge)
            if edge:
                last[x, own_y] = v
            else:
                last[x] = v
            return v

        levels = [(low - 4, high + 4, add), (low - 3, high + 3, first_relax), (low - 2, high + 2, final)]
        top = HX + cells_x + 2
        kept = cascade(levels, 20, None, (top + 2, top + 1, top))
        b_x[0](ODD)

        def along_x(x):
            return near[0, x, own_y] * (0.5 * (last[x + 1, own_y] - last[x - 1, own_y]))

        def along_y(x, y):
            one = pl.ds(y, 1)
            return near[0, x, one] * (0.5 * (last[x, pl.ds((y + 1) % wy, 1)] - last[x, pl.ds(y - 1, 1)]))

        def edge(at):
            v = edge_x[EDGES.index(at), own_y]
            return (v + v) - along_x(HX + at)

        def ends(x):
            lo, hi = edge_y[x, pl.ds(0, 1)], edge_y[x, pl.ds(3, 1)]
            return (lo + lo) - along_y(x, wy - 1), (hi + hi) - along_y(x, cells_y)

        rim_v[0] = edge(-1)
        rim_v[1] = edge(cells_x)
        for x in range(cells_x):
            lo, hi = ends(HX + x)
            rim_w[x, pl.ds(0, 1)] = lo
            rim_w[x, pl.ds(1, 1)] = hi
        v_x[0](ODD)
        cascade(levels, 20, kept)
        out_x[0] = edge(cells_x - 1)
        out_x[cells_x + 1] = edge(rows)
        for x in range(cells_x):
            w = HX + cells_x + x
            m = near[0, w, own_y]
            p = last[w, own_y]
            out_x[1 + x] = velocity[0, x] - along_x(w)
            v = last[w]
            out_y[x, own_y] = velocity[1, x] - m * (0.5 * (next_y(v) - prev_y(v))[:cells_y])
            lo, hi = ends(w)
            out_y[x, pl.ds(wy - 1, 1)] = lo
            out_y[x, pl.ds(cells_y, 1)] = hi
            dz = jnp.where(lane_o == cells_z - 1, 0.0, next_z(p)) - jnp.where(lane_o == 0, 0.0, prev_z(p))
            out_z[x] = velocity[2, x] - m * (0.5 * dz)
            out_p[x] = p
        s_x[1](ODD)
        for x in every[1:]:
            x[2](ODD)

    assert groups == MOVES, groups


MOVES = [36, 24, 14, 14, 14, 10, 8, 8, 1, 4]


def transport(in_x, in_y, in_z, in_p, rim_x, rim_y, species, vel_out, pres_out, spec_out, stage, sems):
    cells_x, cells_y, cells_z = in_p.shape
    lane_o = lax.broadcasted_iota(jnp.int32, (cells_y, cells_z), 1)
    row_o = lax.broadcasted_iota(jnp.int32, (cells_y, cells_z), 0)

    def next_z(v):
        return pltpu.roll(v, cells_z - 1, 1)

    def prev_z(v):
        return pltpu.roll(v, 1, 1)

    def next_y(v):
        return pltpu.roll(v, v.shape[0] - 1, 0)

    def prev_y(v):
        return pltpu.roll(v, 1, 0)

    mid = slice(0, cells_y)
    copies = [
        pltpu.make_async_copy(src, dst, sems.at[at])
        for at, (src, dst) in enumerate(
            (
                (in_x.at[pl.ds(1, cells_x)], vel_out.at[0]),
                (in_y.at[:, pl.ds(0, cells_y)], vel_out.at[1]),
                (in_z, vel_out.at[2]),
                (in_p, pres_out),
                *((stage.at[x], spec_out.at[:, x]) for x in range(cells_x)),
            )
        )
    ]
    for copy in copies[:4]:
        copy.start()
    move_x = [in_x[x] for x in range(cells_x + 2)]
    for x in range(cells_x):
        move_y, move_z = in_y[x], in_z[x]
        lo_x, hi_x = 0.5 * (move_x[x] + move_x[x + 1]), 0.5 * (move_x[x + 1] + move_x[x + 2])
        lo_y, hi_y = (0.5 * (move_y + prev_y(move_y)))[mid], (0.5 * (move_y + next_y(move_y)))[mid]
        lo_z = 0.5 * (move_z + jnp.where(lane_o == 0, 0.0, prev_z(move_z)))
        hi_z = 0.5 * (move_z + jnp.where(lane_o == cells_z - 1, 0.0, next_z(move_z)))

        def into(flow):
            return time_step * jnp.maximum(flow, 0.0)

        def back(flow):
            return -time_step * jnp.minimum(flow, 0.0)

        keep = 1.0 - (into(hi_x) + into(hi_y) + into(hi_z)) - (back(lo_x) + back(lo_y) + back(lo_z))
        from_xl, from_xu = into(lo_x), back(hi_x)
        from_yl, from_yu = into(lo_y), back(hi_y)
        from_zl = jnp.where(lane_o == 0, 0.0, into(lo_z))
        from_zu = jnp.where(lane_o == cells_z - 1, 0.0, back(hi_z))
        for s in range(species.shape[0]):
            q = species[s, x]
            xl = rim_x[0, s] if x == 0 else species[s, x - 1]
            xu = rim_x[1, s] if x == cells_x - 1 else species[s, x + 1]
            yl = jnp.where(row_o == 0, rim_y[0, s, pl.ds(x, 1)], prev_y(q))
            yu = jnp.where(row_o == cells_y - 1, rim_y[1, s, pl.ds(x, 1)], next_y(q))
            total = keep * q + (from_xl * xl + from_xu * xu) + (from_yl * yl + from_yu * yu)
            stage[x, s] = total + (from_zl * prev_z(q) + from_zu * next_z(q))
        copies[4 + x].start()
    for copy in copies:
        copy.wait()


def local(slabs, crosses, velocity, density, source, species):
    cells_x, cells_y, cells_z = density.shape
    assert cells_x == 4 and cells_y == 16 and slabs % 2 == 0
    rows = 2 * cells_x
    wx, wy = rows + 2 * HX, cells_y + 2 * HY
    half_y = cells_y // 2
    kinds = species.shape[0]
    f32 = jnp.float32

    def vmem(*shape):
        return pltpu.VMEM(shape, f32)

    blocks = 2 * OWN + 2
    fine, coarse = (wx, wy, cells_z), (blocks, 3 * half_y, cells_z)
    dma = pltpu.SemaphoreType.DMA
    spec = pl.BlockSpec(memory_space=pltpu.VMEM)
    far = pl.BlockSpec(memory_space=pltpu.HBM)
    moved = [
        (cells_x + 2, cells_y, cells_z), (cells_x, wy, cells_z), density.shape, density.shape,
        (2, kinds, cells_y, cells_z), (2, kinds, cells_x, cells_z), species.shape,
    ]
    between = pl.pallas_call(
        functools.partial(kernel, slabs, crosses),
        out_shape=tuple(pltpu.VMEM(shape, f32) for shape in moved),
        in_specs=[far] * 4,
        out_specs=(spec,) * 7,
        scratch_shapes=[vmem(*velocity.shape), vmem(*density.shape), vmem(*density.shape)]
        + [vmem(2, *density.shape), vmem(2, cells_y, cells_z), vmem(cells_x, 8, cells_z), vmem(half_y, cells_z)]
        + [vmem(2, *fine)] * 2 + [vmem(rows, 8, cells_z), vmem(len(EDGES), wy, cells_z), vmem(wx, 8, cells_z)]
        + [vmem(CYCLES, *fine), vmem(rows, 8, cells_z), vmem(blocks + 2, *coarse[1:]), vmem(CYCLES, *coarse), vmem(cells_x + 2, wy, cells_z)]
        + [vmem(*fine)] * 7 + [vmem(rows, cells_y, cells_z), vmem(*fine)]
        + [vmem(*coarse)] * 8 + [vmem(cells_x, cells_y, cells_z), vmem(rows // 2 + 6, 2 * cells_y, cells_z)]
        + [vmem(2, cells_y, cells_z), vmem(cells_x, 8, cells_z)]
        + [dma((4,))] + [dma((n,)) for n in MOVES for _ in range(2)],
        compiler_params=pltpu.CompilerParams(
            collective_id=0, has_side_effects=True, vmem_limit_bytes=16 << 20,
        ),
        name="projection",
    )(*(pltpu.with_memory_space_constraint(a, pltpu.HBM) for a in (velocity, density, source, species)))
    return pl.pallas_call(
        transport,
        out_shape=tuple(jax.ShapeDtypeStruct(a.shape, f32) for a in (velocity, density, species)),
        in_specs=[spec] * 7,
        out_specs=(far,) * 3,
        scratch_shapes=[vmem(cells_x, kinds, cells_y, cells_z), dma((4 + cells_x,))],
        compiler_params=pltpu.CompilerParams(vmem_limit_bytes=8 << 20),
        name="transport",
    )(*between)


def solution(mesh):
    plane, stack = P("slab", "cross", None), P(None, "slab", "cross", None)
    return jax.shard_map(
        functools.partial(local, mesh.shape["slab"], mesh.shape["cross"]),
        mesh=mesh,
        in_specs=(stack, plane, plane, stack),
        out_specs=(stack, plane, stack),
        check_vma=False,
    )
```

```python
import functools

import jax
import jax.numpy as jnp
from jax import lax
from jax.experimental import pallas as pl
from jax.experimental.pallas import tpu as pltpu
from jax.sharding import PartitionSpec as P

CYCLES = 2
COARSE = 4
damping = 0.8
time_step = 0.25
MESH = pl.DeviceIdType.MESH
HX = 5
HY = 4
EVEN, ODD = 0, 1
OWN = 3

EDGES = (-5, -1, 0, 3, 4, 7, 8, 12)
BELOW = {-1: 2, 3: 4, 7: 6, 11: 7}
ABOVE = {-4: 0, 0: 1, 4: 3, 8: 5}


def kernel(
    slabs, crosses, velocity_in, density_in, source_in, species,
    out_x, out_y, out_z, out_p, rim_x, rim_y, kinds,
    velocity, density, source, stage, stage_x, stage_y, stage_c,
    near, later, fifth_m, edge_x, edge_y, press, fifth_p, coarse_m, packed_r, given,
    xa, xb, ya, yb, za, zb, goal, scale_back, pb,
    cxa, cxb, cya, cyb, cza, czb, cinv, right, fold, spread, rim_v, rim_w, in_sem, *sems,
):
    cells_x, cells_y, cells_z = density.shape
    rows = 2 * cells_x
    wx, wy = rows + 2 * HX, cells_y + 2 * HY
    half_y = cells_y // 2
    blocks = packed_r.shape[1]
    own_y = pl.ds(0, cells_y)
    own_c = pl.ds(half_y, half_y)
    slab, cross = lax.axis_index("slab"), lax.axis_index("cross")
    odd = slab % 2 == 1
    f32 = jnp.float32

    def there(dx, dy):
        return (slab + dx >= 0) & (slab + dx < slabs) & (cross + dy >= 0) & (cross + dy < crosses)

    groups = []

    def exchange(moves):
        at = len(groups)
        send, recv = sems[2 * at], sems[2 * at + 1]
        groups.append(len(moves))

        def copy(index):
            _, dx, dy, src, dst = moves[index]
            return pltpu.make_async_remote_copy(
                src_ref=src, dst_ref=dst, send_sem=send.at[index], recv_sem=recv.at[index],
                device_id=(slab + dx, cross + dy), device_id_type=MESH,
            )

        def each(role, sender, act, only=None):
            for index, (by, dx, dy, _, _) in enumerate(moves):
                if only is not None and ((dx, dy) == (1, 0)) != only:
                    continue
                if sender and by == role:
                    @pl.when(there(dx, dy))
                    def _():
                        act(copy(index))
                if not sender and (by + dx) % 2 == role:
                    @pl.when(there(-dx, -dy))
                    def _():
                        act(copy(index))

        def start(role):
            each(role, True, lambda c: c.start())

        def arrive(role, only=None):
            each(role, False, lambda c: c.wait_recv(), only)

        def leave(role):
            each(role, True, lambda c: c.wait_send())

        return start, arrive, leave

    def cut_y(dy, low, high, home=0, span=cells_y, rim=wy, behind=cells_y):
        depth = high - low + 1
        if dy > 0:
            return pl.ds(home + span - high, depth), pl.ds(rim - high, depth)
        return pl.ds(home + low - 1, depth), pl.ds(behind + low - 1, depth)

    def fifth(dy):
        return (cells_y - 5, 3) if dy > 0 else (4, 4)

    whole = slice(None)
    first, rest = [], []
    for by, base, out in ((EVEN, 0, -1), (ODD, cells_x, 2)):
        to = 1 - by
        lo_edge, hi_edge = EDGES.index(base), EDGES.index(base + cells_x - 1)
        at = rows if by == EVEN else -cells_x
        touch = 0 if by == EVEN else cells_x - 1
        edge = EDGES.index(at + touch)

        def seen(deep, count, at=at, by=by):
            start = deep - 1 if by == EVEN else cells_x - deep - count + 1
            return pl.ds(start, count), pl.ds(HX + at + start, count)

        for dy in (-1, 1):
            j, k = (2, 0) if dy > 0 else (1, 3)
            src, dst = seen(1, 2)
            ys, yd = cut_y(dy, 1, 2)
            first.append((by, out, dy, stage.at[whole, src, ys], near.at[whole, dst, yd]))
            ys, yd = cut_y(dy, 1, 4)
            first.append((by, out, dy, stage_x.at[min(touch, 1), ys], edge_x.at[edge, yd]))
            first.append((by, out, dy, stage_y.at[whole, j], edge_y.at[pl.ds(HX + at, cells_x), k]))
        src, dst = seen(1, 3)
        first.append((by, out, 0, stage.at[0, src], near.at[0, dst, own_y]))
        src, dst = seen(1, 2)
        first.append((by, out, 0, stage.at[1, src], near.at[1, dst, own_y]))
        first.append((by, out, 0, stage_x.at[min(touch, 1)], edge_x.at[edge, own_y]))
        first.append((by, out, 0, stage_y.at[whole, pl.ds(1, 2)], edge_y.at[pl.ds(HX + at, cells_x), pl.ds(1, 2)]))
        mine = pl.ds(HX + base, cells_x)
        for dy in (-1, 1):
            j, k = (2, 0) if dy > 0 else (1, 3)
            ys, yd = cut_y(dy, 1, 3)
            first.append((by, to, dy, stage.at[whole, whole, ys], near.at[whole, mine, yd]))
            ys, yd = cut_y(dy, 1, 4)
            first.append((by, to, dy, stage_x.at[whole, ys], edge_x.at[pl.ds(lo_edge, 2), yd]))
            first.append((by, to, dy, stage_y.at[whole, j], edge_y.at[mine, k]))
        if by == EVEN:
            first.append((by, 1, 0, stage, near.at[whole, mine, own_y]))
            first.append((by, 1, 0, stage_x, edge_x.at[pl.ds(lo_edge, 2), own_y]))
            first.append((by, 1, 0, stage_y.at[whole, pl.ds(1, 2)], edge_y.at[mine, pl.ds(1, 2)]))
            first.append((by, 1, 0, stage_c, coarse_m.at[OWN + 1, own_c]))

        for dy in (-1, 1):
            for deep, low, high in ((1, 3, 4), (3, 1, 2)):
                src, dst = seen(deep, 2)
                ys, yd = cut_y(dy, low, high)
                rest.append((by, out, dy, stage.at[whole, src, ys], later.at[whole, dst, yd]))
        src, dst = seen(4, 1)
        rest.append((by, out, 0, stage.at[0, src], later.at[0, dst, own_y]))
        src, dst = seen(3, 2)
        rest.append((by, out, 0, stage.at[1, src], later.at[1, dst, own_y]))
        far, row, lands = (3, cells_x - 1, -HX) if by == EVEN else (-2, 0, rows + HX - 1)
        rest.append((by, far, 0, stage.at[0, row], later.at[0, HX + lands, own_y]))
        rest.append((by, far, 0, stage_x.at[min(row, 1)], edge_x.at[EDGES.index(lands), own_y]))
        for dy in (-1, 1):
            ys, yd = cut_y(dy, 4, 4)
            rest.append((by, to, dy, stage.at[whole, whole, ys], later.at[whole, mine, yd]))
            y, j = fifth(dy)
            rest.append((by, to, dy, stage.at[0, whole, y], fifth_m.at[pl.ds(base, cells_x), j]))

    def coarse_moves(ref, own, reach):
        moves = []
        ahead, behind, aside = (2, own, own - 2, 2, reach - 1), (-2, own, own + 2, 2, reach - 1), (0, own, own, 2, reach)
        count = (reach - 3) // 2
        ahead_far, behind_far = (4, own + 2 - count, own - 2 - count, count, reach - 5), (-4, own, own + 4, count, reach - 5)
        for dy, kinds_of in (
            (-1, (ahead, behind)), (1, (ahead, behind)), (0, (ahead, behind)),
            (-1, (ahead_far, behind_far)), (1, (ahead_far, behind_far)), (0, (ahead_far, behind_far)), (-1, (aside,)), (1, (aside,)),
        ):
            for dx, src, dst, count, deep in kinds_of:
                ys, yd = (own_c, own_c) if dy == 0 else cut_y(dy, 1, deep, half_y, half_y, half_y, 2 * half_y)
                moves.append((ODD, dx, dy, ref.at[pl.ds(src, count), ys], ref.at[pl.ds(dst, count), yd]))
        return moves

    def press_moves(ref, reach):
        moves = []
        low, high = (pl.ds(HX, reach), pl.ds(HX + rows, reach)), (pl.ds(HX + rows - reach, reach), pl.ds(HX - reach, reach))
        corner = reach - 1
        low_c, high_c = (pl.ds(HX, corner), pl.ds(HX + rows, corner)), (pl.ds(HX + rows - corner, corner), pl.ds(HX - corner, corner))
        for dy in (-1, 1):
            ys, yd = cut_y(dy, 1, corner)
            moves.append((ODD, 2, dy, ref.at[high_c[0], ys], ref.at[high_c[1], yd]))
            moves.append((ODD, -2, dy, ref.at[low_c[0], ys], ref.at[low_c[1], yd]))
        moves.append((ODD, 2, 0, ref.at[high[0], own_y], ref.at[high[1], own_y]))
        moves.append((ODD, -2, 0, ref.at[low[0], own_y], ref.at[low[1], own_y]))
        own_x = pl.ds(HX, rows)
        for dy in (-1, 1):
            ys, yd = cut_y(dy, 1, HY)
            moves.append((ODD, 0, dy, ref.at[own_x, ys], ref.at[own_x, yd]))
            if reach > HY:
                y, j = fifth(dy)
                moves.append((ODD, 0, dy, ref.at[own_x, y], fifth_p.at[:, j]))
        return moves

    def species_moves():
        moves = []
        for by in (EVEN, ODD):
            for dx, dy in ((-1, 0), (1, 0), (0, -1), (0, 1)):
                if dx != 0:
                    src, dst = kinds.at[:, cells_x - 1 if dx > 0 else 0], rim_x.at[0 if dx > 0 else 1]
                else:
                    src, dst = kinds.at[:, :, cells_y - 1 if dy > 0 else 0], rim_y.at[0 if dy > 0 else 1]
                moves.append((by, dx, dy, src, dst))
        return moves

    back = [
        (ODD, -1, 0, pb.at[pl.ds(HX - 1, cells_x + 2), pl.ds(0, cells_y + 1)], given.at[whole, pl.ds(0, cells_y + 1)]),
        (ODD, -1, 0, pb.at[pl.ds(HX, cells_x), wy - 1], given.at[pl.ds(1, cells_x), wy - 1]),
    ]
    sides = [
        (ODD, -1, 0, rim_v.at[0], out_x.at[0]),
        (ODD, -1, 0, rim_v.at[1], out_x.at[cells_x + 1]),
        (ODD, -1, 0, rim_w.at[whole, 0], out_y.at[whole, wy - 1]),
        (ODD, -1, 0, rim_w.at[whole, 1], out_y.at[whole, cells_y]),
    ]

    f_x, g_x, m_x = exchange(first), exchange(rest), exchange(coarse_moves(coarse_m, OWN + 1, 7))
    r_x = [exchange(coarse_moves(packed_r.at[at], OWN, 6)) for at in range(CYCLES)]
    p_x = [exchange(press_moves(press.at[at], HX - at)) for at in range(CYCLES)]
    s_x, b_x, v_x = exchange(species_moves()), exchange(back), exchange(sides)
    every = (f_x, g_x, m_x, *r_x, *p_x, s_x, b_x, v_x)

    def grids(count):
        lane = lax.broadcasted_iota(jnp.int32, (count, cells_z), 1)
        row = lax.broadcasted_iota(jnp.int32, (count, cells_z), 0)
        return row, lane

    def next_z(v, k=1):
        return pltpu.roll(v, cells_z - k, 1)

    def prev_z(v, k=1):
        return pltpu.roll(v, k, 1)

    def next_y(v):
        return pltpu.roll(v, v.shape[0] - 1, 0)

    def prev_y(v):
        return pltpu.roll(v, 1, 0)

    def swap_z(v):
        lane = grids(v.shape[0])[1]
        return jnp.take_along_axis(v, lane + 1 - 2 * (lane % 2), axis=1)

    def pack(two):
        lane = grids(two[0].shape[0])[1]
        return jnp.where(lane % 2 == 0, two[0] + swap_z(two[0]), two[1] + swap_z(two[1]))

    inputs = [
        pltpu.make_async_copy(src, dst, in_sem.at[at])
        for at, (src, dst) in enumerate(
            ((velocity_in, velocity), (density_in, density), (source_in, source), (species, kinds))
        )
    ]
    for copy in inputs:
        copy.start()
    barrier = pltpu.get_barrier_semaphore()
    greet = {ODD: set(), EVEN: set()}
    for moves in (first, rest, coarse_moves(coarse_m, OWN + 1, 7), species_moves(), back):
        for by, dx, dy, _, _ in moves:
            greet[by].add((dx, dy))
            greet[(by + dx) % 2].add((-dx, -dy))

    def enter(role):
        for dx, dy in sorted(greet[role], key=lambda d: (abs(d[0]) == 4, -abs(d[0]) - 2 * abs(d[1]), d)):
            @pl.when(there(dx, dy))
            def _():
                pl.semaphore_signal(barrier, inc=1, device_id=(slab + dx, cross + dy), device_id_type=MESH)

    def entered(role):
        count = jnp.int32(0)
        for dx, dy in sorted(greet[role]):
            count = count + there(dx, dy).astype(jnp.int32)
        return count

    @pl.when(jnp.logical_not(odd))
    def _():
        enter(EVEN)

    @pl.when(odd)
    def _():
        enter(ODD)

    def clear(dx, dy, *refs):
        @pl.when(jnp.logical_not(there(dx, dy)))
        def _():
            for ref in refs:
                ref[...] = jnp.zeros(ref.shape, f32)

    for copy in inputs[:3]:
        copy.wait()
    row_o, lane_o = grids(cells_y)
    for x in range(cells_x):
        v0, v1, v2 = velocity[0, x], velocity[1, x], velocity[2, x]
        dz = jnp.where(lane_o == cells_z - 1, 0.0, next_z(v2)) - jnp.where(lane_o == 0, 0.0, prev_z(v2))
        dy = jnp.where(row_o == cells_y - 1, 0.0, next_y(v1)) - jnp.where(row_o == 0, 0.0, prev_y(v1))
        t = dy + dz
        if x + 1 < cells_x:
            t = t + velocity[0, x + 1]
        if x > 0:
            t = t - velocity[0, x - 1]
        m = 1.0 / density[x]
        stage[0, x] = m
        stage[1, x] = 0.5 * t - source[x]
        fold[x] = m
        stage_y[x, pl.ds(1, 1)] = 0.5 * v1[0:1]
        stage_y[x, pl.ds(2, 1)] = 0.5 * v1[cells_y - 1 : cells_y]
        if x == 0:
            stage_x[0] = 0.5 * v0
        if x == cells_x - 1:
            stage_x[1] = 0.5 * v0

    def folded(x):
        return fold[x, pl.ds(0, half_y, stride=2)] + fold[x, pl.ds(1, half_y, stride=2)]

    mean = 0.125 * pack([folded(0) + folded(1), folded(2) + folded(3)])
    stage_c[...] = mean
    pl.semaphore_wait(barrier, jnp.where(odd, entered(ODD), entered(EVEN)))

    @pl.when(jnp.logical_not(odd))
    def _():
        f_x[0](EVEN)
        clear(-1, 0, rim_x.at[0])
        clear(1, 0, rim_x.at[1])
        clear(0, -1, rim_y.at[0])
        clear(0, 1, rim_y.at[1])
        f_x[2](EVEN)
        g_x[0](EVEN)
        inputs[3].wait()
        s_x[0](EVEN)
        b_x[1](EVEN)
        for x in range(cells_x):
            m = stage[0, x]
            p = given[1 + x, own_y]
            out_x[1 + x] = velocity[0, x] - m * (0.5 * (given[2 + x, own_y] - given[x, own_y]))
            v = given[1 + x]
            out_y[x, own_y] = velocity[1, x] - m * (0.5 * (next_y(v) - prev_y(v))[:cells_y])
            row_o, lane_o = grids(cells_y)
            dz = jnp.where(lane_o == cells_z - 1, 0.0, next_z(p)) - jnp.where(lane_o == 0, 0.0, prev_z(p))
            out_z[x] = velocity[2, x] - m * (0.5 * dz)
            out_p[x] = p
        v_x[1](EVEN)
        s_x[1](EVEN)
        for x in every[1:]:
            x[2](EVEN)

    @pl.when(odd)
    def _():
        f_x[0](ODD)
        clear(-1, 0, rim_x.at[0])
        clear(1, 0, rim_x.at[1])
        clear(0, -1, rim_y.at[0])
        clear(0, 1, rim_y.at[1])
        for dx, lo, hi, edges, m_lo, m_hi, r_lo, r_hi in (
            (-2, 0, HX, 0, 0, OWN + 1, 0, OWN), (2, HX + rows, wx, len(EDGES) - 2, OWN + 3, blocks + 2, OWN + 2, blocks),
        ):
            rim = pl.ds(lo, hi - lo)
            clear(
                dx, 0, near.at[:, rim], later.at[:, rim], press.at[:, rim], edge_y.at[rim], edge_x.at[pl.ds(edges, 2)],
                coarse_m.at[pl.ds(m_lo, m_hi - m_lo)], packed_r.at[:, pl.ds(r_lo, r_hi - r_lo)],
            )
        clear(-4, 0, coarse_m.at[pl.ds(0, 2)], packed_r.at[:, 0])
        clear(4, 0, coarse_m.at[pl.ds(blocks, 2)], packed_r.at[:, blocks - 1])
        for dy, first_y, first_c, j, k in ((-1, wy - HY, 0, 0, 3), (1, cells_y, 2 * half_y, 3, 4)):
            rim, rim_c = pl.ds(first_y, HY), pl.ds(first_c, half_y)
            clear(
                0, dy, near.at[:, :, rim], later.at[:, :, rim], press.at[:, :, rim], edge_x.at[:, rim], edge_y.at[:, j],
                fifth_m.at[:, k], fifth_p.at[:, k], coarse_m.at[:, rim_c], packed_r.at[:, :, rim_c],
            )
        f_x[2](ODD)
        row_w, lane_w = grids(wy)
        row_c, lane_c = grids(2 * half_y + half_y)
        even_c = lane_c % 2 == 0
        row_o, lane_o = grids(cells_y)
        mine = pl.ds(HX + cells_x, cells_x)
        near[0, mine, own_y] = stage[0]
        near[1, mine, own_y] = stage[1]
        edge_x[pl.ds(EDGES.index(cells_x), 2), own_y] = stage_x[...]
        edge_y[mine, pl.ds(1, 2)] = stage_y[:, pl.ds(1, 2)]
        coarse_m[OWN + 2, own_c] = stage_c[...]
        f_x[1](ODD, True)
        m_x[0](ODD)
        g_x[0](ODD)
        f_x[1](ODD, False)

        middle = grids(8)[0]

        def around_y(v, more=None):
            if more is None:
                return prev_y(v), next_y(v)
            own, rim = v[:cells_y], v[cells_y:]
            return (
                prev_y(jnp.concatenate([own, jnp.where(middle == 3, more, rim)], 0)),
                next_y(jnp.concatenate([own, jnp.where(middle == 4, more, rim)], 0)),
            )

        def fine_setup(span, full, edge=False):
            def take(field, x, deep):
                if not full:
                    return near[field, x]
                away = max(0, HX - x, x - (HX + rows - 1))
                own = (near if away <= deep else later)[field, x, own_y]
                cells = (3, 2, 2, 0, 0, 0)[away]
                rim = later[field, x, pl.ds(cells_y, 8)]
                if cells > 0:
                    off = jnp.where(middle < HY, middle + 1, 8 - middle)
                    rim = jnp.where(off <= cells, near[field, x, pl.ds(cells_y, 8)], rim)
                return jnp.concatenate([own, rim], 0)

            def mob(x):
                return take(0, x, 3)

            for x in span:
                m = mob(x)
                lo_x, hi_x = m + mob(x - 1), m + mob(x + 1)
                before, behind = around_y(m, fifth_m[x - HX] if full and HX <= x < HX + rows else None)
                lo_y, hi_y = m + before, m + behind
                lo_z = m + jnp.where(lane_w == 0, 0.0, prev_z(m))
                hi_z = m + jnp.where(lane_w == cells_z - 1, 0.0, next_z(m))
                diag = (lo_x + hi_x) + (lo_y + hi_y) + (lo_z + hi_z)
                inside = m > 0.0
                inv = jnp.where(inside, damping / jnp.where(inside, diag, 1.0), 0.0)
                if not edge:
                    xa[x], xb[x] = lo_x * inv, hi_x * inv
                    ya[x], yb[x] = lo_y * inv, hi_y * inv
                    za[x] = jnp.where(lane_w == 0, 0.0, lo_z * inv)
                    zb[x] = jnp.where(lane_w == cells_z - 1, 0.0, hi_z * inv)
                t = take(1, x, 2)
                at = x - HX
                if at in BELOW and (full or BELOW[at] not in (0, 7)):
                    t = t + edge_x[BELOW[at]]
                if at in ABOVE and (full or ABOVE[at] not in (0, 7)):
                    t = t - edge_x[ABOVE[at]]

                def side(j):
                    return jnp.broadcast_to(edge_y[x, pl.ds(j, 1)], t.shape)

                t = t + jnp.where(row_w == wy - 1, side(1), 0.0) - jnp.where(row_w == 0, side(0), 0.0)
                t = t + jnp.where(row_w == cells_y - 1, side(3), 0.0)
                t = t - jnp.where(row_w == cells_y, side(2), 0.0)
                b = t * (inv + inv)
                if edge:
                    return -b[:cells_y]
                goal[x] = b
                if not full and HX <= x < HX + rows:
                    scale_back[x - HX] = (diag * (0.5 / damping))[:cells_y]
            return -b

        def faces(x, rows_of, more, tall):
            v = rows_of[x]
            before, behind = around_y(v, more)
            v = v[:tall]
            t = xa[x, :tall] * rows_of[x - 1][:tall] + xb[x, :tall] * rows_of[x + 1][:tall]
            t = t + (ya[x, :tall] * before[:tall] + yb[x, :tall] * behind[:tall])
            return v, t + (za[x, :tall] * prev_z(v) + zb[x, :tall] * next_z(v))

        def relax(x, rows_of, edge, more=None):
            tall = cells_y if edge else wy
            v, t = faces(x, rows_of, more, tall)
            return (1.0 - damping) * v + (t - goal[x, :tall])

        def cascade(levels, lag, rows_of=None, part=None):
            if rows_of is None:
                rows_of = [{} for _ in levels]
            low = min(level[0] for level in levels)
            high = max(level[1] for level in levels)
            for step in range(low, high + lag * len(levels)):
                for k, (start, end, row) in enumerate(levels):
                    x = step - lag * k
                    if start <= x < end and x not in rows_of[k] and (part is None or x < part[k]):
                        rows_of[k][x] = row(x, rows_of[k - 1], x in (start, end - 1))
            return rows_of

        def coarse_setup():
            swapped = [swap_z(coarse_m[c]) for c in range(blocks + 2)]
            for c in range(1, blocks + 1):
                lo, hi = jnp.where(even_c, swapped[c - 1], swapped[c]), jnp.where(even_c, swapped[c], swapped[c + 1])
                m, b = coarse_m[c], c - 1
                lo_x, hi_x = m + lo, m + hi
                lo_y, hi_y = m + prev_y(m), m + next_y(m)
                lo_z = m + jnp.where(lane_c < 2, 0.0, prev_z(m, 2))
                hi_z = m + jnp.where(lane_c >= cells_z - 2, 0.0, next_z(m, 2))
                diag = (lo_x + hi_x) + (lo_y + hi_y) + (lo_z + hi_z)
                inside = m > 0.0
                inv = jnp.where(inside, damping / jnp.where(inside, diag, 1.0), 0.0)
                cxa[b], cxb[b] = lo_x * inv, hi_x * inv
                cya[b], cyb[b] = lo_y * inv, hi_y * inv
                cza[b] = jnp.where(lane_c < 2, 0.0, lo_z * inv)
                czb[b] = jnp.where(lane_c >= cells_z - 2, 0.0, hi_z * inv)
                cinv[b] = inv

        shifted = {}

        def pad_c(v):
            if v.shape[0] == 3 * half_y:
                return v
            none = jnp.zeros((half_y, cells_z), f32)
            return jnp.concatenate([none, v, none], 0)

        def swapped(rows_of, b):
            key = (id(rows_of), b)
            if key not in shifted:
                shifted[key] = pad_c(swap_z(rows_of[b]))
            return shifted[key]

        def level_relax(b, rows_of, _):
            return coarse_relax(b, rows_of, False)

        def coarse_relax(b, rows_of, edge):
            v = rows_of[b]
            span = pl.ds(half_y, half_y) if edge else pl.ds(0, 3 * half_y)
            cut = slice(half_y, 2 * half_y) if edge else slice(None)
            before = b - 1 if b - 1 in rows_of else b
            behind = b + 1 if b + 1 in rows_of else b
            lo = jnp.where(even_c, swapped(rows_of, before), swapped(rows_of, b))
            hi = jnp.where(even_c, swapped(rows_of, b), swapped(rows_of, behind))
            before, behind = prev_y(v)[cut], next_y(v)[cut]
            v = v[cut]
            t = cxa[b, span] * lo[cut] + cxb[b, span] * hi[cut]
            t = t + (cya[b, span] * before + cyb[b, span] * behind)
            t = t + (cza[b, span] * prev_z(v, 2) + czb[b, span] * next_z(v, 2))
            return (1.0 - damping) * v + (t - right[b, span])

        own = range(HX, HX + rows)
        margin, tall = half_y // 2, 2 * cells_y

        def send(at, deeper):
            totals = {}

            def smoothed(x, rows_of, edge):
                v = deeper(x, rows_of, edge)
                if x in own:
                    press[at, x, own_y] = v[:cells_y]
                return v

            def residual(x, rows_of, _):
                v, t = faces(x, rows_of, None, cells_y)
                d = (damping * v - (t - goal[x, :cells_y])) * scale_back[x - HX]
                totals[x] = d
                if (x - HX) % 2 == 1:
                    fold[(x - HX) // 2] = totals[x - 1] + d
                return d

            return smoothed, residual

        def leave_off(at):
            for b in range(2):
                packed_r[at, OWN + b, own_c] = pack([folded(2 * b), folded(2 * b + 1)])
            r_x[at][0](ODD)
            p_x[at][0](ODD)

        def correct(at):
            r_x[at][1](ODD)

            def begin(b, _, edge):
                r = packed_r[at, b] * cinv[b]
                right[b] = r
                return -r

            def prolong(b, rows_of, edge):
                c = coarse_relax(b, rows_of, edge)
                d = swap_z(c)
                even = even_c[: c.shape[0]]
                for odd_row in (0, 1):
                    q = 2 * (b - OWN) + odd_row
                    if -3 <= q < rows // 2 + 3:
                        v = jnp.where(even, d, c) if odd_row else jnp.where(even, c, d)
                        v = pad_c(v)[margin : margin + cells_y]
                        spread[q + 3, pl.ds(0, tall // 2, stride=2)] = v
                        spread[q + 3, pl.ds(1, tall // 2, stride=2)] = v
                return c

            held = [(0, blocks, begin), (0, blocks, coarse_relax), (1, blocks - 1, level_relax), (1, blocks - 1, prolong)]
            kept = cascade(held, 20)
            shifted.clear()
            p_x[at][1](ODD)
            fifths = {}

            def add(x, _, edge):
                up = spread.at[(x - HX) // 2 + 3]
                if edge:
                    return press[at, x, own_y] + up[pl.ds(8, cells_y)]
                ahead, after = up[pl.ds(0, 8)], up[pl.ds(8 + cells_y, 8)]
                if at == 0 and x in own:
                    fifths[x] = fifth_p[x - HX] + jnp.where(middle < HY, ahead, after)
                change = jnp.concatenate([up[pl.ds(8, cells_y)], jnp.where(middle < HY, after, ahead)], 0)
                return press[at, x] + change

            return add, lambda x, rows_of, edge: relax(x, rows_of, edge, fifths.get(x))

        low, high = HX, HX + rows
        smoothed, residual = send(0, relax)
        cascade(
            [
                (low - 2, high + 2, lambda x, _, edge: fine_setup((x,), False, edge)),
                (low - 1, high + 1, smoothed),
                (low, high, residual),
            ],
            20,
        )
        leave_off(0)
        inputs[3].wait()
        s_x[0](ODD)
        g_x[1](ODD)
        fine_setup(range(1, wx - 1), True)
        m_x[1](ODD)
        coarse_setup()
        add, first_relax = correct(0)
        smoothed, residual = send(1, relax)
        cascade(
            [
                (low - 5, high + 5, add),
                (low - 4, high + 4, first_relax),
                (low - 3, high + 3, relax),
                (low - 2, high + 2, relax),
                (low - 1, high + 1, smoothed),
                (low, high, residual),
            ],
            20,
        )
        leave_off(1)
        last = pb
        add, first_relax = correct(1)

        def final(x, rows_of, edge):
            v = relax(x, rows_of, edge)
            if edge:
                last[x, own_y] = v
            else:
                last[x] = v
            return v

        levels = [(low - 4, high + 4, add), (low - 3, high + 3, first_relax), (low - 2, high + 2, final)]
        top = HX + cells_x + 2
        kept = cascade(levels, 20, None, (top + 2, top + 1, top))
        b_x[0](ODD)

        def along_x(x):
            return near[0, x, own_y] * (0.5 * (last[x + 1, own_y] - last[x - 1, own_y]))

        def along_y(x, y):
            one = pl.ds(y, 1)
            return near[0, x, one] * (0.5 * (last[x, pl.ds((y + 1) % wy, 1)] - last[x, pl.ds(y - 1, 1)]))

        def edge(at):
            v = edge_x[EDGES.index(at), own_y]
            return (v + v) - along_x(HX + at)

        def ends(x):
            lo, hi = edge_y[x, pl.ds(0, 1)], edge_y[x, pl.ds(3, 1)]
            return (lo + lo) - along_y(x, wy - 1), (hi + hi) - along_y(x, cells_y)

        rim_v[0] = edge(-1)
        rim_v[1] = edge(cells_x)
        for x in range(cells_x):
            lo, hi = ends(HX + x)
            rim_w[x, pl.ds(0, 1)] = lo
            rim_w[x, pl.ds(1, 1)] = hi
        v_x[0](ODD)
        cascade(levels, 20, kept)
        out_x[0] = edge(cells_x - 1)
        out_x[cells_x + 1] = edge(rows)
        for x in range(cells_x):
            w = HX + cells_x + x
            m = near[0, w, own_y]
            p = last[w, own_y]
            out_x[1 + x] = velocity[0, x] - along_x(w)
            v = last[w]
            out_y[x, own_y] = velocity[1, x] - m * (0.5 * (next_y(v) - prev_y(v))[:cells_y])
            lo, hi = ends(w)
            out_y[x, pl.ds(wy - 1, 1)] = lo
            out_y[x, pl.ds(cells_y, 1)] = hi
            dz = jnp.where(lane_o == cells_z - 1, 0.0, next_z(p)) - jnp.where(lane_o == 0, 0.0, prev_z(p))
            out_z[x] = velocity[2, x] - m * (0.5 * dz)
            out_p[x] = p
        s_x[1](ODD)
        for x in every[1:]:
            x[2](ODD)

    assert groups == MOVES, groups


MOVES = [36, 24, 14, 14, 14, 10, 8, 8, 2, 4]


def transport(in_x, in_y, in_z, in_p, rim_x, rim_y, species, vel_out, pres_out, spec_out, stage, sems):
    cells_x, cells_y, cells_z = in_p.shape
    lane_o = lax.broadcasted_iota(jnp.int32, (cells_y, cells_z), 1)
    row_o = lax.broadcasted_iota(jnp.int32, (cells_y, cells_z), 0)

    def next_z(v):
        return pltpu.roll(v, cells_z - 1, 1)

    def prev_z(v):
        return pltpu.roll(v, 1, 1)

    def next_y(v):
        return pltpu.roll(v, v.shape[0] - 1, 0)

    def prev_y(v):
        return pltpu.roll(v, 1, 0)

    mid = slice(0, cells_y)
    copies = [
        pltpu.make_async_copy(src, dst, sems.at[at])
        for at, (src, dst) in enumerate(
            (
                (in_x.at[pl.ds(1, cells_x)], vel_out.at[0]),
                (in_y.at[:, pl.ds(0, cells_y)], vel_out.at[1]),
                (in_z, vel_out.at[2]),
                (in_p, pres_out),
                *((stage.at[x], spec_out.at[:, x]) for x in range(cells_x)),
            )
        )
    ]
    for copy in copies[:4]:
        copy.start()
    move_x = [in_x[x] for x in range(cells_x + 2)]
    for x in range(cells_x):
        move_y, move_z = in_y[x], in_z[x]
        lo_x, hi_x = 0.5 * (move_x[x] + move_x[x + 1]), 0.5 * (move_x[x + 1] + move_x[x + 2])
        lo_y, hi_y = (0.5 * (move_y + prev_y(move_y)))[mid], (0.5 * (move_y + next_y(move_y)))[mid]
        lo_z = 0.5 * (move_z + jnp.where(lane_o == 0, 0.0, prev_z(move_z)))
        hi_z = 0.5 * (move_z + jnp.where(lane_o == cells_z - 1, 0.0, next_z(move_z)))

        def into(flow):
            return time_step * jnp.maximum(flow, 0.0)

        def back(flow):
            return -time_step * jnp.minimum(flow, 0.0)

        keep = 1.0 - (into(hi_x) + into(hi_y) + into(hi_z)) - (back(lo_x) + back(lo_y) + back(lo_z))
        from_xl, from_xu = into(lo_x), back(hi_x)
        from_yl, from_yu = into(lo_y), back(hi_y)
        from_zl = jnp.where(lane_o == 0, 0.0, into(lo_z))
        from_zu = jnp.where(lane_o == cells_z - 1, 0.0, back(hi_z))
        for s in range(species.shape[0]):
            q = species[s, x]
            xl = rim_x[0, s] if x == 0 else species[s, x - 1]
            xu = rim_x[1, s] if x == cells_x - 1 else species[s, x + 1]
            yl = jnp.where(row_o == 0, rim_y[0, s, pl.ds(x, 1)], prev_y(q))
            yu = jnp.where(row_o == cells_y - 1, rim_y[1, s, pl.ds(x, 1)], next_y(q))
            total = keep * q + (from_xl * xl + from_xu * xu) + (from_yl * yl + from_yu * yu)
            stage[x, s] = total + (from_zl * prev_z(q) + from_zu * next_z(q))
        copies[4 + x].start()
    for copy in copies:
        copy.wait()


def local(slabs, crosses, velocity, density, source, species):
    cells_x, cells_y, cells_z = density.shape
    assert cells_x == 4 and cells_y == 16 and slabs % 2 == 0
    rows = 2 * cells_x
    wx, wy = rows + 2 * HX, cells_y + 2 * HY
    half_y = cells_y // 2
    kinds = species.shape[0]
    f32 = jnp.float32

    def vmem(*shape):
        return pltpu.VMEM(shape, f32)

    blocks = 2 * OWN + 2
    fine, coarse = (wx, wy, cells_z), (blocks, 3 * half_y, cells_z)
    dma = pltpu.SemaphoreType.DMA
    spec = pl.BlockSpec(memory_space=pltpu.VMEM)
    far = pl.BlockSpec(memory_space=pltpu.HBM)
    moved = [
        (cells_x + 2, cells_y, cells_z), (cells_x, wy, cells_z), density.shape, density.shape,
        (2, kinds, cells_y, cells_z), (2, kinds, cells_x, cells_z), species.shape,
    ]
    between = pl.pallas_call(
        functools.partial(kernel, slabs, crosses),
        out_shape=tuple(pltpu.VMEM(shape, f32) for shape in moved),
        in_specs=[far] * 4,
        out_specs=(spec,) * 7,
        scratch_shapes=[vmem(*velocity.shape), vmem(*density.shape), vmem(*density.shape)]
        + [vmem(2, *density.shape), vmem(2, cells_y, cells_z), vmem(cells_x, 8, cells_z), vmem(half_y, cells_z)]
        + [vmem(2, *fine)] * 2 + [vmem(rows, 8, cells_z), vmem(len(EDGES), wy, cells_z), vmem(wx, 8, cells_z)]
        + [vmem(CYCLES, *fine), vmem(rows, 8, cells_z), vmem(blocks + 2, *coarse[1:]), vmem(CYCLES, *coarse), vmem(cells_x + 2, wy, cells_z)]
        + [vmem(*fine)] * 7 + [vmem(rows, cells_y, cells_z), vmem(*fine)]
        + [vmem(*coarse)] * 8 + [vmem(cells_x, cells_y, cells_z), vmem(rows // 2 + 6, 2 * cells_y, cells_z)]
        + [vmem(2, cells_y, cells_z), vmem(cells_x, 8, cells_z)]
        + [dma((4,))] + [dma((n,)) for n in MOVES for _ in range(2)],
        compiler_params=pltpu.CompilerParams(
            collective_id=0, has_side_effects=True, vmem_limit_bytes=16 << 20,
        ),
        name="projection",
    )(*(pltpu.with_memory_space_constraint(a, pltpu.HBM) for a in (velocity, density, source, species)))
    return pl.pallas_call(
        transport,
        out_shape=tuple(jax.ShapeDtypeStruct(a.shape, f32) for a in (velocity, density, species)),
        in_specs=[spec] * 7,
        out_specs=(far,) * 3,
        scratch_shapes=[vmem(cells_x, kinds, cells_y, cells_z), dma((4 + cells_x,))],
        compiler_params=pltpu.CompilerParams(vmem_limit_bytes=8 << 20),
        name="transport",
    )(*between)


def solution(mesh):
    plane, stack = P("slab", "cross", None), P(None, "slab", "cross", None)
    return jax.shard_map(
        functools.partial(local, mesh.shape["slab"], mesh.shape["cross"]),
        mesh=mesh,
        in_specs=(stack, plane, plane, stack),
        out_specs=(stack, plane, stack),
        check_vma=False,
    )
```
